128 devices in a mesh: gx: 4 (over z_lo, core), gy: 16 (over x, y), gz: 2 (over z_hi).
Axes of the slice: x: 4, y: 4, z: 4 (z_hi: 2, z_lo: 2; z = z_hi * 2 + z_lo), core: 2. Of those that a mesh axis runs over, the one named last changes fastest.
Arguments:
- eigvecs: bfloat16 [64, 128, 96, 512], P('gx', 'gy', 'gz'), may hold values from -7 to 7, as said below
- material: float32 [2, 64, 128, 96], P(None, 'gx', 'gy', 'gz'), may hold values from 0.5 to 2
Outputs:
- stiffness: float32 [512, 512], P(('gx', 'gy', 'gz'))
- mass_matrix: float32 [512, 512], P(('gx', 'gy', 'gz'))
The draws below stay inside these ranges and needn't reach their ends.
Inputs may be any that keep to these rules, and one draw needn't show every extreme that they name: `eigvecs`: entries are a rough part plus a part that varies slowly over the grid.
All inputs are finite; a program needn't handle non-finite values.
Results may differ from the reference program's by a relative error of at most 0.0003.
Values may be sent and summed in bfloat16 or wider, within the bound.
A program may use at most 128 MiB of HBM per device.

```python
import math
import jax
import jax.numpy as jnp
from jax import lax

K = 512
NX = 64
NY = 128
NZ = 96


def draw_eigvecs(key, part):
    keys = jax.random.split(key, 7)
    rough = jnp.clip(jax.random.normal(keys[0], (NX, NY, NZ, K), jnp.float32), -4.0, 4.0)
    amplitude = 2.0
    freq_x = jax.random.randint(keys[1], (K,), 1, 4).astype(jnp.float32)
    freq_y = jax.random.randint(keys[2], (K,), 1, 4).astype(jnp.float32)
    freq_z = jax.random.randint(keys[3], (K,), 1, 4).astype(jnp.float32)
    phase_x = jax.random.uniform(keys[4], (K,), jnp.float32)
    phase_y = jax.random.uniform(keys[5], (K,), jnp.float32)
    phase_z = jax.random.uniform(keys[6], (K,), jnp.float32)
    coord_x = jnp.arange(NX, dtype=jnp.float32)[:, None] / NX
    coord_y = jnp.arange(NY, dtype=jnp.float32)[:, None] / NY
    coord_z = jnp.arange(NZ, dtype=jnp.float32)[:, None] / NZ
    wave_x = jnp.cos(2.0 * jnp.pi * (coord_x * freq_x + phase_x))
    wave_y = jnp.cos(2.0 * jnp.pi * (coord_y * freq_y + phase_y))
    wave_z = jnp.cos(2.0 * jnp.pi * (coord_z * freq_z + phase_z))
    smooth = wave_x[:, None, None, :] * wave_y[None, :, None, :] * wave_z[None, None, :, :]
    return (rough + amplitude * smooth).astype(jnp.bfloat16)


def shard_levels(own_key, shape, cuts, low, top_value):
    factor_of = 1.0
    for dim, shards_of in cuts:
        heights = jax.random.uniform(jax.random.fold_in(jax.random.fold_in(own_key, 6), dim), (shards_of,), jnp.float32, low / len(cuts), top_value / len(cuts))
        factor_of = factor_of * jnp.repeat(jnp.exp(heights), shape[dim] // shards_of).reshape((-1,) + (1,) * (len(shape) - 1 - dim))
    return factor_of


def setup_inputs(seed: int = 0) -> dict:
    streams_of = jax.random.split(jax.random.key(seed), 3)
    eigvecs = draw_eigvecs(jax.random.fold_in(streams_of[2], 71), 0)
    material = jnp.clip(jnp.exp(math.log(2.0) - 1.3862944 * jax.random.uniform(streams_of[1], (2, NX, NY, NZ), jnp.float32) ** shard_levels(streams_of[1], (2, NX, NY, NZ), ((1, 4), (2, 16), (3, 2)), -0.2, 0.2)), 0.5, 2.0)
    return {"eigvecs": eigvecs, "material": material}


stencil_offsets = [(dx, dy, dz) for dx in (-1, 0, 1) for dy in (-1, 0, 1) for dz in (-1, 0, 1) if (dx, dy, dz) != (0, 0, 0)]


def coupling(offset):
    nonzero = sum(abs(entry) for entry in offset)
    return 0.25 * 0.5 ** (nonzero - 1)


def mass_weight(offset):
    weight = 1.0
    for entry in offset:
        weight = weight * (4.0 / 6.0 if entry == 0 else 1.0 / 6.0)
    return weight


def apply_operators(padded, padded_material):
    size_x = padded.shape[0] - 2
    size_y = padded.shape[1] - 2
    size_z = padded.shape[2] - 2
    centre = padded[1:-1, 1:-1, 1:-1].astype(jnp.float32)
    kappa_centre = padded_material[0, 1:-1, 1:-1, 1:-1]
    rho_centre = padded_material[1, 1:-1, 1:-1, 1:-1]
    stiff_sum = jnp.zeros(centre.shape, jnp.float32)
    mass_sum = mass_weight((0, 0, 0)) * rho_centre[..., None] * centre
    for offset in stencil_offsets:
        lower = (1 + offset[0], 1 + offset[1], 1 + offset[2])
        shifted = padded[lower[0]:lower[0] + size_x, lower[1]:lower[1] + size_y, lower[2]:lower[2] + size_z].astype(jnp.float32)
        kappa_side = padded_material[0, lower[0]:lower[0] + size_x, lower[1]:lower[1] + size_y, lower[2]:lower[2] + size_z]
        rho_side = padded_material[1, lower[0]:lower[0] + size_x, lower[1]:lower[1] + size_y, lower[2]:lower[2] + size_z]
        stiff_sum = stiff_sum + (coupling(offset) * 0.5 * (kappa_centre + kappa_side))[..., None] * (centre - shifted)
        mass_sum = mass_sum + (mass_weight(offset) * 0.5 * (rho_centre + rho_side))[..., None] * shifted
    return stiff_sum.astype(jnp.bfloat16), mass_sum.astype(jnp.bfloat16)


def reference(eigvecs, material):
    cells = NX * NY * NZ
    block_cols = 32
    padded_material = jnp.pad(material, ((0, 0), (1, 1), (1, 1), (1, 1)))
    flat_vectors = eigvecs.reshape(cells, K)

    def column_block(block_index):
        first_col = block_index * block_cols
        col_block = lax.dynamic_slice_in_dim(eigvecs, first_col, block_cols, 3)
        padded = jnp.pad(col_block, ((1, 1), (1, 1), (1, 1), (0, 0)))
        stiff_vecs, mass_vecs = apply_operators(padded, padded_material)
        dims = (((0,), (0,)), ((), ()))
        stiff_cols = lax.dot_general(flat_vectors, stiff_vecs.reshape(cells, block_cols), dims, preferred_element_type=jnp.float32)
        mass_cols = lax.dot_general(flat_vectors, mass_vecs.reshape(cells, block_cols), dims, preferred_element_type=jnp.float32)
        return stiff_cols, mass_cols

    stiff_blocks, mass_blocks = lax.map(column_block, jnp.arange(K // block_cols, dtype=jnp.int32))
    stiffness = jnp.transpose(stiff_blocks, (1, 0, 2)).reshape(K, K) / cells
    mass_matrix = jnp.transpose(mass_blocks, (1, 0, 2)).reshape(K, K) / cells
    return stiffness, mass_matrix
```

```python
import functools
import numpy as np
import jax
import jax.numpy as jnp
from jax import lax
from jax.experimental import pallas as pl
from jax.experimental.pallas import tpu as pltpu
from jax.sharding import PartitionSpec as P


def upper(cells, axis, dim):
    count = lax.axis_size(axis)
    head = lax.slice_in_dim(cells, 0, 1, axis=dim)
    return lax.ppermute(head, axis, [(i + 1, i) for i in range(count - 1)])


def taps(count, middle):
    t = middle * np.eye(count) + np.eye(count, k=1) + np.eye(count, k=-1)
    t[-1, -1] = 0.0
    return t


def rows_of(size_y, size_z):
    order = np.zeros((size_y + 1, size_z + 1), np.int64)
    base = (size_y + 1) * size_z
    for y in range(size_y + 1):
        order[y, :size_z] = y * size_z + np.arange(size_z)
        order[y, size_z] = base + y
    order[size_y, size_z] = base + -(-size_y // 16) * 16
    return order


def plane_matrix(size_y, size_z, rows):
    order = rows_of(size_y, size_z).reshape(-1)
    blocks = []
    for middle in (2.0, 4.0):
        full = np.kron(taps(size_y + 1, middle), taps(size_z + 1, middle))
        block = np.zeros((rows, rows))
        block[np.ix_(order, order)] = full
        blocks.append(block)
    return np.concatenate(blocks, 0)


def coefficients(ext, rows, cells_shape):
    size_x, size_y, size_z = cells_shape
    kappa, rho = ext[0], ext[1]
    field = kappa
    for dim in range(3):
        n = field.shape[dim]
        pad = [(1, 1) if d == dim else (0, 0) for d in range(3)]
        wide = jnp.pad(field, pad)
        lower = lax.slice_in_dim(wide, 0, n, axis=dim)
        above = lax.slice_in_dim(wide, 2, n + 2, axis=dim)
        shape = [1, 1, 1]
        shape[dim] = n
        diag = jnp.asarray(np.r_[np.full(n - 1, 2.0), 0.0].reshape(shape), jnp.float32)
        field = lower + above + diag * field
    owned = np.zeros(kappa.shape, np.float32)
    owned[:size_x, :size_y, :size_z] = 2.0
    diag = owned * kappa + field * (1.0 / 32.0)
    parts = jnp.stack([diag, kappa * (1.0 / 16.0), rho * (1.0 / 216.0)], axis=1)
    main = parts[..., :size_z].reshape(size_x + 1, 3, (size_y + 1) * size_z)
    edge = parts[:, :, :size_y, size_z]
    edge = jnp.pad(edge, ((0, 0), (0, 0), (0, -size_y % 16)))
    both = jnp.concatenate([main, edge, parts[:, :, size_y:, size_z]], axis=2)
    return jnp.pad(both, ((0, 0), (0, 5), (0, rows - both.shape[2])))


OFFSETS = [(0, 1, 0), (0, 0, 1), (1, 0, 0), (0, 1, 1), (1, 0, 1), (1, 1, 0), (1, 1, 1)]
AXES = ("gx", "gy", "gz")


def inside(offset, sign):
    ok = None
    for axis, d in zip(AXES, offset):
        if d:
            at = lax.axis_index(axis)
            here = at > 0 if sign < 0 else at < lax.axis_size(axis) - 1
            ok = here if ok is None else jnp.logical_and(ok, here)
    return ok


def device_at(offset, sign):
    return {axis: lax.axis_index(axis) + sign * d for axis, d in zip(AXES, offset) if d}


def greet_around():
    barrier = pltpu.get_barrier_semaphore()
    total = jnp.int32(greet_reduction())
    for offset in OFFSETS:
        for sign in (-1, 1):
            there = inside(offset, sign)

            @pl.when(there)
            def _(offset=offset, sign=sign):
                pl.semaphore_signal(barrier, inc=1, device_id=device_at(offset, sign),
                                    device_id_type=pl.DeviceIdType.MESH)

            total = total + jnp.where(there, 1, 0)
    pl.semaphore_wait(barrier, total)


def kernel(scale, v_ref, z_ref, k_ref, t_ref, c_ref, stiff_out, mass_out, e_ref, corners, p0, p1, p2, p3, acc,
           own_sem, send, recv, y_send, y_recv, blocks, *reduce_bufs):
    slots = (p0, p1, p2, p3)
    rows, columns = e_ref.shape[1:]
    nx, owned, _ = v_ref.shape
    planes = nx + 1
    edge = z_ref.shape[1]
    width = rows - owned - edge - 16
    y_at, z_at, c_at = owned, owned + width, owned + width + edge
    own = pltpu.make_async_copy(v_ref, e_ref.at[:nx, :owned], own_sem)
    own.start()
    places = {
        (0, 1, 0): (v_ref.at[:, :width], e_ref.at[:nx, y_at:z_at]),
        (0, 0, 1): (z_ref, e_ref.at[:nx, z_at:c_at]),
        (0, 1, 1): (k_ref, corners.at[0]),
        (1, 0, 0): (v_ref.at[0], e_ref.at[nx, :owned]),
        (1, 0, 1): (z_ref.at[0], e_ref.at[nx, z_at:c_at]),
        (1, 1, 0): (v_ref.at[0, :width], e_ref.at[nx, y_at:z_at]),
        (1, 1, 1): (k_ref, corners.at[1]),
    }
    greet_around()
    copies = {}
    y_here, y_below = (0, 1, 0), device_at((0, 1, 0), -1)

    def chunk(i):
        four = pl.ds(4 * i, 4)
        return pltpu.make_async_remote_copy(
            src_ref=v_ref.at[four, :width], dst_ref=e_ref.at[four, y_at:z_at],
            send_sem=y_send.at[i], recv_sem=y_recv.at[i],
            device_id=y_below, device_id_type=pl.DeviceIdType.MESH)

    for n, offset in ((1, (0, 0, 1)), (3, (0, 1, 1)), (0, y_here), (2, (1, 0, 0)),
                      (4, (1, 0, 1)), (5, (1, 1, 0)), (6, (1, 1, 1))):
        if offset == y_here:
            for i in range(nx // 4):
                pl.when(inside(offset, -1))(chunk(i).start)
            continue
        src, dst = places[offset]
        copies[offset] = pltpu.make_async_remote_copy(
            src_ref=src, dst_ref=dst, send_sem=send.at[n], recv_sem=recv.at[n],
            device_id=device_at(offset, -1), device_id_type=pl.DeviceIdType.MESH)
        pl.when(inside(offset, -1))(copies[offset].start)
    for offset in OFFSETS:
        src, dst = places[offset]

        @pl.when(jnp.logical_not(inside(offset, 1)))
        def _(dst=dst):
            dst[...] = jnp.zeros(dst.shape, dst.dtype)

    own.wait()
    for offset in ((0, 0, 1), (0, 1, 1)):
        pl.when(inside(offset, 1))(copies[offset].wait_recv)
    pl.when(inside(y_here, 1))(chunk(0).wait_recv)

    def fill_corner(x, row):
        e_ref[x, c_at:] = jnp.broadcast_to(row.astype(jnp.float32), (16, columns)).astype(e_ref.dtype)

    for x in range(nx):
        fill_corner(x, corners[0, x:x + 1])

    def taps_of(x, slot):
        slots[slot % 4][...] = jnp.dot(t_ref[...], e_ref[x], preferred_element_type=jnp.float32)

    def step(x, slot, two, four, ahead):
        if ahead:
            taps_of(x + 2, slot + 2)
        before, now, after = (slots[(slot + k) % 4] for k in (3, 0, 1))
        coef = c_ref[x].T
        v = e_ref[x]
        stiff = before[:rows] + after[:rows] + two * now[:rows]
        yk = coef[:, 0:1] * v.astype(jnp.float32) - coef[:, 1:2] * stiff
        mass = before[rows:] + after[rows:] + four * now[rows:]
        ym = coef[:, 2:3] * mass
        dims = (((0,), (0,)), ((), ()))
        acc[:, :columns] += lax.dot_general(v, yk.astype(jnp.bfloat16), dims, preferred_element_type=jnp.float32)
        acc[:, columns:] += lax.dot_general(v, ym.astype(jnp.bfloat16), dims, preferred_element_type=jnp.float32)

    acc[...] = jnp.zeros_like(acc)
    e_ref[planes] = jnp.zeros((rows, columns), e_ref.dtype)
    p3[...] = jnp.zeros_like(p3)
    taps_of(0, 0)
    taps_of(1, 1)
    whole = (planes - 1) // 4

    def four_steps(i, carry):
        @pl.when(i < whole - 1)
        def _():
            pl.when(inside(y_here, 1))(chunk(i + 1).wait_recv)

        @pl.when(i == whole - 1)
        def _():
            for offset in OFFSETS:
                if offset[0]:
                    pl.when(inside(offset, 1))(copies[offset].wait_recv)
            fill_corner(nx, corners[1, 0:1])

        for j in range(4):
            step(4 * i + j, j, 2.0, 4.0, True)
        return carry

    lax.fori_loop(0, whole, four_steps, 0)
    for x in range(4 * whole, planes):
        last = x == planes - 1
        step(x, x, 0.0 if last else 2.0, 0.0 if last else 4.0, x + 2 <= planes)
    groups = columns // 128
    for g in range(groups):
        some = slice(g * 128, (g + 1) * 128)
        stiff = (acc[some, :columns] + acc[:, some].T) * scale
        mass = (acc[some, columns:] + acc[:, columns + g * 128:columns + (g + 1) * 128].T) * scale
        stiff = stiff.reshape(4, 4, 8, columns)
        mass = mass.reshape(4, 4, 8, columns)
        upper_rows = lax.broadcasted_iota(jnp.int32, stiff.shape, 2) < 4
        low = jnp.where(upper_rows, stiff, pltpu.roll(mass, 4, 2))
        high = jnp.where(upper_rows, pltpu.roll(stiff, 4, 2), mass)
        blocks[g // 2, g % 2, :, :, 0] = low
        blocks[g // 2, g % 2, :, :, 1] = high
    reduce_blocks(blocks, stiff_out, mass_out, reduce_bufs)
    for i in range(nx // 4):
        pl.when(inside(y_here, -1))(chunk(i).wait_send)
    for offset in OFFSETS:
        if offset != y_here:
            pl.when(inside(offset, -1))(copies[offset].wait_send)


def coordinates():
    gx, gy, gz = (lax.axis_index(a) for a in AXES)
    return gx // 2, gx % 2, gy // 4, gy % 4, gz


def places_along(axis):
    zl, core, cx, cy, zh = coordinates()
    count = 2 if axis == "core" else 4
    me = {"core": core, "x": cx, "y": cy, "z": zh * 2 + zl}[axis]
    found = []
    for k in range(1, count):
        peer = lax.rem(me + k, count)
        if axis == "core":
            device = {"gx": zl * 2 + peer}
        elif axis == "x":
            device = {"gy": peer * 4 + cy}
        elif axis == "y":
            device = {"gy": cx * 4 + peer}
        else:
            device = {"gx": (peer % 2) * 2 + core, "gz": peer // 2}
        found.append((peer, device))
    return found


def greet_reduction():
    barrier = pltpu.get_barrier_semaphore()
    total = 0
    for axis in ("core", "x", "y", "z"):
        for _, device in places_along(axis):
            pl.semaphore_signal(barrier, inc=1, device_id=device, device_id_type=pl.DeviceIdType.MESH)
            total += 1
    return total


def spread(axis, piece, landing, send, recv, base):
    copies = []
    for k, (peer, device) in enumerate(places_along(axis)):
        copy = pltpu.make_async_remote_copy(
            src_ref=piece(peer), dst_ref=landing.at[k],
            send_sem=send.at[base + k], recv_sem=recv.at[base + k],
            device_id=device, device_id_type=pl.DeviceIdType.MESH)
        copy.start()
        copies.append(copy)
    return copies


def gathered(copies, own, landing):
    for copy in copies:
        copy.wait_recv()
    held = own
    for k in range(len(copies)):
        held = held + landing[k]
    return held


def reduce_blocks(r, stiff_out, mass_out, bufs):
    zl, core, cx, cy, zh = coordinates()
    rc, ha, ra1, ha1, ra2, ha2, ra3, hb, rb1, hb1, rb2, hb2, rb3, send, recv = bufs
    half = r.shape[-1] // 2
    lanes = (slice(0, half), slice(half, 2 * half))
    count = 0

    def sems(n):
        nonlocal count
        count += n
        return send, recv, count - n

    first = [spread("core", lambda p, c=c: r.at[:, p, :, :, :, :, c], rc.at[i], *sems(1))
             for i, c in enumerate(lanes)]
    ha[...] = gathered(first[0], r[:, core, :, :, :, :, lanes[0]], rc.at[0])
    a1 = spread("x", lambda p: ha.at[:, p], ra1, *sems(3))
    hb[...] = gathered(first[1], r[:, core, :, :, :, :, lanes[1]], rc.at[1])
    b1 = spread("z", lambda p: hb.at[p % 2, :, :, p // 2], rb1, *sems(3))
    ha1[...] = gathered(a1, ha[:, cx], ra1)
    a2 = spread("y", lambda p: ha1.at[:, p], ra2, *sems(3))
    hb1[...] = gathered(b1, hb[zl, :, :, zh], rb1)
    b2 = spread("x", lambda p: hb1.at[p], rb2, *sems(3))
    ha2[...] = gathered(a2, ha1[:, cy], ra2)
    a3 = spread("z", lambda p: ha2.at[p % 2, p // 2], ra3, *sems(3))
    hb2[...] = gathered(b2, hb1[cx], rb2)
    b3 = spread("y", lambda p: hb2.at[p], rb3, *sems(3))
    done = gathered(a3, ha2[zl, zh], ra3)
    stiff_out[:, :half] = done[:4]
    mass_out[:, :half] = done[4:]
    done = gathered(b3, hb2[cy], rb3)
    stiff_out[:, half:] = done[:4]
    mass_out[:, half:] = done[4:]
    for copy in first[0] + first[1] + a1 + b1 + a2 + b2 + a3 + b3:
        copy.wait_send()


def reduce_scratch(columns):
    half = columns // 2
    f32 = jnp.float32
    shapes = [(2, 1, 2, 4, 4, 2, 8, half),
              (2, 4, 4, 2, 8, half), (3, 2, 4, 2, 8, half), (2, 4, 2, 8, half), (3, 2, 2, 8, half),
              (2, 2, 8, half), (3, 8, half),
              (2, 4, 4, 2, 8, half), (3, 4, 4, 8, half), (4, 4, 8, half), (3, 4, 8, half),
              (4, 8, half), (3, 8, half)]
    return [pltpu.VMEM(shape, f32) for shape in shapes] + [pltpu.SemaphoreType.DMA((20,))] * 2


def per_device(eigvecs, material):
    size_x, size_y, size_z, columns = eigvecs.shape
    axes = ("gx", "gy", "gz")
    devices_all = 1
    for axis in axes:
        devices_all *= lax.axis_size(axis)
    total_cells = size_x * size_y * size_z * devices_all
    ext = material
    for axis, dim in (("gz", 3), ("gy", 2), ("gx", 1)):
        ext = jnp.concatenate([ext, upper(ext, axis, dim)], axis=dim)
    edge = -(-size_y // 16) * 16
    rows = (size_y + 1) * size_z + edge + 16
    coef = coefficients(ext, rows, (size_x, size_y, size_z))
    z_layer = jnp.pad(eigvecs[:, :, 0], ((0, 0), (0, edge - size_y), (0, 0)))
    corner = eigvecs[:, 0, 0]
    matrix = jnp.asarray(plane_matrix(size_y, size_z, rows), jnp.bfloat16)
    vmem = pl.BlockSpec(memory_space=pltpu.VMEM)
    anywhere = pl.BlockSpec(memory_space=pl.ANY)
    return tuple(pl.pallas_call(
        functools.partial(kernel, 0.5 / total_cells),
        out_shape=[jax.ShapeDtypeStruct((4, columns), jnp.float32)] * 2,
        in_specs=[anywhere, vmem, vmem, vmem, vmem],
        out_specs=[vmem, vmem],
        scratch_shapes=[
            pltpu.VMEM((size_x + 2, rows, columns), eigvecs.dtype),
            pltpu.VMEM((2, size_x, columns), eigvecs.dtype),
        ] + [pltpu.VMEM((2 * rows, columns), jnp.float32)] * 4 + [
            pltpu.VMEM((columns, 2 * columns), jnp.float32),
            pltpu.SemaphoreType.DMA,
            pltpu.SemaphoreType.DMA((7,)),
            pltpu.SemaphoreType.DMA((7,)),
            pltpu.SemaphoreType.DMA((size_x // 4,)),
            pltpu.SemaphoreType.DMA((size_x // 4,)),
            pltpu.VMEM((2, 2, 4, 4, 2, 8, columns), jnp.float32),
        ] + reduce_scratch(columns),
        compiler_params=pltpu.CompilerParams(
            vmem_limit_bytes=60 * 1024 * 1024, collective_id=0, has_side_effects=True),
    )(eigvecs.reshape(size_x, size_y * size_z, columns), z_layer, corner, matrix, coef))


def solution(mesh):
    return jax.shard_map(
        per_device,
        mesh=mesh,
        in_specs=(P("gx", "gy", "gz", None), P(None, "gx", "gy", "gz")),
        out_specs=(P(("gx", "gy", "gz"), None), P(("gx", "gy", "gz"), None)),
        check_vma=False,
    )
```

```python
import functools
import numpy as np
import jax
import jax.numpy as jnp
from jax import lax
from jax.experimental import pallas as pl
from jax.experimental.pallas import tpu as pltpu
from jax.sharding import PartitionSpec as P

AXES = ("gx", "gy", "gz")
MESH = pl.DeviceIdType.MESH
NEAR = [(a, b, c) for c in (0, 1) for a in (-1, 0, 1) for b in (-1, 0, 1) if (a, b, c) != (0, 0, 0)]
STEP = 2


def weight(distance, middle):
    return {0: middle, 1: 1.0}.get(abs(distance), 0.0)


def own_row(y, size_y, size_z):
    half = size_y // 2
    if y < half:
        return size_z * (y + 1)
    return size_z * (half + 1) + 16 + size_z * (y - half)


def plane_taps(size_y, size_z):
    half = size_y // 2
    block = size_z * (half + 1) + 16
    taps = np.zeros((2, 2, size_y * size_z, 2 * block), np.float32)
    for side in range(2):
        edge = size_z - 1 if side == 0 else 0
        for n, middle in enumerate((2.0, 4.0)):
            line = np.array([[weight(z - o, middle) for z in range(size_z)] for o in range(size_z)])
            for y in range(size_y):
                rows = slice(y * size_z, (y + 1) * size_z)
                for near in (y - 1, y, y + 1):
                    w = weight(near - y, middle)
                    if near < 0:
                        first = 0
                    else:
                        first = own_row(near, size_y, size_z)
                    taps[side, n, rows, first:first + size_z] = w * line
                    column = near if 0 <= near < size_y else (size_y if near < 0 else size_y + 1)
                    base = (block if near < half else 2 * block) - 16
                    taps[side, n, y * size_z + edge, base + column] = w
    return taps


def material_taps(size_x, size_y):
    cells = size_x * size_y
    places = [(x, y) for x in range(size_x) for y in range(size_y)]
    places += [(x, y) for x in (-1, size_x) for y in range(size_y)]
    places += [(x, y) for y in (-1, size_y) for x in range(size_x)]
    for x in (-1, size_x):
        for y in (-1, size_y):
            places += [(x, y) if n == (7 if x < 0 else 0) else None for n in range(8)]
    rows = -(-len(places) // 128) * 128
    taps = np.zeros((rows, cells), np.float32)
    for row, place in enumerate(places):
        if place is None:
            continue
        for x in range(size_x):
            for y in range(size_y):
                taps[row, x * size_y + y] = weight(x - place[0], 2.0) * weight(y - place[1], 2.0)
    return taps


def inside(a, b):
    gx, gy = lax.axis_index("gx"), lax.axis_index("gy")
    ok = None
    for at, d, count in ((gx, a, lax.axis_size("gx")), (gy, b, lax.axis_size("gy"))):
        if d:
            here = at > 0 if d < 0 else at < count - 1
            ok = here if ok is None else jnp.logical_and(ok, here)
    return ok


def when(condition):
    return (lambda f: f()) if condition is None else pl.when(condition)


def device_at(a, b, c):
    device = {}
    if a:
        device["gx"] = lax.axis_index("gx") + a
    if b:
        device["gy"] = lax.axis_index("gy") + b
    if c:
        device["gz"] = 1 - lax.axis_index("gz")
    return device


def greet_around():
    barrier = pltpu.get_barrier_semaphore()
    total = jnp.int32(greet_reduction())
    for a, b, c in NEAR:
        there = inside(a, b)

        @when(there)
        def _(a=a, b=b, c=c):
            pl.semaphore_signal(barrier, inc=1, device_id=device_at(a, b, c), device_id_type=MESH)

        total = total + (1 if there is None else jnp.where(there, 1, 0))
    return total


class Halo:
    def __init__(self, send, recv):
        self.send, self.recv, self.count, self.all = send, recv, 0, []

    def add(self, side, src, dst):
        a, b, c = side
        copy = pltpu.make_async_remote_copy(
            src_ref=src, dst_ref=dst, send_sem=self.send.at[self.count], recv_sem=self.recv.at[self.count],
            device_id=device_at(-a, -b, c), device_id_type=MESH)
        self.count += 1
        entry = (copy, inside(-a, -b), inside(a, b))
        self.all.append(entry)
        return entry

    def finish(self):
        for copy, sends, _ in self.all:
            when(sends)(copy.wait_send)


def begin(entries):
    for copy, sends, _ in entries:
        when(sends)(copy.start)


def arrive(entries):
    for copy, _, receives in entries:
        when(receives)(copy.wait_recv)


def zero_unless(condition, refs):
    if condition is None:
        return

    @pl.when(jnp.logical_not(condition))
    def _():
        for ref in refs:
            ref[...] = jnp.zeros(ref.shape, ref.dtype)


def kernel(scale, sizes, v_ref, m_ref, t_hbm, w_ref, stiff_out, mass_out,
           e, t, zl, zn, cz, cn, zx, cx, faces, kall, coef, u, ybuf, acc, blocks,
           own_sem, v_send, v_recv, k_send, k_recv, *reduce_bufs):
    nx, ny, nz = sizes
    columns = e.shape[2]
    gz = lax.axis_index("gz")
    hy = ny // 2 * nz
    block = nz + hy + 16
    cells = nx * ny
    low, high = pl.ds(nz, hy), pl.ds(block, hy)
    own = [pltpu.make_async_copy(v_ref.at[:, :hy], e.at[pl.ds(1, nx), low], own_sem.at[0]),
           pltpu.make_async_copy(v_ref.at[:, hy:], e.at[pl.ds(1, nx), high], own_sem.at[1]),
           pltpu.make_async_copy(t_hbm.at[gz], t, own_sem.at[2])]
    for copy in own:
        copy.start()
    total = greet_around()

    kappa = m_ref[0]
    for n, y in enumerate((0, ny - 1)):
        faces[n] = jnp.concatenate([kappa[x * ny + y:x * ny + y + 1] for x in range(nx)], 0)
    kall[0, :cells] = kappa

    row = lax.broadcasted_iota(jnp.int32, (nz, nz), 0)
    col = lax.broadcasted_iota(jnp.int32, (nz, nz), 1)
    exact = functools.partial(lax.dot_general, dimension_numbers=(((1,), (1,)), ((), ())),
                              precision=lax.Precision.HIGHEST, preferred_element_type=jnp.float32)
    unit = jnp.where(row == col, 1.0, 0.0)

    def fill_coefficients(n, field):
        for x in range(nx):
            for y in range(ny):
                at = x * ny + y
                coef[n, x, y * nz:(y + 1) * nz] = jnp.broadcast_to(field[:, at:at + 1], (nz, 128))

    flipped = exact(unit, kappa)
    fill_coefficients(1, flipped * (1.0 / 16.0))
    fill_coefficients(2, exact(unit, m_ref[1]) * (1.0 / 216.0))

    pl.semaphore_wait(pltpu.get_barrier_semaphore(), total)

    kh = Halo(k_send, k_recv)
    x_tile = {-1: pl.ds(cells - ny, ny), 1: pl.ds(0, ny)}
    f_tile = {-1: pl.ds(nx - 8, 8), 1: pl.ds(0, 8)}
    which = {-1: 0, 1: 1}
    y_face = {-1: 1, 1: 0}
    for a, b, c in NEAR:
        if (a, b) == (0, 0):
            src, at, n = m_ref.at[0], 0, cells
        elif b == 0:
            src, at, n = m_ref.at[0, x_tile[a]], cells + which[a] * ny, ny
        elif a == 0:
            src, at, n = faces.at[y_face[b]], cells + 2 * ny + which[b] * nx, nx
        else:
            src = faces.at[y_face[b], f_tile[a]]
            at, n = cells + 2 * ny + 2 * nx + 8 * (2 * which[a] + which[b]), 8
        dst = kall.at[c, pl.ds(at, n)]
        begin([kh.add((a, b, c), src, dst)])
        zero_unless(inside(a, b), [dst])
    used = cells + 2 * ny + 2 * nx + 32
    for c in range(2):
        kall[c, used:] = jnp.zeros((kall.shape[1] - used, nz), jnp.float32)

    vh = Halo(v_send, v_recv)
    steps = nx // STEP
    waits = [[] for _ in range(steps)]
    y_src = {-1: pl.ds((ny - 1) * nz, nz), 1: pl.ds(0, nz)}
    y_dst = {-1: pl.ds(0, nz), 1: pl.ds(block + hy, nz)}
    x_src = {-1: nx - 1, 1: 0}
    x_dst = {-1: 0, 1: nx + 1}

    def y_chunk(i):
        first = 0 if i == 0 else STEP * i + 1
        last = min(STEP * (i + 1) + 1, nx)
        made = [vh.add((0, b, 0), v_ref.at[pl.ds(first, last - first), y_src[b]],
                       e.at[pl.ds(first + 1, last - first), y_dst[b]]) for b in (-1, 1)]
        waits[i].extend(made)
        begin(made)

    def x_plane(a):
        made = [vh.add((a, 0, 0), v_ref.at[x_src[a], pl.ds(0, hy)], e.at[x_dst[a], low]),
                vh.add((a, 0, 0), v_ref.at[x_src[a], pl.ds(hy, hy)], e.at[x_dst[a], high])]
        made += [vh.add((a, b, 0), v_ref.at[x_src[a], y_src[b]], e.at[x_dst[a], y_dst[b]]) for b in (-1, 1)]
        waits[0 if a < 0 else steps - 1].extend(made)
        begin(made)

    y_chunk(0)
    x_plane(-1)
    for i in range(1, steps):
        y_chunk(i)
    for b in (-1, 1):
        zero_unless(inside(0, b), [e.at[pl.ds(1, nx), y_dst[b]]])
    for a in (-1, 1):
        zero_unless(inside(a, 0), [e.at[x_dst[a], low], e.at[x_dst[a], high], zx.at[which[a]]])
        for b in (-1, 1):
            zero_unless(inside(a, b), [e.at[x_dst[a], y_dst[b]], cx.at[which[a], which[b]]])
    for b in (-1, 1):
        zero_unless(inside(0, b), [cn.at[which[b]]])
    acc[...] = jnp.zeros_like(acc)

    own[0].wait()
    own[1].wait()

    def edge_row(x, y, z):
        at = own_row(y, ny, nz) + z
        first = at // 16 * 16
        return e[x + 1, first:first + 16].astype(jnp.float32)[at - first:at - first + 1]

    def extract(z):
        for q in range(nx // 2):
            rows = [edge_row(2 * q + n // ny, n % ny, z) for n in range(2 * ny)]
            zl[q] = jnp.concatenate(rows, 0).astype(zl.dtype)
        for n, y in enumerate((0, ny - 1)):
            cz[n] = jnp.concatenate([edge_row(x, y, z) for x in range(nx)], 0).astype(cz.dtype)

    pl.when(gz == 0)(functools.partial(extract, nz - 1))
    pl.when(gz == 1)(functools.partial(extract, 0))

    def z_chunk(i):
        first, last = (0, 2) if i == 0 else (i + 1, i + 2)
        made = [vh.add((0, 0, 1), zl.at[pl.ds(first, last - first)], zn.at[pl.ds(first, last - first)])]
        waits[i].extend(made)
        begin(made)

    def z_corners(a):
        if a == 0:
            made = [vh.add((0, b, 1), cz.at[y_face[b]], cn.at[which[b]]) for b in (-1, 1)]
        else:
            made = [vh.add((a, 0, 1), zl.at[nx // 2 - 1 if a < 0 else 0], zx.at[which[a]])]
            made += [vh.add((a, b, 1), cz.at[y_face[b]], cx.at[which[a], which[b]]) for b in (-1, 1)]
        waits[0 if a <= 0 else steps - 1].extend(made)
        begin(made)

    z_chunk(0)
    z_corners(0)
    z_corners(-1)
    for i in range(1, steps - 1):
        z_chunk(i)
    z_corners(1)
    x_plane(1)

    arrive(kh.all)
    edge_from = jnp.where(gz == 0, nz - 1, 0)
    near_z = jnp.where(jnp.abs(row - col) == 1, 1.0, 0.0) + 2.0 * unit
    across = jnp.where(jnp.logical_and(row == edge_from, col == nz - 1 - edge_from), 1.0, 0.0)
    along_z = exact(near_z, kall[0]) + exact(across, kall[1])
    field = lax.dot_general(along_z, w_ref[...], (((1,), (0,)), ((), ())),
                            precision=lax.Precision.HIGHEST, preferred_element_type=jnp.float32)
    fill_coefficients(0, 2.0 * flipped + (1.0 / 32.0) * field)
    own[2].wait()

    lane = lax.broadcasted_iota(jnp.int32, (8, columns), 0)

    def fill_edge(x):
        if x < 0:
            z8 = zx[0].astype(jnp.float32)[8:]
            corners = [cx[0, n].astype(jnp.float32)[nx - 1:] for n in range(2)]
        elif x == nx:
            z8 = zx[1].astype(jnp.float32)[:8]
            corners = [cx[1, n].astype(jnp.float32)[:1] for n in range(2)]
        else:
            z8 = zn[x // 2].astype(jnp.float32)[8 * (x % 2):8 * (x % 2) + 8]
            corners = [cn[n].astype(jnp.float32)[x:x + 1] for n in range(2)]
        c8 = jnp.where(lane == 0, corners[0], jnp.where(lane == 1, corners[1], 0.0))
        full = jnp.concatenate([z8, c8], 0).astype(e.dtype)
        e[x + 1, block - 16:block] = full
        e[x + 1, 2 * block - 16:] = full

    def taps_of(n, slot):
        cut = hy - nz
        one = jnp.dot(t[n, :cut, :block], u[slot, n, :block], preferred_element_type=jnp.float32)
        two = jnp.dot(t[n, cut:cut + 2 * nz], u[slot, n], preferred_element_type=jnp.float32)
        three = jnp.dot(t[n, cut + 2 * nz:, block:], u[slot, n, block:], preferred_element_type=jnp.float32)
        return jnp.concatenate([one, two, three], 0)

    def spread_lanes(c):
        return jnp.concatenate([c] * (columns // 128), 1)

    def iteration(i, carry):
        for c in range(steps):
            @pl.when(i == c)
            def _(c=c):
                arrive(waits[c])
                first = -1 if c == 0 else STEP * c + 1
                for x in range(first, STEP * (c + 1) + 1):
                    fill_edge(x)

        held = []
        for j in range(STEP):
            x = STEP * i + j
            here = e[x + 1]
            twice = here + here
            two = e[x] + e[x + 2] + twice
            u[j, 0] = two
            u[j, 1] = two + twice
            v = jnp.concatenate([here[nz:nz + hy], here[block:block + hy]], 0)
            held.append(v)
            rows = slice(j * ny * nz, (j + 1) * ny * nz)
            stiff = spread_lanes(coef[0, x]) * v.astype(jnp.float32) - spread_lanes(coef[1, x]) * taps_of(0, j)
            ybuf[rows, :columns] = stiff.astype(ybuf.dtype)
            mass = spread_lanes(coef[2, x]) * taps_of(1, j)
            ybuf[rows, columns:] = mass.astype(ybuf.dtype)
        acc[...] += lax.dot_general(jnp.concatenate(held, 0), ybuf[...], (((0,), (0,)), ((), ())),
                                    preferred_element_type=jnp.float32)
        return carry

    lax.fori_loop(0, steps, iteration, 0)

    for g in range(columns // 128):
        some = slice(g * 128, (g + 1) * 128)
        stiff = (acc[some, :columns] + acc[:, some].T) * scale
        mass = (acc[some, columns:] + acc[:, columns + g * 128:columns + (g + 1) * 128].T) * scale
        stiff = stiff.reshape(4, 4, 8, columns)
        mass = mass.reshape(4, 4, 8, columns)
        upper_rows = lax.broadcasted_iota(jnp.int32, stiff.shape, 2) < 4
        blocks[g // 2, g % 2, :, :, 0] = jnp.where(upper_rows, stiff, pltpu.roll(mass, 4, 2))
        blocks[g // 2, g % 2, :, :, 1] = jnp.where(upper_rows, pltpu.roll(stiff, 4, 2), mass)
    reduce_blocks(blocks, stiff_out, mass_out, reduce_bufs)
    kh.finish()
    vh.finish()


def coordinates():
    gx, gy, gz = (lax.axis_index(a) for a in AXES)
    return gx // 2, gx % 2, gy // 4, gy % 4, gz


def places_along(axis):
    zl, core, cx, cy, zh = coordinates()
    count = 2 if axis == "core" else 4
    me = {"core": core, "x": cx, "y": cy, "z": zh * 2 + zl}[axis]
    found = []
    for k in range(1, count):
        peer = lax.rem(me + k, count)
        if axis == "core":
            device = {"gx": zl * 2 + peer}
        elif axis == "x":
            device = {"gy": peer * 4 + cy}
        elif axis == "y":
            device = {"gy": cx * 4 + peer}
        else:
            device = {"gx": (peer % 2) * 2 + core, "gz": peer // 2}
        found.append((peer, device))
    return found


def greet_reduction():
    barrier = pltpu.get_barrier_semaphore()
    total = 0
    for axis in ("core", "x", "y", "z"):
        for _, device in places_along(axis):
            pl.semaphore_signal(barrier, inc=1, device_id=device, device_id_type=pl.DeviceIdType.MESH)
            total += 1
    return total


def spread(axis, piece, landing, send, recv, base):
    copies = []
    for k, (peer, device) in enumerate(places_along(axis)):
        copy = pltpu.make_async_remote_copy(
            src_ref=piece(peer), dst_ref=landing.at[k],
            send_sem=send.at[base + k], recv_sem=recv.at[base + k],
            device_id=device, device_id_type=pl.DeviceIdType.MESH)
        copy.start()
        copies.append(copy)
    return copies


def gathered(copies, own, landing):
    for copy in copies:
        copy.wait_recv()
    held = own
    for k in range(len(copies)):
        held = held + landing[k]
    return held


def reduce_blocks(r, stiff_out, mass_out, bufs):
    zl, core, cx, cy, zh = coordinates()
    rc, ha, ra1, ha1, ra2, ha2, ra3, hb, rb1, hb1, rb2, hb2, rb3, send, recv = bufs
    half = r.shape[-1] // 2
    lanes = (slice(0, half), slice(half, 2 * half))
    count = 0

    def sems(n):
        nonlocal count
        count += n
        return send, recv, count - n

    first = [spread("core", lambda p, c=c: r.at[:, p, :, :, :, :, c], rc.at[i], *sems(1))
             for i, c in enumerate(lanes)]
    ha[...] = gathered(first[0], r[:, core, :, :, :, :, lanes[0]], rc.at[0])
    a1 = spread("x", lambda p: ha.at[:, p], ra1, *sems(3))
    hb[...] = gathered(first[1], r[:, core, :, :, :, :, lanes[1]], rc.at[1])
    b1 = spread("z", lambda p: hb.at[p % 2, :, :, p // 2], rb1, *sems(3))
    ha1[...] = gathered(a1, ha[:, cx], ra1)
    a2 = spread("y", lambda p: ha1.at[:, p], ra2, *sems(3))
    hb1[...] = gathered(b1, hb[zl, :, :, zh], rb1)
    b2 = spread("x", lambda p: hb1.at[p], rb2, *sems(3))
    ha2[...] = gathered(a2, ha1[:, cy], ra2)
    a3 = spread("z", lambda p: ha2.at[p % 2, p // 2], ra3, *sems(3))
    hb2[...] = gathered(b2, hb1[cx], rb2)
    b3 = spread("y", lambda p: hb2.at[p], rb3, *sems(3))
    done = gathered(a3, ha2[zl, zh], ra3)
    stiff_out[:, :half] = done[:4]
    mass_out[:, :half] = done[4:]
    done = gathered(b3, hb2[cy], rb3)
    stiff_out[:, half:] = done[:4]
    mass_out[:, half:] = done[4:]
    for copy in first[0] + first[1] + a1 + b1 + a2 + b2 + a3 + b3:
        copy.wait_send()


def reduce_scratch(columns):
    half = columns // 2
    f32 = jnp.float32
    shapes = [(2, 1, 2, 4, 4, 2, 8, half),
              (2, 4, 4, 2, 8, half), (3, 2, 4, 2, 8, half), (2, 4, 2, 8, half), (3, 2, 2, 8, half),
              (2, 2, 8, half), (3, 8, half),
              (2, 4, 4, 2, 8, half), (3, 4, 4, 8, half), (4, 4, 8, half), (3, 4, 8, half),
              (4, 8, half), (3, 8, half)]
    return [pltpu.VMEM(shape, f32) for shape in shapes] + [pltpu.SemaphoreType.DMA((20,))] * 2


def per_device(eigvecs, material):
    nx, ny, nz, columns = eigvecs.shape
    total_cells = nx * ny * nz
    for axis in AXES:
        total_cells *= lax.axis_size(axis)
    hy = ny // 2 * nz
    block = nz + hy + 16
    cells = nx * ny
    taps = jnp.asarray(plane_taps(ny, nz), jnp.bfloat16)
    around = jnp.asarray(material_taps(nx, ny), jnp.float32)
    bf16, f32 = jnp.bfloat16, jnp.float32
    dma = pltpu.SemaphoreType.DMA
    vmem = pl.BlockSpec(memory_space=pltpu.VMEM)
    anywhere = pl.BlockSpec(memory_space=pl.ANY)
    scratch = [
        pltpu.VMEM((nx + 2, 2 * block, columns), bf16),
        pltpu.VMEM((2, ny * nz, 2 * block), bf16),
        pltpu.VMEM((nx // 2, 2 * ny, columns), bf16),
        pltpu.VMEM((nx // 2, 2 * ny, columns), bf16),
        pltpu.VMEM((2, nx, columns), bf16),
        pltpu.VMEM((2, nx, columns), bf16),
        pltpu.VMEM((2, 2 * ny, columns), bf16),
        pltpu.VMEM((2, 2, nx, columns), bf16),
        pltpu.VMEM((2, nx, nz), f32),
        pltpu.VMEM((2, around.shape[0], nz), f32),
        pltpu.VMEM((3, nx, ny * nz, 128), f32),
        pltpu.VMEM((STEP, 2, 2 * block, columns), bf16),
        pltpu.VMEM((STEP * ny * nz, 2 * columns), bf16),
        pltpu.VMEM((columns, 2 * columns), f32),
        pltpu.VMEM((2, 2, 4, 4, 2, 8, columns), f32),
        dma((3,)), dma((48,)), dma((48,)), dma((17,)), dma((17,)),
    ] + reduce_scratch(columns)
    return tuple(pl.pallas_call(
        functools.partial(kernel, 0.5 / total_cells, (nx, ny, nz)),
        out_shape=[jax.ShapeDtypeStruct((4, columns), f32)] * 2,
        in_specs=[anywhere, vmem, anywhere, vmem],
        out_specs=[vmem, vmem],
        scratch_shapes=scratch,
        compiler_params=pltpu.CompilerParams(
            vmem_limit_bytes=60 * 1024 * 1024, collective_id=0, has_side_effects=True),
    )(eigvecs.reshape(nx, ny * nz, columns), material.reshape(2, cells, nz), taps, around))


def solution(mesh):
    return jax.shard_map(
        per_device,
        mesh=mesh,
        in_specs=(P("gx", "gy", "gz", None), P(None, "gx", "gy", "gz")),
        out_specs=(P(("gx", "gy", "gz"), None), P(("gx", "gy", "gz"), None)),
        check_vma=False,
    )
```

```python
import functools
import numpy as np
import jax
import jax.numpy as jnp
from jax import lax
from jax.experimental import pallas as pl
from jax.experimental.pallas import tpu as pltpu
from jax.sharding import PartitionSpec as P

AXES = ("gx", "gy", "gz")
MESH = pl.DeviceIdType.MESH
NEAR = [(a, b, c) for c in (0, 1) for a in (-1, 0, 1) for b in (-1, 0, 1) if (a, b, c) != (0, 0, 0)]
STEP = 2


def weight(distance, middle):
    return {0: middle, 1: 1.0}.get(abs(distance), 0.0)


def own_row(y, size_y, size_z):
    half = size_y // 2
    if y < half:
        return size_z * (y + 1)
    return size_z * (half + 1) + 16 + size_z * (y - half)


def plane_taps(size_y, size_z):
    half = size_y // 2
    block = size_z * (half + 1) + 16
    taps = np.zeros((2, 2, size_y * size_z, 2 * block), np.float32)
    for side in range(2):
        edge = size_z - 1 if side == 0 else 0
        for n, middle in enumerate((2.0, 4.0)):
            line = np.array([[weight(z - o, middle) for z in range(size_z)] for o in range(size_z)])
            for y in range(size_y):
                rows = slice(y * size_z, (y + 1) * size_z)
                for near in (y - 1, y, y + 1):
                    w = weight(near - y, middle)
                    if near < 0:
                        first = 0
                    else:
                        first = own_row(near, size_y, size_z)
                    taps[side, n, rows, first:first + size_z] = w * line
                    column = near if 0 <= near < size_y else (size_y if near < 0 else size_y + 1)
                    base = (block if near < half else 2 * block) - 16
                    taps[side, n, y * size_z + edge, base + column] = w
    return taps


def material_taps(size_x, size_y):
    cells = size_x * size_y
    places = [(x, y) for x in range(size_x) for y in range(size_y)]
    places += [(x, y) for x in (-1, size_x) for y in range(size_y)]
    places += [(x, y) for y in (-1, size_y) for x in range(size_x)]
    for x in (-1, size_x):
        for y in (-1, size_y):
            places += [(x, y) if n == (7 if x < 0 else 0) else None for n in range(8)]
    rows = -(-len(places) // 128) * 128
    taps = np.zeros((rows, cells), np.float32)
    for row, place in enumerate(places):
        if place is None:
            continue
        for x in range(size_x):
            for y in range(size_y):
                taps[row, x * size_y + y] = weight(x - place[0], 2.0) * weight(y - place[1], 2.0)
    return taps


def inside(a, b):
    gx, gy = lax.axis_index("gx"), lax.axis_index("gy")
    ok = None
    for at, d, count in ((gx, a, lax.axis_size("gx")), (gy, b, lax.axis_size("gy"))):
        if d:
            here = at > 0 if d < 0 else at < count - 1
            ok = here if ok is None else jnp.logical_and(ok, here)
    return ok


def when(condition):
    return (lambda f: f()) if condition is None else pl.when(condition)


def device_at(a, b, c):
    device = {}
    if a:
        device["gx"] = lax.axis_index("gx") + a
    if b:
        device["gy"] = lax.axis_index("gy") + b
    if c:
        device["gz"] = 1 - lax.axis_index("gz")
    return device


def greet_around():
    barrier = pltpu.get_barrier_semaphore()
    total = jnp.int32(greet_reduction())
    for a, b, c in NEAR:
        there = inside(a, b)

        @when(there)
        def _(a=a, b=b, c=c):
            pl.semaphore_signal(barrier, inc=1, device_id=device_at(a, b, c), device_id_type=MESH)

        total = total + (1 if there is None else jnp.where(there, 1, 0))
    return total


class Halo:
    def __init__(self, send, recv):
        self.send, self.recv, self.count, self.all = send, recv, 0, []

    def add(self, side, src, dst):
        a, b, c = side
        copy = pltpu.make_async_remote_copy(
            src_ref=src, dst_ref=dst, send_sem=self.send.at[self.count], recv_sem=self.recv.at[self.count],
            device_id=device_at(-a, -b, c), device_id_type=MESH)
        self.count += 1
        entry = (copy, inside(-a, -b), inside(a, b))
        self.all.append(entry)
        return entry

    def finish(self):
        for copy, sends, _ in self.all:
            when(sends)(copy.wait_send)


def begin(entries):
    for copy, sends, _ in entries:
        when(sends)(copy.start)


def arrive(entries):
    for copy, _, receives in entries:
        when(receives)(copy.wait_recv)


def zero_unless(condition, refs):
    if condition is None:
        return

    @pl.when(jnp.logical_not(condition))
    def _():
        for ref in refs:
            ref[...] = jnp.zeros(ref.shape, ref.dtype)


def kernel(scale, sizes, v_ref, m_ref, t_hbm, w_ref, out,
           e, t, ztile, zl, zn, cz, cn, zx, cx, faces, kall, coef, u, ybuf, acc, blocks,
           own_sem, v_send, v_recv, k_send, k_recv, *reduce_bufs):
    nx, ny, nz = sizes
    columns = e.shape[2]
    gz = lax.axis_index("gz")
    hy = ny // 2 * nz
    block = nz + hy + 16
    cells = nx * ny
    low, high = pl.ds(nz, hy), pl.ds(block, hy)
    own = [pltpu.make_async_copy(v_ref.at[:, :hy], e.at[pl.ds(1, nx), low], own_sem.at[0]),
           pltpu.make_async_copy(v_ref.at[:, hy:], e.at[pl.ds(1, nx), high], own_sem.at[1]),
           pltpu.make_async_copy(t_hbm.at[gz], t, own_sem.at[2])]
    z_first = pl.multiple_of((nz - 16) * (1 - gz), 16)
    tiles = [pltpu.make_async_copy(v_ref.at[:, pl.ds(y * nz + z_first, 16)], ztile.at[y], own_sem.at[3 + y])
             for y in range(ny)]
    for copy in tiles + own:
        copy.start()
    total = greet_around()

    kappa = m_ref[0]
    for n, y in enumerate((0, ny - 1)):
        faces[n] = jnp.concatenate([kappa[x * ny + y:x * ny + y + 1] for x in range(nx)], 0)
    kall[0, :cells] = kappa

    for copy in tiles:
        copy.wait()

    def extract(at):
        def edge_row(x, y):
            return ztile[y, x].astype(jnp.float32)[at:at + 1]

        for q in range(nx // 2):
            rows = [edge_row(2 * q + n // ny, n % ny) for n in range(2 * ny)]
            zl[q] = jnp.concatenate(rows, 0).astype(zl.dtype)
        for n, y in enumerate((0, ny - 1)):
            cz[n] = jnp.concatenate([edge_row(x, y) for x in range(nx)], 0).astype(cz.dtype)

    pl.when(gz == 0)(functools.partial(extract, 15))
    pl.when(gz == 1)(functools.partial(extract, 0))

    pl.semaphore_wait(pltpu.get_barrier_semaphore(), total)

    kh = Halo(k_send, k_recv)
    x_tile = {-1: pl.ds(cells - ny, ny), 1: pl.ds(0, ny)}
    f_tile = {-1: pl.ds(nx - 8, 8), 1: pl.ds(0, 8)}
    which = {-1: 0, 1: 1}
    y_face = {-1: 1, 1: 0}
    for a, b, c in NEAR:
        if (a, b) == (0, 0):
            src, at, n = m_ref.at[0], 0, cells
        elif b == 0:
            src, at, n = m_ref.at[0, x_tile[a]], cells + which[a] * ny, ny
        elif a == 0:
            src, at, n = faces.at[y_face[b]], cells + 2 * ny + which[b] * nx, nx
        else:
            src = faces.at[y_face[b], f_tile[a]]
            at, n = cells + 2 * ny + 2 * nx + 8 * (2 * which[a] + which[b]), 8
        dst = kall.at[c, pl.ds(at, n)]
        begin([kh.add((a, b, c), src, dst)])
        zero_unless(inside(a, b), [dst])
    used = cells + 2 * ny + 2 * nx + 32
    for c in range(2):
        kall[c, used:] = jnp.zeros((kall.shape[1] - used, nz), jnp.float32)

    vh = Halo(v_send, v_recv)
    steps = nx // STEP
    waits = [[] for _ in range(steps)]
    y_src = {-1: pl.ds((ny - 1) * nz, nz), 1: pl.ds(0, nz)}
    y_dst = {-1: pl.ds(0, nz), 1: pl.ds(block + hy, nz)}
    x_src = {-1: nx - 1, 1: 0}
    x_dst = {-1: 0, 1: nx + 1}

    def y_chunk(i):
        first = 0 if i == 0 else STEP * i + 1
        last = min(STEP * (i + 1) + 1, nx)
        made = [vh.add((0, b, 0), v_ref.at[pl.ds(first, last - first), y_src[b]],
                       e.at[pl.ds(first + 1, last - first), y_dst[b]]) for b in (-1, 1)]
        waits[i].extend(made)
        begin(made)

    def x_plane(a):
        made = [vh.add((a, 0, 0), v_ref.at[x_src[a], pl.ds(0, hy)], e.at[x_dst[a], low]),
                vh.add((a, 0, 0), v_ref.at[x_src[a], pl.ds(hy, hy)], e.at[x_dst[a], high])]
        made += [vh.add((a, b, 0), v_ref.at[x_src[a], y_src[b]], e.at[x_dst[a], y_dst[b]]) for b in (-1, 1)]
        waits[0 if a < 0 else steps - 1].extend(made)
        begin(made)

    def z_chunk(i):
        first, last = (0, 2) if i == 0 else (i + 1, i + 2)
        made = [vh.add((0, 0, 1), zl.at[pl.ds(first, last - first)], zn.at[pl.ds(first, last - first)])]
        waits[i].extend(made)
        begin(made)

    def z_corners(a):
        if a == 0:
            made = [vh.add((0, b, 1), cz.at[y_face[b]], cn.at[which[b]]) for b in (-1, 1)]
        else:
            made = [vh.add((a, 0, 1), zl.at[nx // 2 - 1 if a < 0 else 0], zx.at[which[a]])]
            made += [vh.add((a, b, 1), cz.at[y_face[b]], cx.at[which[a], which[b]]) for b in (-1, 1)]
        waits[0 if a <= 0 else steps - 1].extend(made)
        begin(made)

    z_chunk(0)
    z_corners(0)
    z_corners(-1)
    y_chunk(0)
    x_plane(-1)
    for i in range(1, steps - 1):
        z_chunk(i)
        y_chunk(i)
        if i == steps // 2:
            z_corners(1)
            x_plane(1)
    y_chunk(steps - 1)
    for b in (-1, 1):
        zero_unless(inside(0, b), [e.at[pl.ds(1, nx), y_dst[b]]])
    for a in (-1, 1):
        zero_unless(inside(a, 0), [e.at[x_dst[a], low], e.at[x_dst[a], high], zx.at[which[a]]])
        for b in (-1, 1):
            zero_unless(inside(a, b), [e.at[x_dst[a], y_dst[b]], cx.at[which[a], which[b]]])
    for b in (-1, 1):
        zero_unless(inside(0, b), [cn.at[which[b]]])
    acc[...] = jnp.zeros_like(acc)

    row = lax.broadcasted_iota(jnp.int32, (nz, nz), 0)
    col = lax.broadcasted_iota(jnp.int32, (nz, nz), 1)
    exact = functools.partial(lax.dot_general, dimension_numbers=(((1,), (1,)), ((), ())),
                              precision=lax.Precision.HIGHEST, preferred_element_type=jnp.float32)
    unit = jnp.where(row == col, 1.0, 0.0)

    def fill_coefficients(n, field):
        for x in range(nx):
            for y in range(ny):
                at = x * ny + y
                coef[n, x, y * nz:(y + 1) * nz] = jnp.broadcast_to(field[:, at:at + 1], (nz, 128))

    flipped = exact(unit, kappa)
    fill_coefficients(1, flipped * (1.0 / 16.0))
    fill_coefficients(2, exact(unit, m_ref[1]) * (1.0 / 216.0))

    arrive(kh.all)
    edge_from = jnp.where(gz == 0, nz - 1, 0)
    near_z = jnp.where(jnp.abs(row - col) == 1, 1.0, 0.0) + 2.0 * unit
    across = jnp.where(jnp.logical_and(row == edge_from, col == nz - 1 - edge_from), 1.0, 0.0)
    along_z = exact(near_z, kall[0]) + exact(across, kall[1])
    field = lax.dot_general(along_z, w_ref[...], (((1,), (0,)), ((), ())),
                            precision=lax.Precision.HIGHEST, preferred_element_type=jnp.float32)
    fill_coefficients(0, 2.0 * flipped + (1.0 / 32.0) * field)
    for copy in own:
        copy.wait()

    lane = lax.broadcasted_iota(jnp.int32, (8, columns), 0)

    def fill_edge(x):
        if x < 0:
            z8 = zx[0].astype(jnp.float32)[8:]
            corners = [cx[0, n].astype(jnp.float32)[nx - 1:] for n in range(2)]
        elif x == nx:
            z8 = zx[1].astype(jnp.float32)[:8]
            corners = [cx[1, n].astype(jnp.float32)[:1] for n in range(2)]
        else:
            z8 = zn[x // 2].astype(jnp.float32)[8 * (x % 2):8 * (x % 2) + 8]
            corners = [cn[n].astype(jnp.float32)[x:x + 1] for n in range(2)]
        c8 = jnp.where(lane == 0, corners[0], jnp.where(lane == 1, corners[1], 0.0))
        full = jnp.concatenate([z8, c8], 0).astype(e.dtype)
        e[x + 1, block - 16:block] = full
        e[x + 1, 2 * block - 16:] = full

    def taps_of(n, slot):
        cut = hy - nz
        one = jnp.dot(t[n, :cut, :block], u[slot, n, :block], preferred_element_type=jnp.float32)
        two = jnp.dot(t[n, cut:cut + 2 * nz], u[slot, n], preferred_element_type=jnp.float32)
        three = jnp.dot(t[n, cut + 2 * nz:, block:], u[slot, n, block:], preferred_element_type=jnp.float32)
        return jnp.concatenate([one, two, three], 0)

    def spread_lanes(c):
        return jnp.concatenate([c] * (columns // 128), 1)

    def iteration(i, carry):
        for c in range(steps):
            @pl.when(i == c)
            def _(c=c):
                arrive(waits[c])
                first = -1 if c == 0 else STEP * c + 1
                for x in range(first, STEP * (c + 1) + 1):
                    fill_edge(x)

        held = []
        for j in range(STEP):
            x = STEP * i + j
            here = e[x + 1]
            twice = here + here
            two = e[x] + e[x + 2] + twice
            u[j, 0] = two
            u[j, 1] = two + twice
            v = jnp.concatenate([here[nz:nz + hy], here[block:block + hy]], 0)
            held.append(v)
            rows = slice(j * ny * nz, (j + 1) * ny * nz)
            stiff = spread_lanes(coef[0, x]) * v.astype(jnp.float32) - spread_lanes(coef[1, x]) * taps_of(0, j)
            ybuf[rows, :columns] = stiff.astype(ybuf.dtype)
            mass = spread_lanes(coef[2, x]) * taps_of(1, j)
            ybuf[rows, columns:] = mass.astype(ybuf.dtype)
        acc[...] += lax.dot_general(jnp.concatenate(held, 0), ybuf[...], (((0,), (0,)), ((), ())),
                                    preferred_element_type=jnp.float32)
        return carry

    lax.fori_loop(0, steps, iteration, 0)

    for g in range(columns // 128):
        some = slice(g * 128, (g + 1) * 128)
        stiff = (acc[some, :columns] + acc[:, some].T) * scale
        mass = (acc[some, columns:] + acc[:, columns + g * 128:columns + (g + 1) * 128].T) * scale
        stiff = stiff.reshape(4, 4, 8, columns)
        mass = mass.reshape(4, 4, 8, columns)
        upper_rows = lax.broadcasted_iota(jnp.int32, stiff.shape, 2) < 4
        blocks[g // 2, g % 2, :, :, 0] = jnp.where(upper_rows, stiff, pltpu.roll(mass, 4, 2))
        blocks[g // 2, g % 2, :, :, 1] = jnp.where(upper_rows, pltpu.roll(stiff, 4, 2), mass)
    reduce_blocks(blocks, out, reduce_bufs)
    kh.finish()
    vh.finish()


def coordinates():
    gx, gy, gz = (lax.axis_index(a) for a in AXES)
    return gx // 2, gx % 2, gy // 4, gy % 4, gz


def places_along(axis):
    zl, core, cx, cy, zh = coordinates()
    count = 2 if axis == "core" else 4
    me = {"core": core, "x": cx, "y": cy, "z": zh * 2 + zl}[axis]
    found = []
    for k in range(1, count):
        peer = lax.rem(me + k, count)
        if axis == "core":
            device = {"gx": zl * 2 + peer}
        elif axis == "x":
            device = {"gy": peer * 4 + cy}
        elif axis == "y":
            device = {"gy": cx * 4 + peer}
        else:
            device = {"gx": (peer % 2) * 2 + core, "gz": peer // 2}
        found.append((peer, device))
    return found


def greet_reduction():
    barrier = pltpu.get_barrier_semaphore()
    total = 0
    for axis in ("core", "x", "y", "z"):
        for _, device in places_along(axis):
            pl.semaphore_signal(barrier, inc=1, device_id=device, device_id_type=pl.DeviceIdType.MESH)
            total += 1
    return total


def spread(axis, piece, landing, send, recv, base):
    copies = []
    for k, (peer, device) in enumerate(places_along(axis)):
        copy = pltpu.make_async_remote_copy(
            src_ref=piece(peer), dst_ref=landing.at[k],
            send_sem=send.at[base + k], recv_sem=recv.at[base + k],
            device_id=device, device_id_type=pl.DeviceIdType.MESH)
        copy.start()
        copies.append(copy)
    return copies


def gathered(copies, own, landing):
    for copy in copies:
        copy.wait_recv()
    held = own
    for k in range(len(copies)):
        held = held + landing[k]
    return held


def reduce_blocks(r, out, bufs):
    zl, core, cx, cy, zh = coordinates()
    rc, ha, ra1, ha1, ra2, ha2, ra3, hb, rb1, hb1, rb2, hb2, rb3, send, recv = bufs
    half = r.shape[-1] // 2
    lanes = (slice(0, half), slice(half, 2 * half))
    count = 0

    def sems(n):
        nonlocal count
        count += n
        return send, recv, count - n

    first = [spread("core", lambda p, c=c: r.at[:, p, :, :, :, :, c], rc.at[i], *sems(1))
             for i, c in enumerate(lanes)]
    ha[...] = gathered(first[0], r[:, core, :, :, :, :, lanes[0]], rc.at[0])
    a1 = spread("x", lambda p: ha.at[:, p], ra1, *sems(3))
    hb[...] = gathered(first[1], r[:, core, :, :, :, :, lanes[1]], rc.at[1])
    b1 = spread("z", lambda p: hb.at[p % 2, :, :, p // 2], rb1, *sems(3))
    ha1[...] = gathered(a1, ha[:, cx], ra1)
    a2 = spread("y", lambda p: ha1.at[:, p], ra2, *sems(3))
    hb1[...] = gathered(b1, hb[zl, :, :, zh], rb1)
    b2 = spread("x", lambda p: hb1.at[p], rb2, *sems(3))
    ha2[...] = gathered(a2, ha1[:, cy], ra2)
    a3 = spread("z", lambda p: ha2.at[p % 2, p // 2], ra3, *sems(3))
    hb2[...] = gathered(b2, hb1[cx], rb2)
    b3 = spread("y", lambda p: hb2.at[p], rb3, *sems(3))
    out[:, :half] = gathered(a3, ha2[zl, zh], ra3)
    out[:, half:] = gathered(b3, hb2[cy], rb3)
    for copy in first[0] + first[1] + a1 + b1 + a2 + b2 + a3 + b3:
        copy.wait_send()


def reduce_scratch(columns):
    half = columns // 2
    f32 = jnp.float32
    shapes = [(2, 1, 2, 4, 4, 2, 8, half),
              (2, 4, 4, 2, 8, half), (3, 2, 4, 2, 8, half), (2, 4, 2, 8, half), (3, 2, 2, 8, half),
              (2, 2, 8, half), (3, 8, half),
              (2, 4, 4, 2, 8, half), (3, 4, 4, 8, half), (4, 4, 8, half), (3, 4, 8, half),
              (4, 8, half), (3, 8, half)]
    return [pltpu.VMEM(shape, f32) for shape in shapes] + [pltpu.SemaphoreType.DMA((20,))] * 2


def per_device(eigvecs, material):
    nx, ny, nz, columns = eigvecs.shape
    total_cells = nx * ny * nz
    for axis in AXES:
        total_cells *= lax.axis_size(axis)
    hy = ny // 2 * nz
    block = nz + hy + 16
    cells = nx * ny
    taps = jnp.asarray(plane_taps(ny, nz), jnp.bfloat16)
    around = jnp.asarray(material_taps(nx, ny), jnp.float32)
    bf16, f32 = jnp.bfloat16, jnp.float32
    dma = pltpu.SemaphoreType.DMA
    vmem = pl.BlockSpec(memory_space=pltpu.VMEM)
    anywhere = pl.BlockSpec(memory_space=pl.ANY)
    scratch = [
        pltpu.VMEM((nx + 2, 2 * block, columns), bf16),
        pltpu.VMEM((2, ny * nz, 2 * block), bf16),
        pltpu.VMEM((ny, nx, 16, columns), bf16),
        pltpu.VMEM((nx // 2, 2 * ny, columns), bf16),
        pltpu.VMEM((nx // 2, 2 * ny, columns), bf16),
        pltpu.VMEM((2, nx, columns), bf16),
        pltpu.VMEM((2, nx, columns), bf16),
        pltpu.VMEM((2, 2 * ny, columns), bf16),
        pltpu.VMEM((2, 2, nx, columns), bf16),
        pltpu.VMEM((2, nx, nz), f32),
        pltpu.VMEM((2, around.shape[0], nz), f32),
        pltpu.VMEM((3, nx, ny * nz, 128), f32),
        pltpu.VMEM((STEP, 2, 2 * block, columns), bf16),
        pltpu.VMEM((STEP * ny * nz, 2 * columns), bf16),
        pltpu.VMEM((columns, 2 * columns), f32),
        pltpu.VMEM((2, 2, 4, 4, 2, 8, columns), f32),
        dma((3 + ny,)), dma((48,)), dma((48,)), dma((17,)), dma((17,)),
    ] + reduce_scratch(columns)
    both = pl.pallas_call(
        functools.partial(kernel, 0.5 / total_cells, (nx, ny, nz)),
        out_shape=jax.ShapeDtypeStruct((8, columns), f32),
        in_specs=[anywhere, vmem, anywhere, vmem],
        out_specs=vmem,
        scratch_shapes=scratch,
        compiler_params=pltpu.CompilerParams(
            vmem_limit_bytes=60 * 1024 * 1024, collective_id=0, has_side_effects=True),
    )(eigvecs.reshape(nx, ny * nz, columns), material.reshape(2, cells, nz), taps, around)
    return both[:4], both[4:]


def solution(mesh):
    return jax.shard_map(
        per_device,
        mesh=mesh,
        in_specs=(P("gx", "gy", "gz", None), P(None, "gx", "gy", "gz")),
        out_specs=(P(("gx", "gy", "gz"), None), P(("gx", "gy", "gz"), None)),
        check_vma=False,
    )
```

```python
import functools
import numpy as np
import jax
import jax.numpy as jnp
from jax import lax
from jax.experimental import pallas as pl
from jax.experimental.pallas import tpu as pltpu
from jax.sharding import PartitionSpec as P

AXES = ("gx", "gy", "gz")
MESH = pl.DeviceIdType.MESH
SIDES = [(0, -1, 0), (0, 1, 0), (0, 0, 1), (0, -1, 1), (0, 1, 1)]
NEAR = SIDES + [(-1, 0, 0), (1, 0, 0)]
STEP = 2


def weight(distance, middle):
    return {0: middle, 1: 1.0}.get(abs(distance), 0.0)


def own_row(y, size_y, size_z):
    half = size_y // 2
    if y < half:
        return size_z * (y + 1)
    return size_z * (half + 1) + 16 + size_z * (y - half)


def plane_taps(size_y, size_z):
    half = size_y // 2
    block = size_z * (half + 1) + 16
    taps = np.zeros((2, 2, size_y * size_z, 2 * block), np.float32)
    for side in range(2):
        edge = size_z - 1 if side == 0 else 0
        for n, middle in enumerate((2.0, 4.0)):
            line = np.array([[weight(z - o, middle) for z in range(size_z)] for o in range(size_z)])
            for y in range(size_y):
                rows = slice(y * size_z, (y + 1) * size_z)
                for near in (y - 1, y, y + 1):
                    w = weight(near - y, middle)
                    if near < 0:
                        first = 0
                    else:
                        first = own_row(near, size_y, size_z)
                    taps[side, n, rows, first:first + size_z] = w * line
                    column = near if 0 <= near < size_y else (size_y if near < 0 else size_y + 1)
                    base = (block if near < half else 2 * block) - 16
                    taps[side, n, y * size_z + edge, base + column] = w
    return taps


def material_taps(size_x, size_y):
    cells = size_x * size_y
    own = [(x, y) for x in range(size_x) for y in range(size_y)]
    faces = [(x, y) for y in (-1, size_y) for x in range(size_x)]
    rows = -(-(cells + 2 * size_x) // 128) * 128
    along_y = np.zeros((rows, cells), np.float32)
    for row, (near_x, near_y) in enumerate(own + faces):
        for col, (x, y) in enumerate(own):
            if x == near_x:
                along_y[row, col] = weight(y - near_y, 2.0)
    along_x = np.zeros((3, cells, cells), np.float32)
    for n, shift in enumerate((0, -size_x, size_x)):
        for row, (near_x, near_y) in enumerate(own):
            for col, (x, y) in enumerate(own):
                if y == near_y:
                    along_x[n, row, col] = weight(x - near_x - shift, 2.0)
    return np.concatenate([along_y, along_x.reshape(3 * cells, cells)], 0)


def inside(a, b):
    gx, gy = lax.axis_index("gx"), lax.axis_index("gy")
    ok = None
    for at, d, count in ((gx, a, lax.axis_size("gx")), (gy, b, lax.axis_size("gy"))):
        if d:
            here = at > 0 if d < 0 else at < count - 1
            ok = here if ok is None else jnp.logical_and(ok, here)
    return ok


def when(condition):
    return (lambda f: f()) if condition is None else pl.when(condition)


def device_at(a, b, c):
    device = {}
    if a:
        device["gx"] = lax.axis_index("gx") + a
    if b:
        device["gy"] = lax.axis_index("gy") + b
    if c:
        device["gz"] = 1 - lax.axis_index("gz")
    return device


def greet_around():
    barrier = pltpu.get_barrier_semaphore()
    total = jnp.int32(greet_reduction())
    for a, b, c in NEAR:
        there = inside(a, b)

        @when(there)
        def _(a=a, b=b, c=c):
            pl.semaphore_signal(barrier, inc=1, device_id=device_at(a, b, c), device_id_type=MESH)

        total = total + (1 if there is None else jnp.where(there, 1, 0))
    return total


class Halo:
    def __init__(self, send, recv):
        self.send, self.recv, self.count, self.all = send, recv, 0, []

    def add(self, side, src, dst):
        a, b, c = side
        copy = pltpu.make_async_remote_copy(
            src_ref=src, dst_ref=dst, send_sem=self.send.at[self.count], recv_sem=self.recv.at[self.count],
            device_id=device_at(-a, -b, c), device_id_type=MESH)
        self.count += 1
        entry = (copy, inside(-a, -b), inside(a, b))
        self.all.append(entry)
        return entry

    def finish(self):
        for copy, sends, _ in self.all:
            when(sends)(copy.wait_send)


def begin(entries):
    for copy, sends, _ in entries:
        when(sends)(copy.start)


def arrive(entries):
    for copy, _, receives in entries:
        when(receives)(copy.wait_recv)


def zero_unless(condition, refs):
    if condition is None:
        return

    @pl.when(jnp.logical_not(condition))
    def _():
        for ref in refs:
            ref[...] = jnp.zeros(ref.shape, ref.dtype)


def kernel(scale, sizes, v_ref, m_ref, t_hbm, w_ref, out,
           e, t, ztile, zl, zn, cz, cn, faces, kall, spans, coef, u, ybuf, acc, blocks,
           own_sem, v_send, v_recv, k_send, k_recv, *reduce_bufs):
    nx, ny, nz = sizes
    columns = e.shape[2]
    gz = lax.axis_index("gz")
    hy = ny // 2 * nz
    block = nz + hy + 16
    cells = nx * ny
    low, high = pl.ds(nz, hy), pl.ds(block, hy)
    own = [pltpu.make_async_copy(v_ref.at[:, :hy], e.at[pl.ds(1, nx), low], own_sem.at[0]),
           pltpu.make_async_copy(v_ref.at[:, hy:], e.at[pl.ds(1, nx), high], own_sem.at[1]),
           pltpu.make_async_copy(t_hbm.at[gz], t, own_sem.at[2])]
    z_first = pl.multiple_of((nz - 16) * (1 - gz), 16)
    tiles = [pltpu.make_async_copy(v_ref.at[:, pl.ds(y * nz + z_first, 16)], ztile.at[y], own_sem.at[3 + y])
             for y in range(ny)]
    for copy in tiles + own:
        copy.start()
    total = greet_around()

    kappa = m_ref[0]
    for n, y in enumerate((0, ny - 1)):
        faces[n] = jnp.concatenate([kappa[x * ny + y:x * ny + y + 1] for x in range(nx)], 0)
    kall[0, :cells] = kappa

    for copy in tiles:
        copy.wait()

    def extract(at):
        def edge_row(x, y):
            return ztile[y, x].astype(jnp.float32)[at:at + 1]

        for q in range(nx // 2):
            rows = [edge_row(2 * q + n // ny, n % ny) for n in range(2 * ny)]
            zl[q] = jnp.concatenate(rows, 0).astype(zl.dtype)
        for n, y in enumerate((0, ny - 1)):
            cz[n] = jnp.concatenate([edge_row(x, y) for x in range(nx)], 0).astype(cz.dtype)

    pl.when(gz == 0)(functools.partial(extract, 15))
    pl.when(gz == 1)(functools.partial(extract, 0))

    pl.semaphore_wait(pltpu.get_barrier_semaphore(), total)

    kh = Halo(k_send, k_recv)
    which = {-1: 0, 1: 1}
    y_face = {-1: 1, 1: 0}
    for a, b, c in SIDES:
        if b == 0:
            src, dst = m_ref.at[0], kall.at[c, pl.ds(0, cells)]
        else:
            src, dst = faces.at[y_face[b]], kall.at[c, pl.ds(cells + which[b] * nx, nx)]
        begin([kh.add((a, b, c), src, dst)])
        zero_unless(inside(a, b), [dst])
    used = cells + 2 * nx
    for c in range(2):
        kall[c, used:] = jnp.zeros((kall.shape[1] - used, nz), jnp.float32)

    vh = Halo(v_send, v_recv)
    steps = nx // STEP
    waits = [[] for _ in range(steps)]
    y_planes = [[(2 * i + 2, 2 * i + 4)] for i in range(steps - 1)] + [[]]
    y_planes[0] = [(0, 4)]
    y_planes[1].append((nx - 1, nx))
    y_planes[steps - 2] = [(nx - 2, nx - 1)]
    z_pairs = [[i + 1] for i in range(steps - 2)] + [[], []]
    z_pairs[0] = [0, 1]
    z_pairs[1].append(nx // 2 - 1)
    y_src = {-1: pl.ds((ny - 1) * nz, nz), 1: pl.ds(0, nz)}
    y_dst = {-1: pl.ds(0, nz), 1: pl.ds(block + hy, nz)}

    def y_chunk(i):
        for first, last in y_planes[i]:
            made = [vh.add((0, b, 0), v_ref.at[pl.ds(first, last - first), y_src[b]],
                           e.at[pl.ds(first + 1, last - first), y_dst[b]]) for b in (-1, 1)]
            waits[i].extend(made)
            begin(made)

    def z_chunk(i):
        for pair in z_pairs[i]:
            made = [vh.add((0, 0, 1), zl.at[pair], zn.at[pair])]
            waits[i].extend(made)
            begin(made)

    corners = [vh.add((0, b, 1), cz.at[y_face[b]], cn.at[which[b]]) for b in (-1, 1)]
    waits[0].extend(corners)
    begin(corners)
    for i in range(steps):
        z_chunk(i)
        y_chunk(i)
    x_below = vh.add((1, 0, 0), e.at[1], e.at[nx + 1])
    x_above = vh.add((-1, 0, 0), e.at[nx], e.at[0])
    waits[steps - 1].extend([x_below, x_above])
    for a, at in ((-1, 0), (1, nx + 1)):
        zero_unless(inside(a, 0), [e.at[at]])
    for b in (-1, 1):
        zero_unless(inside(0, b), [e.at[pl.ds(1, nx), y_dst[b]]])
    for b in (-1, 1):
        zero_unless(inside(0, b), [cn.at[which[b]]])
    acc[...] = jnp.zeros_like(acc)

    row = lax.broadcasted_iota(jnp.int32, (nz, nz), 0)
    col = lax.broadcasted_iota(jnp.int32, (nz, nz), 1)
    exact = functools.partial(lax.dot_general, dimension_numbers=(((1,), (1,)), ((), ())),
                              precision=lax.Precision.HIGHEST, preferred_element_type=jnp.float32)
    unit = jnp.where(row == col, 1.0, 0.0)

    def fill_coefficients(n, field, planes):
        for x in planes:
            for y in range(ny):
                at = x * ny + y
                coef[n, x, y * nz:(y + 1) * nz] = jnp.broadcast_to(field[:, at:at + 1], (nz, 128))

    flipped = exact(unit, kappa)
    fill_coefficients(1, flipped * (1.0 / 16.0), range(nx))
    fill_coefficients(2, exact(unit, m_ref[1]) * (1.0 / 216.0), range(nx))

    arrive(kh.all)
    edge_from = jnp.where(gz == 0, nz - 1, 0)
    near_z = jnp.where(jnp.abs(row - col) == 1, 1.0, 0.0) + 2.0 * unit
    across = jnp.where(jnp.logical_and(row == edge_from, col == nz - 1 - edge_from), 1.0, 0.0)
    along_z = exact(near_z, kall[0]) + exact(across, kall[1])
    wide = kall.shape[1]
    plain = functools.partial(jnp.dot, precision=lax.Precision.HIGHEST, preferred_element_type=jnp.float32)
    spans[0] = plain(along_z, w_ref[:wide])

    def diagonal(kappa, field):
        return 2.0 * kappa + (1.0 / 32.0) * field

    inner = plain(spans[0], w_ref[wide:wide + cells])
    fill_coefficients(0, diagonal(flipped, inner), range(1, nx - 1))
    spreads = [kh.add((a, 0, 0), spans.at[0], spans.at[1 + which[a]]) for a in (-1, 1)]
    begin(spreads)
    for a in (-1, 1):
        zero_unless(inside(a, 0), [spans.at[1 + which[a]]])
    for copy in own:
        copy.wait()

    lane = lax.broadcasted_iota(jnp.int32, (8, columns), 0)

    def fill_edge(x):
        z8 = zn[x // 2].astype(jnp.float32)[8 * (x % 2):8 * (x % 2) + 8]
        corners = [cn[n].astype(jnp.float32)[x:x + 1] for n in range(2)]
        c8 = jnp.where(lane == 0, corners[0], jnp.where(lane == 1, corners[1], 0.0))
        full = jnp.concatenate([z8, c8], 0).astype(e.dtype)
        e[x + 1, block - 16:block] = full
        e[x + 1, 2 * block - 16:] = full

    def taps_of(n, slot):
        cut = hy - nz
        one = jnp.dot(t[n, :cut, :block], u[slot, n, :block], preferred_element_type=jnp.float32)
        two = jnp.dot(t[n, cut:cut + 2 * nz], u[slot, n], preferred_element_type=jnp.float32)
        three = jnp.dot(t[n, cut + 2 * nz:, block:], u[slot, n, block:], preferred_element_type=jnp.float32)
        return jnp.concatenate([one, two, three], 0)

    def spread_lanes(c):
        return jnp.concatenate([c] * (columns // 128), 1)

    def iteration(i, carry):
        for c in range(steps):
            @pl.when(i == c)
            def _(c=c):
                arrive(waits[c])
                for first, last in y_planes[c]:
                    for x in range(first, last):
                        fill_edge(x)
                if c == 1:
                    begin([x_below])
                if c == 2:
                    begin([x_above])
                if c == steps - 1:
                    arrive(spreads)
                    field = plain(spans[0], w_ref[wide:wide + cells])
                    for n in (1, 2):
                        field = field + plain(spans[n], w_ref[wide + n * cells:wide + (n + 1) * cells])
                    fill_coefficients(0, diagonal(exact(unit, m_ref[0]), field), (0, nx - 1))

        held = []
        for j in range(STEP):
            x = lax.rem(STEP * i + j + 1, nx)
            here = e[x + 1]
            twice = here + here
            two = e[x] + e[x + 2] + twice
            u[j, 0] = two
            u[j, 1] = two + twice
            v = jnp.concatenate([here[nz:nz + hy], here[block:block + hy]], 0)
            held.append(v)
            rows = slice(j * ny * nz, (j + 1) * ny * nz)
            stiff = spread_lanes(coef[0, x]) * v.astype(jnp.float32) - spread_lanes(coef[1, x]) * taps_of(0, j)
            ybuf[rows, :columns] = stiff.astype(ybuf.dtype)
            mass = spread_lanes(coef[2, x]) * taps_of(1, j)
            ybuf[rows, columns:] = mass.astype(ybuf.dtype)
        acc[...] += lax.dot_general(jnp.concatenate(held, 0), ybuf[...], (((0,), (0,)), ((), ())),
                                    preferred_element_type=jnp.float32)
        return carry

    lax.fori_loop(0, steps, iteration, 0)

    core = lax.axis_index("gx") % 2

    def symmetric(zl_at, core_at):
        some = pl.ds(pl.multiple_of((2 * zl_at + core_at) * 128, 128), 128)
        also = pl.ds(pl.multiple_of((2 * zl_at + core_at) * 128 + columns, 128), 128)
        stiff = ((acc[some, :columns] + acc[:, some].T) * scale).reshape(4, 4, 8, columns)
        mass = ((acc[some, columns:] + acc[:, also].T) * scale).reshape(4, 4, 8, columns)
        upper_rows = lax.broadcasted_iota(jnp.int32, stiff.shape, 2) < 4
        blocks[zl_at, core_at, :, :, 0] = jnp.where(upper_rows, stiff, pltpu.roll(mass, 4, 2))
        blocks[zl_at, core_at, :, :, 1] = jnp.where(upper_rows, pltpu.roll(stiff, 4, 2), mass)

    for zl_at in range(2):
        symmetric(zl_at, 1 - core)
    first = send_across(blocks, reduce_bufs)
    for zl_at in range(2):
        symmetric(zl_at, core)
    reduce_blocks(blocks, out, reduce_bufs, first)
    kh.finish()
    vh.finish()


def coordinates():
    gx, gy, gz = (lax.axis_index(a) for a in AXES)
    return gx // 2, gx % 2, gy // 4, gy % 4, gz


def places_along(axes):
    zl, core, cx, cy, zh = coordinates()
    if axes == "core":
        peer = 1 - core
        return [(peer, {"gx": zl * 2 + peer})]
    me = {"x": cx, "y": cy, "z": zh * 2 + zl}
    found = []
    for k in range(1, 4 ** len(axes)):
        at = dict(me)
        for n, axis in enumerate(axes):
            at[axis] = lax.rem(me[axis] + (k >> 2 * n) % 4, 4)
        device = {}
        if "x" in axes or "y" in axes:
            device["gy"] = at["x"] * 4 + at["y"]
        if "z" in axes:
            device["gx"] = (at["z"] % 2) * 2 + core
            device["gz"] = at["z"] // 2
        peer = tuple(at[axis] for axis in axes)
        found.append((peer if len(axes) > 1 else peer[0], device))
    return found


def greet_reduction():
    barrier = pltpu.get_barrier_semaphore()
    total = 0
    for axis in ("core", "xy", "yz"):
        for _, device in places_along(axis):
            pl.semaphore_signal(barrier, inc=1, device_id=device, device_id_type=pl.DeviceIdType.MESH)
            total += 1
    return total


def spread(axis, piece, landing, send, recv, base):
    copies = []
    for k, (peer, device) in enumerate(places_along(axis)):
        copy = pltpu.make_async_remote_copy(
            src_ref=piece(peer), dst_ref=landing.at[k],
            send_sem=send.at[base + k], recv_sem=recv.at[base + k],
            device_id=device, device_id_type=pl.DeviceIdType.MESH)
        copy.start()
        copies.append(copy)
    return copies


def gathered(copies, own, landing):
    for copy in copies:
        copy.wait_recv()
    held = own
    for k in range(len(copies)):
        held = held + landing[k]
    return held


def lanes_of(columns):
    return slice(0, columns // 2), slice(columns // 2, columns)


def send_across(r, bufs):
    rc, send, recv = bufs[0], bufs[-2], bufs[-1]
    return [spread("core", lambda p, c=c: r.at[:, p, :, :, :, :, c], rc.at[i], send, recv, i)
            for i, c in enumerate(lanes_of(r.shape[-1]))]


def reduce_blocks(r, out, bufs, first):
    zl, core, cx, cy, zh = coordinates()
    rc, ha, ra1, ha1, ra2, hb, rb1, hb1, rb2, send, recv = bufs
    lanes = lanes_of(r.shape[-1])
    ha[...] = gathered(first[0], r[:, core, :, :, :, :, lanes[0]], rc.at[0])
    a1 = spread("x", lambda p: ha.at[:, p], ra1, send, recv, 2)
    hb[...] = gathered(first[1], r[:, core, :, :, :, :, lanes[1]], rc.at[1])
    b1 = spread("z", lambda p: hb.at[p % 2, :, :, p // 2], rb1, send, recv, 5)
    ha1[...] = gathered(a1, ha[:, cx], ra1)
    a2 = spread("yz", lambda p: ha1.at[p[1] % 2, p[0], p[1] // 2], ra2, send, recv, 8)
    hb1[...] = gathered(b1, hb[zl, :, :, zh], rb1)
    b2 = spread("xy", lambda p: hb1.at[p[0], p[1]], rb2, send, recv, 23)
    out[:, lanes[0]] = gathered(a2, ha1[zl, cy, zh], ra2)
    out[:, lanes[1]] = gathered(b2, hb1[cx, cy], rb2)
    for copy in first[0] + first[1] + a1 + b1 + a2 + b2:
        copy.wait_send()


def reduce_scratch(columns):
    half = columns // 2
    f32 = jnp.float32
    shapes = [(2, 1, 2, 4, 4, 2, 8, half),
              (2, 4, 4, 2, 8, half), (3, 2, 4, 2, 8, half), (2, 4, 2, 8, half), (15, 8, half),
              (2, 4, 4, 2, 8, half), (3, 4, 4, 8, half), (4, 4, 8, half), (15, 8, half)]
    return [pltpu.VMEM(shape, f32) for shape in shapes] + [pltpu.SemaphoreType.DMA((38,))] * 2


def per_device(eigvecs, material):
    nx, ny, nz, columns = eigvecs.shape
    total_cells = nx * ny * nz
    for axis in AXES:
        total_cells *= lax.axis_size(axis)
    hy = ny // 2 * nz
    block = nz + hy + 16
    cells = nx * ny
    taps = jnp.asarray(plane_taps(ny, nz), jnp.bfloat16)
    around = jnp.asarray(material_taps(nx, ny), jnp.float32)
    bf16, f32 = jnp.bfloat16, jnp.float32
    dma = pltpu.SemaphoreType.DMA
    vmem = pl.BlockSpec(memory_space=pltpu.VMEM)
    anywhere = pl.BlockSpec(memory_space=pl.ANY)
    scratch = [
        pltpu.VMEM((nx + 2, 2 * block, columns), bf16),
        pltpu.VMEM((2, ny * nz, 2 * block), bf16),
        pltpu.VMEM((ny, nx, 16, columns), bf16),
        pltpu.VMEM((nx // 2, 2 * ny, columns), bf16),
        pltpu.VMEM((nx // 2, 2 * ny, columns), bf16),
        pltpu.VMEM((2, nx, columns), bf16),
        pltpu.VMEM((2, nx, columns), bf16),
        pltpu.VMEM((2, nx, nz), f32),
        pltpu.VMEM((2, around.shape[0] - 3 * cells, nz), f32),
        pltpu.VMEM((3, nz, cells), f32),
        pltpu.VMEM((3, nx, ny * nz, 128), f32),
        pltpu.VMEM((STEP, 2, 2 * block, columns), bf16),
        pltpu.VMEM((STEP * ny * nz, 2 * columns), bf16),
        pltpu.VMEM((columns, 2 * columns), f32),
        pltpu.VMEM((2, 2, 4, 4, 2, 8, columns), f32),
        dma((3 + ny,)), dma((32,)), dma((32,)), dma((7,)), dma((7,)),
    ] + reduce_scratch(columns)
    both = pl.pallas_call(
        functools.partial(kernel, 0.5 / total_cells, (nx, ny, nz)),
        out_shape=jax.ShapeDtypeStruct((8, columns), f32),
        in_specs=[anywhere, vmem, anywhere, vmem],
        out_specs=vmem,
        scratch_shapes=scratch,
        compiler_params=pltpu.CompilerParams(
            vmem_limit_bytes=60 * 1024 * 1024, collective_id=0, has_side_effects=True),
    )(eigvecs.reshape(nx, ny * nz, columns), material.reshape(2, cells, nz), taps, around)
    return both[:4], both[4:]


def solution(mesh):
    return jax.shard_map(
        per_device,
        mesh=mesh,
        in_specs=(P("gx", "gy", "gz", None), P(None, "gx", "gy", "gz")),
        out_specs=(P(("gx", "gy", "gz"), None), P(("gx", "gy", "gz"), None)),
        check_vma=False,
    )
```

```python
import functools
import numpy as np
import jax
import jax.numpy as jnp
from jax import lax
from jax.experimental import pallas as pl
from jax.experimental.pallas import tpu as pltpu
from jax.sharding import PartitionSpec as P

AXES = ("gx", "gy", "gz")
MESH = pl.DeviceIdType.MESH
SIDES = [(0, -1, 0), (0, 1, 0), (0, 0, 1), (0, -1, 1), (0, 1, 1)]
NEAR = SIDES + [(-1, 0, 0), (1, 0, 0)]
STEP = 2


def weight(distance, middle):
    return {0: middle, 1: 1.0}.get(abs(distance), 0.0)


def own_row(y, size_y, size_z):
    half = size_y // 2
    if y < half:
        return size_z * (y + 1)
    return size_z * (half + 1) + 16 + size_z * (y - half)


def plane_taps(size_y, size_z):
    half = size_y // 2
    block = size_z * (half + 1) + 16
    taps = np.zeros((2, 2, size_y * size_z, 2 * block), np.float32)
    for side in range(2):
        edge = size_z - 1 if side == 0 else 0
        for n, middle in enumerate((2.0, 4.0)):
            line = np.array([[weight(z - o, middle) for z in range(size_z)] for o in range(size_z)])
            for y in range(size_y):
                rows = slice(y * size_z, (y + 1) * size_z)
                for near in (y - 1, y, y + 1):
                    w = weight(near - y, middle)
                    if near < 0:
                        first = 0
                    else:
                        first = own_row(near, size_y, size_z)
                    taps[side, n, rows, first:first + size_z] = w * line
                    column = near if 0 <= near < size_y else (size_y if near < 0 else size_y + 1)
                    base = (block if near < half else 2 * block) - 16
                    taps[side, n, y * size_z + edge, base + column] = w
    return taps


def material_taps(size_x, size_y):
    cells = size_x * size_y
    own = [(x, y) for x in range(size_x) for y in range(size_y)]
    faces = [(x, y) for y in (-1, size_y) for x in range(size_x)]
    rows = -(-(cells + 2 * size_x) // 128) * 128
    along_y = np.zeros((rows, cells), np.float32)
    for row, (near_x, near_y) in enumerate(own + faces):
        for col, (x, y) in enumerate(own):
            if x == near_x:
                along_y[row, col] = weight(y - near_y, 2.0)
    along_x = np.zeros((3, cells, cells), np.float32)
    for n, shift in enumerate((0, -size_x, size_x)):
        for row, (near_x, near_y) in enumerate(own):
            for col, (x, y) in enumerate(own):
                if y == near_y:
                    along_x[n, row, col] = weight(x - near_x - shift, 2.0)
    return np.concatenate([along_y, along_x.reshape(3 * cells, cells)], 0)


def inside(a, b):
    gx, gy = lax.axis_index("gx"), lax.axis_index("gy")
    ok = None
    for at, d, count in ((gx, a, lax.axis_size("gx")), (gy, b, lax.axis_size("gy"))):
        if d:
            here = at > 0 if d < 0 else at < count - 1
            ok = here if ok is None else jnp.logical_and(ok, here)
    return ok


def when(condition):
    return (lambda f: f()) if condition is None else pl.when(condition)


def device_at(a, b, c):
    device = {}
    if a:
        device["gx"] = lax.axis_index("gx") + a
    if b:
        device["gy"] = lax.axis_index("gy") + b
    if c:
        device["gz"] = 1 - lax.axis_index("gz")
    return device


def greet_around():
    barrier = pltpu.get_barrier_semaphore()
    total = jnp.int32(greet_reduction())
    for a, b, c in NEAR:
        there = inside(a, b)

        @when(there)
        def _(a=a, b=b, c=c):
            pl.semaphore_signal(barrier, inc=1, device_id=device_at(a, b, c), device_id_type=MESH)

        total = total + (1 if there is None else jnp.where(there, 1, 0))
    return total


class Halo:
    def __init__(self, send, recv):
        self.send, self.recv, self.count, self.all = send, recv, 0, []

    def add(self, side, src, dst):
        a, b, c = side
        copy = pltpu.make_async_remote_copy(
            src_ref=src, dst_ref=dst, send_sem=self.send.at[self.count], recv_sem=self.recv.at[self.count],
            device_id=device_at(-a, -b, c), device_id_type=MESH)
        self.count += 1
        entry = (copy, inside(-a, -b), inside(a, b))
        self.all.append(entry)
        return entry

    def finish(self):
        for copy, sends, _ in self.all:
            when(sends)(copy.wait_send)


def begin(entries):
    for copy, sends, _ in entries:
        when(sends)(copy.start)


def arrive(entries):
    for copy, _, receives in entries:
        when(receives)(copy.wait_recv)


def zero_unless(condition, refs):
    if condition is None:
        return

    @pl.when(jnp.logical_not(condition))
    def _():
        for ref in refs:
            ref[...] = jnp.zeros(ref.shape, ref.dtype)


def kernel(scale, sizes, v_ref, m_ref, t_hbm, w_ref, out,
           e, t, ztile, zl, zn, cz, cn, faces, kall, spans, coef, u, q, ybuf, acc,
           own_sem, v_send, v_recv, k_send, k_recv, *reduce_bufs):
    nx, ny, nz = sizes
    columns = e.shape[2]
    gz = lax.axis_index("gz")
    hy = ny // 2 * nz
    block = nz + hy + 16
    cells = nx * ny
    low, high = pl.ds(nz, hy), pl.ds(block, hy)
    own = [pltpu.make_async_copy(v_ref.at[:, :hy], e.at[pl.ds(1, nx), low], own_sem.at[0]),
           pltpu.make_async_copy(v_ref.at[:, hy:], e.at[pl.ds(1, nx), high], own_sem.at[1]),
           pltpu.make_async_copy(t_hbm.at[gz], t, own_sem.at[2])]
    z_first = pl.multiple_of((nz - 16) * (1 - gz), 16)
    tiles = [pltpu.make_async_copy(v_ref.at[:, pl.ds(y * nz + z_first, 16)], ztile.at[y], own_sem.at[3 + y])
             for y in range(ny)]
    for copy in tiles + own:
        copy.start()
    total = greet_around()

    kappa = m_ref[0]
    for n, y in enumerate((0, ny - 1)):
        faces[n] = jnp.concatenate([kappa[x * ny + y:x * ny + y + 1] for x in range(nx)], 0)
    kall[0, :cells] = kappa

    for copy in tiles:
        copy.wait()

    def extract(at):
        def edge_row(x, y):
            return ztile[y, x].astype(jnp.float32)[at:at + 1]

        for q in range(nx // 2):
            rows = [edge_row(2 * q + n // ny, n % ny) for n in range(2 * ny)]
            zl[q] = jnp.concatenate(rows, 0).astype(zl.dtype)
        for n, y in enumerate((0, ny - 1)):
            cz[n] = jnp.concatenate([edge_row(x, y) for x in range(nx)], 0).astype(cz.dtype)

    pl.when(gz == 0)(functools.partial(extract, 15))
    pl.when(gz == 1)(functools.partial(extract, 0))

    pl.semaphore_wait(pltpu.get_barrier_semaphore(), total)

    kh = Halo(k_send, k_recv)
    which = {-1: 0, 1: 1}
    y_face = {-1: 1, 1: 0}
    for a, b, c in SIDES:
        if b == 0:
            src, dst = m_ref.at[0], kall.at[c, pl.ds(0, cells)]
        else:
            src, dst = faces.at[y_face[b]], kall.at[c, pl.ds(cells + which[b] * nx, nx)]
        begin([kh.add((a, b, c), src, dst)])
        zero_unless(inside(a, b), [dst])
    used = cells + 2 * nx
    for c in range(2):
        kall[c, used:] = jnp.zeros((kall.shape[1] - used, nz), jnp.float32)

    vh = Halo(v_send, v_recv)
    steps = nx // STEP
    waits = [[] for _ in range(steps)]
    y_planes = [[(2 * i + 2, 2 * i + 4)] for i in range(steps - 1)] + [[]]
    y_planes[0] = [(0, 4)]
    y_planes[1].append((nx - 1, nx))
    y_planes[steps - 2] = [(nx - 2, nx - 1)]
    z_pairs = [[i + 1] for i in range(steps - 2)] + [[], []]
    z_pairs[0] = [0, 1]
    z_pairs[1].append(nx // 2 - 1)
    y_src = {-1: pl.ds((ny - 1) * nz, nz), 1: pl.ds(0, nz)}
    y_dst = {-1: pl.ds(0, nz), 1: pl.ds(block + hy, nz)}

    def y_chunk(i):
        for first, last in y_planes[i]:
            made = [vh.add((0, b, 0), v_ref.at[pl.ds(first, last - first), y_src[b]],
                           e.at[pl.ds(first + 1, last - first), y_dst[b]]) for b in (-1, 1)]
            waits[i].extend(made)
            begin(made)

    def z_chunk(i):
        for pair in z_pairs[i]:
            made = [vh.add((0, 0, 1), zl.at[pair], zn.at[pair])]
            waits[i].extend(made)
            begin(made)

    corners = [vh.add((0, b, 1), cz.at[y_face[b]], cn.at[which[b]]) for b in (-1, 1)]
    waits[0].extend(corners)
    begin(corners)
    for i in range(steps):
        z_chunk(i)
        y_chunk(i)
    x_below = vh.add((1, 0, 0), e.at[1], e.at[nx + 1])
    x_above = vh.add((-1, 0, 0), e.at[nx], e.at[0])
    waits[steps - 1].extend([x_below, x_above])
    for a, at in ((-1, 0), (1, nx + 1)):
        zero_unless(inside(a, 0), [e.at[at]])
    for b in (-1, 1):
        zero_unless(inside(0, b), [e.at[pl.ds(1, nx), y_dst[b]]])
    for b in (-1, 1):
        zero_unless(inside(0, b), [cn.at[which[b]]])
    acc[...] = jnp.zeros_like(acc)

    row = lax.broadcasted_iota(jnp.int32, (nz, nz), 0)
    col = lax.broadcasted_iota(jnp.int32, (nz, nz), 1)
    exact = functools.partial(lax.dot_general, dimension_numbers=(((1,), (1,)), ((), ())),
                              precision=lax.Precision.HIGHEST, preferred_element_type=jnp.float32)
    unit = jnp.where(row == col, 1.0, 0.0)

    def keep(n, field):
        for i in range(steps):
            first = (STEP * i + 1) * ny
            coef[n, i] = pltpu.roll(field, (cells - first) % cells, 1)

    keep(1, exact(unit, kappa) * (1.0 / 16.0))
    keep(2, exact(unit, m_ref[1]) * (1.0 / 216.0))

    wide = kall.shape[1]
    plain = functools.partial(jnp.dot, precision=lax.Precision.HIGHEST, preferred_element_type=jnp.float32)
    near = list(kh.all)
    spreads = [kh.add((a, 0, 0), spans.at[0], spans.at[1 + which[a]]) for a in (-1, 1)]
    for a in (-1, 1):
        zero_unless(inside(a, 0), [spans.at[1 + which[a]]])

    def tap_material():
        arrive(near)
        edge_from = jnp.where(gz == 0, nz - 1, 0)
        near_z = jnp.where(jnp.abs(row - col) == 1, 1.0, 0.0) + 2.0 * unit
        across = jnp.where(jnp.logical_and(row == edge_from, col == nz - 1 - edge_from), 1.0, 0.0)
        along_z = exact(near_z, kall[0]) + exact(across, kall[1])
        spans[0] = plain(along_z, w_ref[:wide])

    def diagonal():
        arrive(spreads)
        field = plain(spans[0], w_ref[wide:wide + cells])
        for n in (1, 2):
            field = field + plain(spans[n], w_ref[wide + n * cells:wide + (n + 1) * cells])
        keep(0, 2.0 * exact(unit, m_ref[0]) + (1.0 / 32.0) * field)

    for copy in own:
        copy.wait()

    lane = lax.broadcasted_iota(jnp.int32, (8, columns), 0)

    def fill_edge(x):
        z8 = zn[x // 2].astype(jnp.float32)[8 * (x % 2):8 * (x % 2) + 8]
        corners = [cn[n].astype(jnp.float32)[x:x + 1] for n in range(2)]
        c8 = jnp.where(lane == 0, corners[0], jnp.where(lane == 1, corners[1], 0.0))
        full = jnp.concatenate([z8, c8], 0).astype(e.dtype)
        e[x + 1, block - 16:block] = full
        e[x + 1, 2 * block - 16:] = full

    def taps_of(n, slot):
        cut = hy - nz
        one = jnp.dot(t[n, :cut, :block], u[slot, n, :block], preferred_element_type=jnp.float32)
        two = jnp.dot(t[n, cut:cut + 2 * nz], u[slot, n], preferred_element_type=jnp.float32)
        three = jnp.dot(t[n, cut + 2 * nz:, block:], u[slot, n, block:], preferred_element_type=jnp.float32)
        return jnp.concatenate([one, two, three], 0)

    def coefficient(n, i, j):
        field = coef[n, i]
        tall = [jnp.broadcast_to(field[:, j * ny + y:j * ny + y + 1], (nz, 128)) for y in range(ny)]
        return jnp.concatenate([jnp.concatenate(tall, 0)] * (columns // 128), 1)

    def own_cells(x):
        return jnp.concatenate([e[x + 1, nz:nz + hy], e[x + 1, block:block + hy]], 0)

    def gram(n, cells_of):
        acc[n] += lax.dot_general(jnp.concatenate(cells_of, 0), ybuf[n], (((0,), (0,)), ((), ())),
                                  preferred_element_type=jnp.float32)

    def iteration(i, carry):
        for c in range(steps):
            @pl.when(i == c)
            def _(c=c):
                arrive(waits[c])
                for first, last in y_planes[c]:
                    for x in range(first, last):
                        fill_edge(x)
                if c == 1:
                    begin([x_below])
                if c == 2:
                    begin([x_above])
                if c == 3:
                    tap_material()
                if c == 4:
                    begin(spreads)

        held = []
        for j in range(STEP):
            x = lax.rem(STEP * i + j + 1, nx)
            here = e[x + 1]
            twice = here + here
            two = e[x] + e[x + 2] + twice
            u[j, 0] = two
            u[j, 1] = two + twice
            held.append(own_cells(x))
            q[x] = (coefficient(1, i, j) * taps_of(0, j)).astype(q.dtype)
            rows = slice(j * ny * nz, (j + 1) * ny * nz)
            ybuf[0, rows] = (coefficient(2, i, j) * taps_of(1, j)).astype(ybuf.dtype)
        gram(0, held)
        return carry

    def stiff_iteration(i, carry):
        held = []
        for j in range(STEP):
            x = lax.rem(STEP * i + j + 1, nx)
            v = own_cells(x)
            held.append(v)
            stiff = coefficient(0, i, j) * v.astype(jnp.float32) - q[x].astype(jnp.float32)
            ybuf[1, j * ny * nz:(j + 1) * ny * nz] = stiff.astype(ybuf.dtype)
        gram(1, held)
        return carry

    lax.fori_loop(0, steps, iteration, 0)

    core = lax.axis_index("gx") % 2
    many = len(reduce_bufs) // 2
    mass_bufs, stiff_bufs = reduce_bufs[:many], reduce_bufs[many:]

    def symmetric(n, blocks, core_at):
        for zl_at in range(2):
            some = pl.ds(pl.multiple_of((2 * zl_at + core_at) * 128, 128), 128)
            full = ((acc[n, some] + acc[n, :, some].T) * scale).reshape(4, 4, 8, columns)
            left, right = full[..., :columns // 2], full[..., columns // 2:]
            upper_rows = lax.broadcasted_iota(jnp.int32, left.shape, 2) < 4
            blocks[zl_at, core_at, :, :, 0] = jnp.where(upper_rows, left, pltpu.roll(right, 4, 2))
            blocks[zl_at, core_at, :, :, 1] = jnp.where(upper_rows, pltpu.roll(left, 4, 2), right)

    symmetric(0, mass_bufs[0], 1 - core)
    mass_sum = Reduction(mass_bufs)
    mass_sum.across()
    symmetric(0, mass_bufs[0], core)
    diagonal()
    some = steps * 5 // 8
    lax.fori_loop(0, some, stiff_iteration, 0)
    mass_sum.first()
    lax.fori_loop(some, steps, stiff_iteration, 0)
    symmetric(1, stiff_bufs[0], 1 - core)
    stiff_sum = Reduction(stiff_bufs)
    stiff_sum.across()
    symmetric(1, stiff_bufs[0], core)
    stiff_sum.first()
    mass_sum.second()
    stiff_sum.second()
    mass_sum.store(out, 4)
    stiff_sum.store(out, 0)
    mass_sum.finish()
    stiff_sum.finish()
    kh.finish()
    vh.finish()


def coordinates():
    gx, gy, gz = (lax.axis_index(a) for a in AXES)
    return gx // 2, gx % 2, gy // 4, gy % 4, gz


def places_along(axes):
    zl, core, cx, cy, zh = coordinates()
    if axes == "core":
        peer = 1 - core
        return [(peer, {"gx": zl * 2 + peer})]
    me = {"x": cx, "y": cy, "z": zh * 2 + zl}
    found = []
    for k in range(1, 4 ** len(axes)):
        at = dict(me)
        for n, axis in enumerate(axes):
            at[axis] = lax.rem(me[axis] + (k >> 2 * n) % 4, 4)
        device = {}
        if "x" in axes or "y" in axes:
            device["gy"] = at["x"] * 4 + at["y"]
        if "z" in axes:
            device["gx"] = (at["z"] % 2) * 2 + core
            device["gz"] = at["z"] // 2
        peer = tuple(at[axis] for axis in axes)
        found.append((peer if len(axes) > 1 else peer[0], device))
    return found


def greet_reduction():
    barrier = pltpu.get_barrier_semaphore()
    total = 0
    for axis in ("core", "xy", "yz"):
        for _, device in places_along(axis):
            pl.semaphore_signal(barrier, inc=1, device_id=device, device_id_type=pl.DeviceIdType.MESH)
            total += 1
    return total


def spread(axis, piece, landing, send, recv, base):
    copies = []
    for k, (peer, device) in enumerate(places_along(axis)):
        copy = pltpu.make_async_remote_copy(
            src_ref=piece(peer), dst_ref=landing.at[k],
            send_sem=send.at[base + k], recv_sem=recv.at[base + k],
            device_id=device, device_id_type=pl.DeviceIdType.MESH)
        copy.start()
        copies.append(copy)
    return copies


def gathered(copies, own, landing):
    for copy in copies:
        copy.wait_recv()
    held = own
    for k in range(len(copies)):
        held = held + landing[k]
    return held


class Reduction:
    def __init__(self, bufs):
        (self.r, self.rc, self.ha, self.ra1, self.ha1, self.ra2,
         self.hb, self.rb1, self.hb1, self.rb2, self.send, self.recv) = bufs
        half = self.r.shape[-1] // 2
        self.lanes = slice(0, half), slice(half, 2 * half)
        self.all = []

    def spread(self, axes, piece, landing, base):
        copies = spread(axes, piece, landing, self.send, self.recv, base)
        self.all.extend(copies)
        return copies

    def across(self):
        self.crossed = [self.spread("core", lambda p, c=c: self.r.at[:, p, :, :, :, :, c], self.rc.at[i], i)
                        for i, c in enumerate(self.lanes)]

    def first(self):
        core = lax.axis_index("gx") % 2
        self.ha[...] = gathered(self.crossed[0], self.r[:, core, :, :, :, :, self.lanes[0]], self.rc.at[0])
        self.a1 = self.spread("x", lambda p: self.ha.at[:, p], self.ra1, 2)
        self.hb[...] = gathered(self.crossed[1], self.r[:, core, :, :, :, :, self.lanes[1]], self.rc.at[1])
        self.b1 = self.spread("z", lambda p: self.hb.at[p % 2, :, :, p // 2], self.rb1, 5)

    def second(self):
        zl, core, cx, cy, zh = coordinates()
        self.ha1[...] = gathered(self.a1, self.ha[:, cx], self.ra1)
        self.a2 = self.spread("yz", lambda p: self.ha1.at[p[1] % 2, p[0], p[1] // 2], self.ra2, 8)
        self.hb1[...] = gathered(self.b1, self.hb[zl, :, :, zh], self.rb1)
        self.b2 = self.spread("xy", lambda p: self.hb1.at[p[0], p[1]], self.rb2, 23)

    def store(self, out, row):
        zl, core, cx, cy, zh = coordinates()
        half = out.shape[1] // 2
        for lanes, copies, own, landing in ((self.lanes[0], self.a2, self.ha1[zl, cy, zh], self.ra2),
                                            (self.lanes[1], self.b2, self.hb1[cx, cy], self.rb2)):
            done = gathered(copies, own, landing)
            out[row:row + 4, lanes] = done[:4]
            out[row:row + 4, slice(half + lanes.start, half + lanes.stop)] = done[4:]

    def finish(self):
        for copy in self.all:
            copy.wait_send()


def reduce_scratch(columns):
    half = columns // 4
    f32 = jnp.float32
    shapes = [(2, 2, 4, 4, 2, 8, 2 * half), (2, 1, 2, 4, 4, 2, 8, half),
              (2, 4, 4, 2, 8, half), (3, 2, 4, 2, 8, half), (2, 4, 2, 8, half), (15, 8, half),
              (2, 4, 4, 2, 8, half), (3, 4, 4, 8, half), (4, 4, 8, half), (15, 8, half)]
    return [pltpu.VMEM(shape, f32) for shape in shapes] + [pltpu.SemaphoreType.DMA((38,))] * 2


def per_device(eigvecs, material):
    nx, ny, nz, columns = eigvecs.shape
    total_cells = nx * ny * nz
    for axis in AXES:
        total_cells *= lax.axis_size(axis)
    hy = ny // 2 * nz
    block = nz + hy + 16
    cells = nx * ny
    taps = jnp.asarray(plane_taps(ny, nz), jnp.bfloat16)
    around = jnp.asarray(material_taps(nx, ny), jnp.float32)
    bf16, f32 = jnp.bfloat16, jnp.float32
    dma = pltpu.SemaphoreType.DMA
    vmem = pl.BlockSpec(memory_space=pltpu.VMEM)
    anywhere = pl.BlockSpec(memory_space=pl.ANY)
    scratch = [
        pltpu.VMEM((nx + 2, 2 * block, columns), bf16),
        pltpu.VMEM((2, ny * nz, 2 * block), bf16),
        pltpu.VMEM((ny, nx, 16, columns), bf16),
        pltpu.VMEM((nx // 2, 2 * ny, columns), bf16),
        pltpu.VMEM((nx // 2, 2 * ny, columns), bf16),
        pltpu.VMEM((2, nx, columns), bf16),
        pltpu.VMEM((2, nx, columns), bf16),
        pltpu.VMEM((2, nx, nz), f32),
        pltpu.VMEM((2, around.shape[0] - 3 * cells, nz), f32),
        pltpu.VMEM((3, nz, cells), f32),
        pltpu.VMEM((3, nx // STEP, nz, cells), f32),
        pltpu.VMEM((STEP, 2, 2 * block, columns), bf16),
        pltpu.VMEM((nx, ny * nz, columns), bf16),
        pltpu.VMEM((2, STEP * ny * nz, columns), bf16),
        pltpu.VMEM((2, columns, columns), f32),
        dma((3 + ny,)), dma((32,)), dma((32,)), dma((7,)), dma((7,)),
    ] + reduce_scratch(columns) * 2
    both = pl.pallas_call(
        functools.partial(kernel, 0.5 / total_cells, (nx, ny, nz)),
        out_shape=jax.ShapeDtypeStruct((8, columns), f32),
        in_specs=[anywhere, vmem, anywhere, vmem],
        out_specs=vmem,
        scratch_shapes=scratch,
        compiler_params=pltpu.CompilerParams(
            vmem_limit_bytes=60 * 1024 * 1024, collective_id=0, has_side_effects=True),
    )(eigvecs.reshape(nx, ny * nz, columns), material.reshape(2, cells, nz), taps, around)
    return both[:4], both[4:]


def solution(mesh):
    return jax.shard_map(
        per_device,
        mesh=mesh,
        in_specs=(P("gx", "gy", "gz", None), P(None, "gx", "gy", "gz")),
        out_specs=(P(("gx", "gy", "gz"), None), P(("gx", "gy", "gz"), None)),
        check_vma=False,
    )
```

```python
import functools
import numpy as np
import jax
import jax.numpy as jnp
from jax import lax
from jax.experimental import pallas as pl
from jax.experimental.pallas import tpu as pltpu
from jax.sharding import PartitionSpec as P

AXES = ("gx", "gy", "gz")
MESH = pl.DeviceIdType.MESH
SIDES = [(0, -1, 0), (0, 1, 0), (0, 0, 1), (0, -1, 1), (0, 1, 1)]
NEAR = SIDES + [(-1, 0, 0), (1, 0, 0)]
STEP = 2


def weight(distance, middle):
    return {0: middle, 1: 1.0}.get(abs(distance), 0.0)


def own_row(y, size_y, size_z):
    half = size_y // 2
    if y < half:
        return size_z * (y + 1)
    return size_z * (half + 1) + 16 + size_z * (y - half)


def plane_taps(size_y, size_z):
    half = size_y // 2
    block = size_z * (half + 1) + 16
    taps = np.zeros((2, 2, size_y * size_z, 2 * block), np.float32)
    for side in range(2):
        edge = size_z - 1 if side == 0 else 0
        for n, middle in enumerate((2.0, 4.0)):
            line = np.array([[weight(z - o, middle) for z in range(size_z)] for o in range(size_z)])
            for y in range(size_y):
                rows = slice(y * size_z, (y + 1) * size_z)
                for near in (y - 1, y, y + 1):
                    w = weight(near - y, middle)
                    if near < 0:
                        first = 0
                    else:
                        first = own_row(near, size_y, size_z)
                    taps[side, n, rows, first:first + size_z] = w * line
                    column = near if 0 <= near < size_y else (size_y if near < 0 else size_y + 1)
                    base = (block if near < half else 2 * block) - 16
                    taps[side, n, y * size_z + edge, base + column] = w
    return taps


def material_taps(size_x, size_y):
    cells = size_x * size_y
    own = [(x, y) for x in range(size_x) for y in range(size_y)]
    faces = [(x, y) for y in (-1, size_y) for x in range(size_x)]
    rows = -(-(cells + 2 * size_x) // 128) * 128
    along_y = np.zeros((rows, cells), np.float32)
    for row, (near_x, near_y) in enumerate(own + faces):
        for col, (x, y) in enumerate(own):
            if x == near_x:
                along_y[row, col] = weight(y - near_y, 2.0)
    along_x = np.zeros((3, cells, cells), np.float32)
    for n, shift in enumerate((0, -size_x, size_x)):
        for row, (near_x, near_y) in enumerate(own):
            for col, (x, y) in enumerate(own):
                if y == near_y:
                    along_x[n, row, col] = weight(x - near_x - shift, 2.0)
    return np.concatenate([along_y, along_x.reshape(3 * cells, cells)], 0)


def inside(a, b):
    gx, gy = lax.axis_index("gx"), lax.axis_index("gy")
    ok = None
    for at, d, count in ((gx, a, lax.axis_size("gx")), (gy, b, lax.axis_size("gy"))):
        if d:
            here = at > 0 if d < 0 else at < count - 1
            ok = here if ok is None else jnp.logical_and(ok, here)
    return ok


def when(condition):
    return (lambda f: f()) if condition is None else pl.when(condition)


def device_at(a, b, c):
    device = {}
    if a:
        device["gx"] = lax.axis_index("gx") + a
    if b:
        device["gy"] = lax.axis_index("gy") + b
    if c:
        device["gz"] = 1 - lax.axis_index("gz")
    return device


def greet_around():
    barrier = pltpu.get_barrier_semaphore()
    total = jnp.int32(greet_reduction())
    for a, b, c in NEAR:
        if b and c:
            continue
        there = inside(a, b)

        @when(there)
        def _(a=a, b=b, c=c):
            pl.semaphore_signal(barrier, inc=1, device_id=device_at(a, b, c), device_id_type=MESH)

        total = total + (1 if there is None else jnp.where(there, 1, 0))
    return total


def vouch(far_sem):
    total = jnp.int32(3)
    for _, device in places_along("y"):
        pl.semaphore_signal(far_sem, inc=1, device_id=device, device_id_type=MESH)
    for b in (-1, 1):
        there = inside(0, b)

        @when(there)
        def _(b=b):
            pl.semaphore_signal(far_sem, inc=1, device_id=device_at(0, b, 0), device_id_type=MESH)

        total = total + jnp.where(there, 1, 0)
    return total


class Halo:
    def __init__(self, send, recv):
        self.send, self.recv, self.count, self.all = send, recv, 0, []

    def add(self, side, src, dst):
        a, b, c = side
        copy = pltpu.make_async_remote_copy(
            src_ref=src, dst_ref=dst, send_sem=self.send.at[self.count], recv_sem=self.recv.at[self.count],
            device_id=device_at(-a, -b, c), device_id_type=MESH)
        self.count += 1
        entry = (copy, inside(-a, -b), inside(a, b))
        self.all.append(entry)
        return entry

    def finish(self):
        for copy, sends, _ in self.all:
            when(sends)(copy.wait_send)


def begin(entries):
    for copy, sends, _ in entries:
        when(sends)(copy.start)


def arrive(entries):
    for copy, _, receives in entries:
        when(receives)(copy.wait_recv)


def zero_unless(condition, refs):
    if condition is None:
        return

    @pl.when(jnp.logical_not(condition))
    def _():
        for ref in refs:
            ref[...] = jnp.zeros(ref.shape, ref.dtype)


def kernel(scale, sizes, v_ref, m_ref, t_hbm, w_ref, out,
           e, t, ztile, zl, zn, cz, cn, faces, kall, spans, coef, u, ybuf, acc, blocks,
           own_sem, v_send, v_recv, k_send, k_recv, far_sem, *reduce_bufs):
    nx, ny, nz = sizes
    columns = e.shape[2]
    gz = lax.axis_index("gz")
    hy = ny // 2 * nz
    block = nz + hy + 16
    cells = nx * ny
    low, high = pl.ds(nz, hy), pl.ds(block, hy)
    own = [pltpu.make_async_copy(v_ref.at[:, :hy], e.at[pl.ds(1, nx), low], own_sem.at[0]),
           pltpu.make_async_copy(v_ref.at[:, hy:], e.at[pl.ds(1, nx), high], own_sem.at[1]),
           pltpu.make_async_copy(t_hbm.at[gz], t, own_sem.at[2])]
    z_first = pl.multiple_of((nz - 16) * (1 - gz), 16)
    tiles = [pltpu.make_async_copy(v_ref.at[:, pl.ds(y * nz + z_first, 16)], ztile.at[y], own_sem.at[3 + y])
             for y in range(ny)]
    for copy in tiles + own:
        copy.start()
    total = greet_around()

    kappa = m_ref[0]
    for n, y in enumerate((0, ny - 1)):
        faces[n] = jnp.concatenate([kappa[x * ny + y:x * ny + y + 1] for x in range(nx)], 0)
    kall[0, :cells] = kappa

    for copy in tiles:
        copy.wait()

    def extract(at):
        def edge_row(x, y):
            return ztile[y, x].astype(jnp.float32)[at:at + 1]

        for q in range(nx // 2):
            rows = [edge_row(2 * q + n // ny, n % ny) for n in range(2 * ny)]
            zl[q] = jnp.concatenate(rows, 0).astype(zl.dtype)
        for n, y in enumerate((0, ny - 1)):
            cz[n] = jnp.concatenate([edge_row(x, y) for x in range(nx)], 0).astype(cz.dtype)

    pl.when(gz == 0)(functools.partial(extract, 15))
    pl.when(gz == 1)(functools.partial(extract, 0))

    pl.semaphore_wait(pltpu.get_barrier_semaphore(), total)
    vouched = vouch(far_sem)

    kh = Halo(k_send, k_recv)
    which = {-1: 0, 1: 1}
    y_face = {-1: 1, 1: 0}
    def exchange_material(sides):
        for a, b, c in sides:
            if b == 0:
                src, dst = m_ref.at[0], kall.at[c, pl.ds(0, cells)]
            else:
                src, dst = faces.at[y_face[b]], kall.at[c, pl.ds(cells + which[b] * nx, nx)]
            begin([kh.add((a, b, c), src, dst)])
            zero_unless(inside(a, b), [dst])

    exchange_material([side for side in SIDES if not (side[1] and side[2])])
    used = cells + 2 * nx
    for c in range(2):
        kall[c, used:] = jnp.zeros((kall.shape[1] - used, nz), jnp.float32)

    vh = Halo(v_send, v_recv)
    steps = nx // STEP
    waits = [[] for _ in range(steps)]
    y_planes = [[(2 * i + 2, 2 * i + 4)] for i in range(steps - 1)] + [[]]
    y_planes[0] = [(0, 2), (2, 4)]
    y_planes[1].append((nx - 1, nx))
    y_planes[steps - 2] = [(nx - 2, nx - 1)]
    z_pairs = [[i + 1] for i in range(steps - 2)] + [[], []]
    z_pairs[0] = [0, 1]
    z_pairs[1].append(nx // 2 - 1)
    y_src = {-1: pl.ds((ny - 1) * nz, nz), 1: pl.ds(0, nz)}
    y_dst = {-1: pl.ds(0, nz), 1: pl.ds(block + hy, nz)}

    def y_chunk(i, planes=None):
        for first, last in planes or y_planes[i]:
            made = [vh.add((0, b, 0), v_ref.at[pl.ds(first, last - first), y_src[b]],
                           e.at[pl.ds(first + 1, last - first), y_dst[b]]) for b in (-1, 1)]
            waits[i].extend(made)
            begin(made)

    def z_chunk(i):
        for pair in z_pairs[i]:
            made = [vh.add((0, 0, 1), zl.at[pair], zn.at[pair])]
            waits[i].extend(made)
            begin(made)

    far = [(a, b, c) for a, b, c in SIDES if b and c]
    z_chunk(0)
    y_chunk(0, y_planes[0][:1])
    pl.semaphore_wait(far_sem, vouched)
    exchange_material(far)
    corners = [vh.add((0, b, 1), cz.at[y_face[b]], cn.at[which[b]]) for b in (-1, 1)]
    waits[0].extend(corners)
    begin(corners)
    y_chunk(0, y_planes[0][1:])
    for i in range(1, steps):
        z_chunk(i)
        y_chunk(i)
    x_forward = {}
    for a, mine, there in ((1, 0, nx + 1), (-1, nx - 1, 0)):
        early = [vh.add((a, 0, 0), v_ref.at[mine, pl.ds(0, hy)], e.at[there, low]),
                 vh.add((a, 0, 0), v_ref.at[mine, pl.ds(hy, hy)], e.at[there, high])]
        begin(early)
        x_forward[a] = [vh.add((a, 0, 0), e.at[mine + 1, rows], e.at[there, rows])
                        for rows in (pl.ds(0, nz), pl.ds(nz + hy, 16), pl.ds(block + hy, nz + 16))]
        waits[steps - 1].extend(early + x_forward[a])
    for a, at in ((-1, 0), (1, nx + 1)):
        zero_unless(inside(a, 0), [e.at[at]])
    for b in (-1, 1):
        zero_unless(inside(0, b), [e.at[pl.ds(1, nx), y_dst[b]]])
    for b in (-1, 1):
        zero_unless(inside(0, b), [cn.at[which[b]]])
    acc[...] = jnp.zeros_like(acc)

    row = lax.broadcasted_iota(jnp.int32, (nz, nz), 0)
    col = lax.broadcasted_iota(jnp.int32, (nz, nz), 1)
    exact = functools.partial(lax.dot_general, dimension_numbers=(((1,), (1,)), ((), ())),
                              precision=lax.Precision.HIGHEST, preferred_element_type=jnp.float32)
    unit = jnp.where(row == col, 1.0, 0.0)

    def keep(n, field, only=None):
        for i in range(steps) if only is None else only:
            first = (STEP * i + 1) * ny
            coef[n, i] = pltpu.roll(field, (cells - first) % cells, 1)

    flipped = exact(unit, kappa)
    keep(1, flipped * (1.0 / 16.0))
    keep(2, exact(unit, m_ref[1]) * (1.0 / 216.0))

    arrive(kh.all)
    edge_from = jnp.where(gz == 0, nz - 1, 0)
    near_z = jnp.where(jnp.abs(row - col) == 1, 1.0, 0.0) + 2.0 * unit
    across = jnp.where(jnp.logical_and(row == edge_from, col == nz - 1 - edge_from), 1.0, 0.0)
    along_z = exact(near_z, kall[0]) + exact(across, kall[1])
    wide = kall.shape[1]
    plain = functools.partial(jnp.dot, precision=lax.Precision.HIGHEST, preferred_element_type=jnp.float32)
    spans[0] = plain(along_z, w_ref[:wide])

    def diagonal(kappa, field):
        return 2.0 * kappa + (1.0 / 32.0) * field

    inner = plain(spans[0], w_ref[wide:wide + cells])
    keep(0, diagonal(flipped, inner))
    spreads = [kh.add((a, 0, 0), spans.at[0], spans.at[1 + which[a]]) for a in (-1, 1)]
    for a in (-1, 1):
        zero_unless(inside(a, 0), [spans.at[1 + which[a]]])
    for copy in own:
        copy.wait()

    lane = lax.broadcasted_iota(jnp.int32, (8, columns), 0)

    def fill_edge(x):
        z8 = zn[x // 2].astype(jnp.float32)[8 * (x % 2):8 * (x % 2) + 8]
        corners = [cn[n].astype(jnp.float32)[x:x + 1] for n in range(2)]
        c8 = jnp.where(lane == 0, corners[0], jnp.where(lane == 1, corners[1], 0.0))
        full = jnp.concatenate([z8, c8], 0).astype(e.dtype)
        e[x + 1, block - 16:block] = full
        e[x + 1, 2 * block - 16:] = full

    def taps_of(n, slot):
        cut = hy - nz
        one = jnp.dot(t[n, :cut, :block], u[slot, n, :block], preferred_element_type=jnp.float32)
        two = jnp.dot(t[n, cut:cut + 2 * nz], u[slot, n], preferred_element_type=jnp.float32)
        three = jnp.dot(t[n, cut + 2 * nz:, block:], u[slot, n, block:], preferred_element_type=jnp.float32)
        return jnp.concatenate([one, two, three], 0)

    def coefficient(n, i, j):
        field = coef[n, i]
        tall = [jnp.broadcast_to(field[:, j * ny + y:j * ny + y + 1], (nz, 128)) for y in range(ny)]
        return jnp.concatenate([jnp.concatenate(tall, 0)] * (columns // 128), 1)

    def iteration(i, carry):
        for c in range(steps):
            @pl.when(i == c)
            def _(c=c):
                arrive(waits[c])
                for first, last in y_planes[c]:
                    for x in range(first, last):
                        fill_edge(x)
                if c == 1:
                    begin(spreads)
                if c == 2:
                    begin(x_forward[1])
                if c == 3:
                    begin(x_forward[-1])
                if c == steps - 2:
                    arrive(spreads)
                    field = plain(spans[0], w_ref[wide:wide + cells])
                    for n in (1, 2):
                        field = field + plain(spans[n], w_ref[wide + n * cells:wide + (n + 1) * cells])
                    keep(0, diagonal(exact(unit, m_ref[0]), field), (steps - 1,))

        held = []
        for j in range(STEP):
            x = lax.rem(STEP * i + j + 1, nx)
            here = e[x + 1]
            twice = here + here
            two = e[x] + e[x + 2] + twice
            u[j, 0] = two
            u[j, 1] = two + twice
            v = jnp.concatenate([here[nz:nz + hy], here[block:block + hy]], 0)
            held.append(v)
            rows = slice(j * ny * nz, (j + 1) * ny * nz)
            stiff = coefficient(0, i, j) * v.astype(jnp.float32) - coefficient(1, i, j) * taps_of(0, j)
            ybuf[rows, :columns] = stiff.astype(ybuf.dtype)
            mass = coefficient(2, i, j) * taps_of(1, j)
            ybuf[rows, columns:] = mass.astype(ybuf.dtype)
        acc[...] += lax.dot_general(jnp.concatenate(held, 0), ybuf[...], (((0,), (0,)), ((), ())),
                                    preferred_element_type=jnp.float32)
        return carry

    lax.fori_loop(0, steps, iteration, 0)

    core = lax.axis_index("gx") % 2

    def symmetric(zl_at, core_at):
        some = pl.ds(pl.multiple_of((2 * zl_at + core_at) * 128, 128), 128)
        also = pl.ds(pl.multiple_of((2 * zl_at + core_at) * 128 + columns, 128), 128)
        stiff = ((acc[some, :columns] + acc[:, some].T) * scale).reshape(4, 4, 8, columns)
        mass = ((acc[some, columns:] + acc[:, also].T) * scale).reshape(4, 4, 8, columns)
        upper_rows = lax.broadcasted_iota(jnp.int32, stiff.shape, 2) < 4
        blocks[zl_at, core_at, :, :, 0] = jnp.where(upper_rows, stiff, pltpu.roll(mass, 4, 2))
        blocks[zl_at, core_at, :, :, 1] = jnp.where(upper_rows, pltpu.roll(stiff, 4, 2), mass)

    for zl_at in range(2):
        symmetric(zl_at, 1 - core)
    first = send_across(blocks, reduce_bufs)
    for zl_at in range(2):
        symmetric(zl_at, core)
    reduce_blocks(blocks, out, reduce_bufs, first)
    kh.finish()
    vh.finish()


def coordinates():
    gx, gy, gz = (lax.axis_index(a) for a in AXES)
    return gx // 2, gx % 2, gy // 4, gy % 4, gz


def places_along(axes):
    zl, core, cx, cy, zh = coordinates()
    if axes == "core":
        peer = 1 - core
        return [(peer, {"gx": zl * 2 + peer})]
    me = {"x": cx, "y": cy, "z": zh * 2 + zl}
    found = []
    for k in range(1, 4 ** len(axes)):
        at = dict(me)
        for n, axis in enumerate(axes):
            at[axis] = lax.rem(me[axis] + (k >> 2 * n) % 4, 4)
        device = {}
        if "x" in axes or "y" in axes:
            device["gy"] = at["x"] * 4 + at["y"]
        if "z" in axes:
            device["gx"] = (at["z"] % 2) * 2 + core
            device["gz"] = at["z"] // 2
        peer = tuple(at[axis] for axis in axes)
        found.append((peer if len(axes) > 1 else peer[0], device))
    return found


def greet_reduction():
    barrier = pltpu.get_barrier_semaphore()
    total = 0
    for axis in ("core", "x", "y", "z"):
        for _, device in places_along(axis):
            pl.semaphore_signal(barrier, inc=1, device_id=device, device_id_type=pl.DeviceIdType.MESH)
            total += 1
    return total


def spread(axis, piece, landing, send, recv, base):
    copies = []
    for k, (peer, device) in enumerate(places_along(axis)):
        copy = pltpu.make_async_remote_copy(
            src_ref=piece(peer), dst_ref=landing.at[k],
            send_sem=send.at[base + k], recv_sem=recv.at[base + k],
            device_id=device, device_id_type=pl.DeviceIdType.MESH)
        copy.start()
        copies.append(copy)
    return copies


def gathered(copies, own, landing):
    for copy in copies:
        copy.wait_recv()
    held = own
    for k in range(len(copies)):
        held = held + landing[k]
    return held


def lanes_of(columns):
    return slice(0, columns // 2), slice(columns // 2, columns)


def send_across(r, bufs):
    rc, send, recv = bufs[0], bufs[-2], bufs[-1]
    return [spread("core", lambda p, c=c: r.at[:, p, :, :, :, :, c], rc.at[i], send, recv, i)
            for i, c in enumerate(lanes_of(r.shape[-1]))]


def reduce_blocks(r, out, bufs, first):
    zl, core, cx, cy, zh = coordinates()
    rc, ha, ra1, ha1, ra2, hb, rb1, hb1, rb2, send, recv = bufs
    lanes = lanes_of(r.shape[-1])
    ha[...] = gathered(first[0], r[:, core, :, :, :, :, lanes[0]], rc.at[0])
    a1 = spread("x", lambda p: ha.at[:, p], ra1, send, recv, 2)
    hb[...] = gathered(first[1], r[:, core, :, :, :, :, lanes[1]], rc.at[1])
    b1 = spread("z", lambda p: hb.at[p % 2, :, :, p // 2], rb1, send, recv, 5)
    ha1[...] = gathered(a1, ha[:, cx], ra1)
    a2 = spread("yz", lambda p: ha1.at[p[1] % 2, p[0], p[1] // 2], ra2, send, recv, 8)
    hb1[...] = gathered(b1, hb[zl, :, :, zh], rb1)
    b2 = spread("xy", lambda p: hb1.at[p[0], p[1]], rb2, send, recv, 23)
    out[:, lanes[0]] = gathered(a2, ha1[zl, cy, zh], ra2)
    out[:, lanes[1]] = gathered(b2, hb1[cx, cy], rb2)
    for copy in first[0] + first[1] + a1 + b1 + a2 + b2:
        copy.wait_send()


def reduce_scratch(columns):
    half = columns // 2
    f32 = jnp.float32
    shapes = [(2, 1, 2, 4, 4, 2, 8, half),
              (2, 4, 4, 2, 8, half), (3, 2, 4, 2, 8, half), (2, 4, 2, 8, half), (15, 8, half),
              (2, 4, 4, 2, 8, half), (3, 4, 4, 8, half), (4, 4, 8, half), (15, 8, half)]
    return [pltpu.VMEM(shape, f32) for shape in shapes] + [pltpu.SemaphoreType.DMA((38,))] * 2


def per_device(eigvecs, material):
    nx, ny, nz, columns = eigvecs.shape
    total_cells = nx * ny * nz
    for axis in AXES:
        total_cells *= lax.axis_size(axis)
    hy = ny // 2 * nz
    block = nz + hy + 16
    cells = nx * ny
    taps = jnp.asarray(plane_taps(ny, nz), jnp.bfloat16)
    around = jnp.asarray(material_taps(nx, ny), jnp.float32)
    bf16, f32 = jnp.bfloat16, jnp.float32
    dma = pltpu.SemaphoreType.DMA
    vmem = pl.BlockSpec(memory_space=pltpu.VMEM)
    anywhere = pl.BlockSpec(memory_space=pl.ANY)
    scratch = [
        pltpu.VMEM((nx + 2, 2 * block, columns), bf16),
        pltpu.VMEM((2, ny * nz, 2 * block), bf16),
        pltpu.VMEM((ny, nx, 16, columns), bf16),
        pltpu.VMEM((nx // 2, 2 * ny, columns), bf16),
        pltpu.VMEM((nx // 2, 2 * ny, columns), bf16),
        pltpu.VMEM((2, nx, columns), bf16),
        pltpu.VMEM((2, nx, columns), bf16),
        pltpu.VMEM((2, nx, nz), f32),
        pltpu.VMEM((2, around.shape[0] - 3 * cells, nz), f32),
        pltpu.VMEM((3, nz, cells), f32),
        pltpu.VMEM((3, nx // STEP, nz, cells), f32),
        pltpu.VMEM((STEP, 2, 2 * block, columns), bf16),
        pltpu.VMEM((STEP * ny * nz, 2 * columns), bf16),
        pltpu.VMEM((columns, 2 * columns), f32),
        pltpu.VMEM((2, 2, 4, 4, 2, 8, columns), f32),
        dma((3 + ny,)), dma((48,)), dma((48,)), dma((7,)), dma((7,)), pltpu.SemaphoreType.REGULAR,
    ] + reduce_scratch(columns)
    both = pl.pallas_call(
        functools.partial(kernel, 0.5 / total_cells, (nx, ny, nz)),
        out_shape=jax.ShapeDtypeStruct((8, columns), f32),
        in_specs=[anywhere, vmem, anywhere, vmem],
        out_specs=vmem,
        scratch_shapes=scratch,
        compiler_params=pltpu.CompilerParams(
            vmem_limit_bytes=60 * 1024 * 1024, collective_id=0, has_side_effects=True),
    )(eigvecs.reshape(nx, ny * nz, columns), material.reshape(2, cells, nz), taps, around)
    return both[:4], both[4:]


def solution(mesh):
    return jax.shard_map(
        per_device,
        mesh=mesh,
        in_specs=(P("gx", "gy", "gz", None), P(None, "gx", "gy", "gz")),
        out_specs=(P(("gx", "gy", "gz"), None), P(("gx", "gy", "gz"), None)),
        check_vma=False,
    )
```

```python
import functools
import numpy as np
import jax
import jax.numpy as jnp
from jax import lax
from jax.experimental import pallas as pl
from jax.experimental.pallas import tpu as pltpu
from jax.sharding import PartitionSpec as P

AXES = ("gx", "gy", "gz")
MESH = pl.DeviceIdType.MESH
SIDES = [(0, -1, 0), (0, 1, 0), (0, 0, 1), (0, -1, 1), (0, 1, 1)]
NEAR = SIDES + [(-1, 0, 0), (1, 0, 0)]
STEP = 2


def weight(distance, middle):
    return {0: middle, 1: 1.0}.get(abs(distance), 0.0)


def own_row(y, size_y, size_z):
    half = size_y // 2
    if y < half:
        return size_z * (y + 1)
    return size_z * (half + 1) + 16 + size_z * (y - half)


def plane_taps(size_y, size_z):
    half = size_y // 2
    block = size_z * (half + 1) + 16
    taps = np.zeros((2, 2, size_y * size_z, 2 * block), np.float32)
    for side in range(2):
        edge = size_z - 1 if side == 0 else 0
        for n, middle in enumerate((2.0, 4.0)):
            line = np.array([[weight(z - o, middle) for z in range(size_z)] for o in range(size_z)])
            for y in range(size_y):
                rows = slice(y * size_z, (y + 1) * size_z)
                for near in (y - 1, y, y + 1):
                    w = weight(near - y, middle)
                    if near < 0:
                        first = 0
                    else:
                        first = own_row(near, size_y, size_z)
                    taps[side, n, rows, first:first + size_z] = w * line
                    column = near if 0 <= near < size_y else (size_y if near < 0 else size_y + 1)
                    base = (block if near < half else 2 * block) - 16
                    taps[side, n, y * size_z + edge, base + column] = w
    return taps


def material_taps(size_x, size_y):
    cells = size_x * size_y
    own = [(x, y) for x in range(size_x) for y in range(size_y)]
    faces = [(x, y) for y in (-1, size_y) for x in range(size_x)]
    rows = -(-(cells + 2 * size_x) // 128) * 128
    along_y = np.zeros((rows, cells), np.float32)
    for row, (near_x, near_y) in enumerate(own + faces):
        for col, (x, y) in enumerate(own):
            if x == near_x:
                along_y[row, col] = weight(y - near_y, 2.0)
    along_x = np.zeros((3, cells, cells), np.float32)
    for n, shift in enumerate((0, -size_x, size_x)):
        for row, (near_x, near_y) in enumerate(own):
            for col, (x, y) in enumerate(own):
                if y == near_y:
                    along_x[n, row, col] = weight(x - near_x - shift, 2.0)
    return np.concatenate([along_y, along_x.reshape(3 * cells, cells)], 0)


def inside(a, b):
    gx, gy = lax.axis_index("gx"), lax.axis_index("gy")
    ok = None
    for at, d, count in ((gx, a, lax.axis_size("gx")), (gy, b, lax.axis_size("gy"))):
        if d:
            here = at > 0 if d < 0 else at < count - 1
            ok = here if ok is None else jnp.logical_and(ok, here)
    return ok


def when(condition):
    return (lambda f: f()) if condition is None else pl.when(condition)


def device_at(a, b, c):
    device = {}
    if a:
        device["gx"] = lax.axis_index("gx") + a
    if b:
        device["gy"] = lax.axis_index("gy") + b
    if c:
        device["gz"] = 1 - lax.axis_index("gz")
    return device


def greet_around():
    barrier = pltpu.get_barrier_semaphore()
    total = jnp.int32(greet_reduction())
    for a, b, c in NEAR:
        if b and c:
            continue
        there = inside(a, b)

        @when(there)
        def _(a=a, b=b, c=c):
            pl.semaphore_signal(barrier, inc=1, device_id=device_at(a, b, c), device_id_type=MESH)

        total = total + (1 if there is None else jnp.where(there, 1, 0))
    return total


def vouch(far_sem):
    total = jnp.int32(3)
    for _, device in places_along("y"):
        pl.semaphore_signal(far_sem, inc=1, device_id=device, device_id_type=MESH)
    for b in (-1, 1):
        there = inside(0, b)

        @when(there)
        def _(b=b):
            pl.semaphore_signal(far_sem, inc=1, device_id=device_at(0, b, 0), device_id_type=MESH)

        total = total + jnp.where(there, 1, 0)
    return total


def first_plane(i, steps):
    late = i // (steps - 3) - i // (steps - 2)
    return STEP * i + 1 - 2 * (i // (steps - 2)) + 4 * late


class Halo:
    def __init__(self, send, recv):
        self.send, self.recv, self.count, self.all = send, recv, 0, []

    def add(self, side, src, dst):
        a, b, c = side
        copy = pltpu.make_async_remote_copy(
            src_ref=src, dst_ref=dst, send_sem=self.send.at[self.count], recv_sem=self.recv.at[self.count],
            device_id=device_at(-a, -b, c), device_id_type=MESH)
        self.count += 1
        entry = (copy, inside(-a, -b), inside(a, b))
        self.all.append(entry)
        return entry

    def finish(self):
        for copy, sends, _ in self.all:
            when(sends)(copy.wait_send)


def begin(entries):
    for copy, sends, _ in entries:
        when(sends)(copy.start)


def arrive(entries):
    for copy, _, receives in entries:
        when(receives)(copy.wait_recv)


def zero_unless(condition, refs):
    if condition is None:
        return

    @pl.when(jnp.logical_not(condition))
    def _():
        for ref in refs:
            ref[...] = jnp.zeros(ref.shape, ref.dtype)


def kernel(scale, sizes, v_ref, m_ref, t_hbm, w_ref, out,
           e, t, ztile, zl, zn, cz, cn, faces, kall, spans, inner, coef, u, ybuf, acc, blocks,
           own_sem, v_send, v_recv, k_send, k_recv, far_sem, *reduce_bufs):
    nx, ny, nz = sizes
    columns = e.shape[2]
    gz = lax.axis_index("gz")
    hy = ny // 2 * nz
    block = nz + hy + 16
    cells = nx * ny
    low, high = pl.ds(nz, hy), pl.ds(block, hy)
    own = [pltpu.make_async_copy(v_ref.at[:, :hy], e.at[pl.ds(1, nx), low], own_sem.at[0]),
           pltpu.make_async_copy(v_ref.at[:, hy:], e.at[pl.ds(1, nx), high], own_sem.at[1]),
           pltpu.make_async_copy(t_hbm.at[gz], t, own_sem.at[2])]
    z_first = pl.multiple_of((nz - 16) * (1 - gz), 16)
    tiles = [pltpu.make_async_copy(v_ref.at[:, pl.ds(y * nz + z_first, 16)], ztile.at[y], own_sem.at[3 + y])
             for y in range(ny)]
    for copy in tiles + own:
        copy.start()
    total = greet_around()

    kappa = m_ref[0]
    for n, y in enumerate((0, ny - 1)):
        faces[n] = jnp.concatenate([kappa[x * ny + y:x * ny + y + 1] for x in range(nx)], 0)
    kall[0, :cells] = kappa

    for copy in tiles:
        copy.wait()

    def extract(at):
        def edge_row(x, y):
            return ztile[y, x].astype(jnp.float32)[at:at + 1]

        for q in range(nx // 2):
            rows = [edge_row(2 * q + n // ny, n % ny) for n in range(2 * ny)]
            zl[q] = jnp.concatenate(rows, 0).astype(zl.dtype)
        for n, y in enumerate((0, ny - 1)):
            cz[n] = jnp.concatenate([edge_row(x, y) for x in range(nx)], 0).astype(cz.dtype)

    pl.when(gz == 0)(functools.partial(extract, 15))
    pl.when(gz == 1)(functools.partial(extract, 0))

    pl.semaphore_wait(pltpu.get_barrier_semaphore(), total)
    vouched = vouch(far_sem)

    kh = Halo(k_send, k_recv)
    which = {-1: 0, 1: 1}
    y_face = {-1: 1, 1: 0}
    sent = []

    def exchange_material(sides):
        for a, b, c in sides:
            if b == 0:
                src, dst = m_ref.at[0], kall.at[c, pl.ds(0, cells)]
            else:
                src, dst = faces.at[y_face[b]], kall.at[c, pl.ds(cells + which[b] * nx, nx)]
            begin([kh.add((a, b, c), src, dst)])
            sent.append((a, b, c))
            zero_unless(inside(a, b), [dst])

    exchange_material([side for side in SIDES if not (side[1] and side[2])])
    used = cells + 2 * nx
    for c in range(2):
        kall[c, used:] = jnp.zeros((kall.shape[1] - used, nz), jnp.float32)

    vh = Halo(v_send, v_recv)
    steps = nx // STEP
    waits = [[] for _ in range(steps)]
    split = steps - 3
    y_planes = [[(2 * i + 2, 2 * i + 4)] for i in range(split)] + [[], [(nx - 4, nx - 2)], []]
    y_planes[0] = [(0, 2), (2, 4)]
    y_planes[1].append((nx - 1, nx))
    y_planes[2].append((nx - 2, nx - 1))
    z_pairs = [[i + 1] for i in range(split)] + [[], [nx // 2 - 2], []]
    z_pairs[0] = [0, 1]
    z_pairs[1].append(nx // 2 - 1)
    y_src = {-1: pl.ds((ny - 1) * nz, nz), 1: pl.ds(0, nz)}
    y_dst = {-1: pl.ds(0, nz), 1: pl.ds(block + hy, nz)}

    def y_chunk(i, planes=None):
        for first, last in planes or y_planes[i]:
            made = [vh.add((0, b, 0), v_ref.at[pl.ds(first, last - first), y_src[b]],
                           e.at[pl.ds(first + 1, last - first), y_dst[b]]) for b in (-1, 1)]
            waits[i].extend(made)
            begin(made)

    def z_chunk(i):
        for pair in z_pairs[i]:
            made = [vh.add((0, 0, 1), zl.at[pair], zn.at[pair])]
            waits[i].extend(made)
            begin(made)

    far = [(a, b, c) for a, b, c in SIDES if b and c]
    z_chunk(0)
    y_chunk(0, y_planes[0][:1])
    pl.semaphore_wait(far_sem, vouched)
    exchange_material(far)
    corners = [vh.add((0, b, 1), cz.at[y_face[b]], cn.at[which[b]]) for b in (-1, 1)]
    begin(corners)
    y_chunk(0, y_planes[0][1:])
    for i in range(1, steps):
        z_chunk(i)
        y_chunk(i)
    x_forward = {}
    for a, mine, there in ((1, 0, nx + 1), (-1, nx - 1, 0)):
        early = [vh.add((a, 0, 0), v_ref.at[mine, pl.ds(0, hy)], e.at[there, low]),
                 vh.add((a, 0, 0), v_ref.at[mine, pl.ds(hy, hy)], e.at[there, high])]
        begin(early)
        x_forward[a] = [vh.add((a, 0, 0), e.at[mine + 1, rows], e.at[there, rows])
                        for rows in (pl.ds(0, nz), pl.ds(nz + hy, 16), pl.ds(block + hy, nz + 16))]
        waits[split].extend(early + x_forward[a])
    for a, at in ((-1, 0), (1, nx + 1)):
        zero_unless(inside(a, 0), [e.at[at]])
    for b in (-1, 1):
        zero_unless(inside(0, b), [e.at[pl.ds(1, nx), y_dst[b]]])
    for b in (-1, 1):
        zero_unless(inside(0, b), [cn.at[which[b]]])
    acc[...] = jnp.zeros_like(acc)

    row = lax.broadcasted_iota(jnp.int32, (nz, nz), 0)
    col = lax.broadcasted_iota(jnp.int32, (nz, nz), 1)
    exact = functools.partial(lax.dot_general, dimension_numbers=(((1,), (1,)), ((), ())),
                              precision=lax.Precision.HIGHEST, preferred_element_type=jnp.float32)
    unit = jnp.where(row == col, 1.0, 0.0)

    def keep(n, field, only=None):
        for i in range(steps) if only is None else only:
            first = first_plane(i, steps) * ny
            coef[n, i] = pltpu.roll(field, (cells - first) % cells, 1)

    flipped = exact(unit, kappa)
    keep(1, flipped * (1.0 / 16.0))
    keep(2, exact(unit, m_ref[1]) * (1.0 / 216.0))

    material = {side: entry for side, entry in zip(sent, kh.all)}
    arrive([material[side] for side in sent if side not in far])
    edge_from = jnp.where(gz == 0, nz - 1, 0)
    near_z = jnp.where(jnp.abs(row - col) == 1, 1.0, 0.0) + 2.0 * unit
    across = jnp.where(jnp.logical_and(row == edge_from, col == nz - 1 - edge_from), 1.0, 0.0)
    wide = kall.shape[1]
    plain = functools.partial(jnp.dot, precision=lax.Precision.HIGHEST, preferred_element_type=jnp.float32)
    along_x = w_ref[wide:wide + cells]
    along_z = exact(near_z, kall[0])
    inner[0] = plain(along_z, w_ref[:wide]) + plain(exact(across, kall[1, :cells]), w_ref[:cells])
    inner[1] = plain(inner[0], along_x)

    def diagonal(kappa, field):
        return 2.0 * kappa + (1.0 / 32.0) * field

    keep(0, diagonal(flipped, inner[1]))
    spreads = [kh.add((a, 0, 0), spans.at[0], spans.at[1 + which[a]]) for a in (-1, 1)]
    for a in (-1, 1):
        zero_unless(inside(a, 0), [spans.at[1 + which[a]]])

    def far_material():
        arrive([material[side] for side in far])
        here = plain(exact(across, kall[1, cells:]), w_ref[cells:wide])
        spans[0] = inner[0] + here
        keep(0, diagonal(exact(unit, m_ref[0]), inner[1] + plain(here, along_x)))

    def along_planes(rows, middle):
        return pltpu.roll(rows, 1, 0) + pltpu.roll(rows, nx - 1, 0) + middle * rows

    def late_corners():
        lanes = lax.broadcasted_iota(jnp.int32, (nx, nz), 1)
        planes = lax.broadcasted_iota(jnp.int32, (nx, columns), 0)
        done = jnp.logical_and(planes >= 1, planes <= 2 * STEP)

        def at_edge(rows, edge):
            return jnp.broadcast_to(jnp.sum(jnp.where(lanes == edge, rows, 0.0), axis=1, keepdims=True), (nx, columns))

        added = []
        for n, y in enumerate((0, ny - 1)):
            rho = jnp.concatenate([m_ref[1, x * ny + y:x * ny + y + 1] for x in range(nx)], 0)
            beyond = at_edge(kall[1, cells + n * nx:cells + (n + 1) * nx], nz - 1 - edge_from)
            corner = cn[n].astype(jnp.float32)
            stiff = (1.0 / 32.0) * along_planes(beyond, 2.0) * cz[n].astype(jnp.float32)
            stiff = stiff - (1.0 / 16.0) * at_edge(faces[n], edge_from) * along_planes(corner, 2.0)
            mass = (1.0 / 216.0) * at_edge(rho, edge_from) * along_planes(corner, 4.0)
            added.append(jnp.concatenate([jnp.where(done, stiff, 0.0), jnp.where(done, mass, 0.0)], 1))
        acc[...] += lax.dot_general(jnp.concatenate([cz[0], cz[1]], 0), jnp.concatenate(added, 0).astype(cz.dtype),
                                    (((0,), (0,)), ((), ())), preferred_element_type=jnp.float32)

    for copy in own:
        copy.wait()

    lane = lax.broadcasted_iota(jnp.int32, (8, columns), 0)

    def fill_edge(x, with_corners):
        z8 = zn[x // 2].astype(jnp.float32)[8 * (x % 2):8 * (x % 2) + 8]
        if with_corners:
            rows = [cn[n].astype(jnp.float32)[x:x + 1] for n in range(2)]
            c8 = jnp.where(lane == 0, rows[0], jnp.where(lane == 1, rows[1], 0.0))
        else:
            c8 = jnp.zeros((8, columns), jnp.float32)
        full = jnp.concatenate([z8, c8], 0).astype(e.dtype)
        e[x + 1, block - 16:block] = full
        e[x + 1, 2 * block - 16:] = full

    def taps_of(n, slot):
        cut = hy - nz
        one = jnp.dot(t[n, :cut, :block], u[slot, n, :block], preferred_element_type=jnp.float32)
        two = jnp.dot(t[n, cut:cut + 2 * nz], u[slot, n], preferred_element_type=jnp.float32)
        three = jnp.dot(t[n, cut + 2 * nz:, block:], u[slot, n, block:], preferred_element_type=jnp.float32)
        return jnp.concatenate([one, two, three], 0)

    def coefficient(n, i, j):
        field = coef[n, i]
        tall = [jnp.broadcast_to(field[:, j * ny + y:j * ny + y + 1], (nz, 128)) for y in range(ny)]
        return jnp.concatenate([jnp.concatenate(tall, 0)] * (columns // 128), 1)

    def iteration(i, carry):
        for c in range(steps):
            @pl.when(i == c)
            def _(c=c):
                arrive(waits[c])
                planes = [x for first, last in y_planes[c] for x in range(first, last)]
                if c == 2:
                    arrive(corners)
                    planes += [x for k in range(2) for first, last in y_planes[k] for x in range(first, last)]
                for x in planes:
                    fill_edge(x, c >= 2)
                if c == 2:
                    far_material()
                    late_corners()
                if c == 3:
                    begin(spreads + x_forward[1] + x_forward[-1])
                if c == split:
                    arrive(spreads)
                    field = plain(spans[0], along_x)
                    for n in (1, 2):
                        field = field + plain(spans[n], w_ref[wide + n * cells:wide + (n + 1) * cells])
                    keep(0, diagonal(exact(unit, m_ref[0]), field), (split,))

        held = []
        for j in range(STEP):
            x = lax.rem(first_plane(i, steps) + j, nx)
            here = e[x + 1]
            twice = here + here
            two = e[x] + e[x + 2] + twice
            u[j, 0] = two
            u[j, 1] = two + twice
            v = jnp.concatenate([here[nz:nz + hy], here[block:block + hy]], 0)
            held.append(v)
            rows = slice(j * ny * nz, (j + 1) * ny * nz)
            stiff = coefficient(0, i, j) * v.astype(jnp.float32) - coefficient(1, i, j) * taps_of(0, j)
            ybuf[rows, :columns] = stiff.astype(ybuf.dtype)
            mass = coefficient(2, i, j) * taps_of(1, j)
            ybuf[rows, columns:] = mass.astype(ybuf.dtype)
        acc[...] += lax.dot_general(jnp.concatenate(held, 0), ybuf[...], (((0,), (0,)), ((), ())),
                                    preferred_element_type=jnp.float32)
        return carry

    lax.fori_loop(0, steps, iteration, 0)

    core = lax.axis_index("gx") % 2

    def symmetric(zl_at, core_at):
        some = pl.ds(pl.multiple_of((2 * zl_at + core_at) * 128, 128), 128)
        also = pl.ds(pl.multiple_of((2 * zl_at + core_at) * 128 + columns, 128), 128)
        stiff = ((acc[some, :columns] + acc[:, some].T) * scale).reshape(4, 4, 8, columns)
        mass = ((acc[some, columns:] + acc[:, also].T) * scale).reshape(4, 4, 8, columns)
        upper_rows = lax.broadcasted_iota(jnp.int32, stiff.shape, 2) < 4
        blocks[zl_at, core_at, :, :, 0] = jnp.where(upper_rows, stiff, pltpu.roll(mass, 4, 2))
        blocks[zl_at, core_at, :, :, 1] = jnp.where(upper_rows, pltpu.roll(stiff, 4, 2), mass)

    for zl_at in range(2):
        symmetric(zl_at, 1 - core)
    first = send_across(blocks, reduce_bufs)
    for zl_at in range(2):
        symmetric(zl_at, core)
    reduce_blocks(blocks, out, reduce_bufs, first)
    kh.finish()
    vh.finish()


def coordinates():
    gx, gy, gz = (lax.axis_index(a) for a in AXES)
    return gx // 2, gx % 2, gy // 4, gy % 4, gz


def places_along(axes):
    zl, core, cx, cy, zh = coordinates()
    if axes == "core":
        peer = 1 - core
        return [(peer, {"gx": zl * 2 + peer})]
    me = {"x": cx, "y": cy, "z": zh * 2 + zl}
    found = []
    for k in range(1, 4 ** len(axes)):
        at = dict(me)
        for n, axis in enumerate(axes):
            at[axis] = lax.rem(me[axis] + (k >> 2 * n) % 4, 4)
        device = {}
        if "x" in axes or "y" in axes:
            device["gy"] = at["x"] * 4 + at["y"]
        if "z" in axes:
            device["gx"] = (at["z"] % 2) * 2 + core
            device["gz"] = at["z"] // 2
        peer = tuple(at[axis] for axis in axes)
        found.append((peer if len(axes) > 1 else peer[0], device))
    return found


def greet_reduction():
    barrier = pltpu.get_barrier_semaphore()
    total = 0
    for axis in ("core", "x", "y", "z"):
        for _, device in places_along(axis):
            pl.semaphore_signal(barrier, inc=1, device_id=device, device_id_type=pl.DeviceIdType.MESH)
            total += 1
    return total


def spread(axis, piece, landing, send, recv, base):
    copies = []
    for k, (peer, device) in enumerate(places_along(axis)):
        copy = pltpu.make_async_remote_copy(
            src_ref=piece(peer), dst_ref=landing.at[k],
            send_sem=send.at[base + k], recv_sem=recv.at[base + k],
            device_id=device, device_id_type=pl.DeviceIdType.MESH)
        copy.start()
        copies.append(copy)
    return copies


def gathered(copies, own, landing):
    for copy in copies:
        copy.wait_recv()
    held = own
    for k in range(len(copies)):
        held = held + landing[k]
    return held


def lanes_of(columns):
    return slice(0, columns // 2), slice(columns // 2, columns)


def send_across(r, bufs):
    rc, send, recv = bufs[0], bufs[-2], bufs[-1]
    return [spread("core", lambda p, c=c: r.at[:, p, :, :, :, :, c], rc.at[i], send, recv, i)
            for i, c in enumerate(lanes_of(r.shape[-1]))]


def reduce_blocks(r, out, bufs, first):
    zl, core, cx, cy, zh = coordinates()
    rc, ha, ra1, ha1, ra2, hb, rb1, hb1, rb2, send, recv = bufs
    lanes = lanes_of(r.shape[-1])
    ha[...] = gathered(first[0], r[:, core, :, :, :, :, lanes[0]], rc.at[0])
    a1 = spread("x", lambda p: ha.at[:, p], ra1, send, recv, 2)
    hb[...] = gathered(first[1], r[:, core, :, :, :, :, lanes[1]], rc.at[1])
    b1 = spread("z", lambda p: hb.at[p % 2, :, :, p // 2], rb1, send, recv, 5)
    ha1[...] = gathered(a1, ha[:, cx], ra1)
    a2 = spread("yz", lambda p: ha1.at[p[1] % 2, p[0], p[1] // 2], ra2, send, recv, 8)
    hb1[...] = gathered(b1, hb[zl, :, :, zh], rb1)
    b2 = spread("xy", lambda p: hb1.at[p[0], p[1]], rb2, send, recv, 23)
    out[:, lanes[0]] = gathered(a2, ha1[zl, cy, zh], ra2)
    out[:, lanes[1]] = gathered(b2, hb1[cx, cy], rb2)
    for copy in first[0] + first[1] + a1 + b1 + a2 + b2:
        copy.wait_send()


def reduce_scratch(columns):
    half = columns // 2
    f32 = jnp.float32
    shapes = [(2, 1, 2, 4, 4, 2, 8, half),
              (2, 4, 4, 2, 8, half), (3, 2, 4, 2, 8, half), (2, 4, 2, 8, half), (15, 8, half),
              (2, 4, 4, 2, 8, half), (3, 4, 4, 8, half), (4, 4, 8, half), (15, 8, half)]
    return [pltpu.VMEM(shape, f32) for shape in shapes] + [pltpu.SemaphoreType.DMA((38,))] * 2


def per_device(eigvecs, material):
    nx, ny, nz, columns = eigvecs.shape
    total_cells = nx * ny * nz
    for axis in AXES:
        total_cells *= lax.axis_size(axis)
    hy = ny // 2 * nz
    block = nz + hy + 16
    cells = nx * ny
    taps = jnp.asarray(plane_taps(ny, nz), jnp.bfloat16)
    around = jnp.asarray(material_taps(nx, ny), jnp.float32)
    bf16, f32 = jnp.bfloat16, jnp.float32
    dma = pltpu.SemaphoreType.DMA
    vmem = pl.BlockSpec(memory_space=pltpu.VMEM)
    anywhere = pl.BlockSpec(memory_space=pl.ANY)
    scratch = [
        pltpu.VMEM((nx + 2, 2 * block, columns), bf16),
        pltpu.VMEM((2, ny * nz, 2 * block), bf16),
        pltpu.VMEM((ny, nx, 16, columns), bf16),
        pltpu.VMEM((nx // 2, 2 * ny, columns), bf16),
        pltpu.VMEM((nx // 2, 2 * ny, columns), bf16),
        pltpu.VMEM((2, nx, columns), bf16),
        pltpu.VMEM((2, nx, columns), bf16),
        pltpu.VMEM((2, nx, nz), f32),
        pltpu.VMEM((2, around.shape[0] - 3 * cells, nz), f32),
        pltpu.VMEM((3, nz, cells), f32),
        pltpu.VMEM((2, nz, cells), f32),
        pltpu.VMEM((3, nx // STEP, nz, cells), f32),
        pltpu.VMEM((STEP, 2, 2 * block, columns), bf16),
        pltpu.VMEM((STEP * ny * nz, 2 * columns), bf16),
        pltpu.VMEM((columns, 2 * columns), f32),
        pltpu.VMEM((2, 2, 4, 4, 2, 8, columns), f32),
        dma((3 + ny,)), dma((48,)), dma((48,)), dma((7,)), dma((7,)), pltpu.SemaphoreType.REGULAR,
    ] + reduce_scratch(columns)
    both = pl.pallas_call(
        functools.partial(kernel, 0.5 / total_cells, (nx, ny, nz)),
        out_shape=jax.ShapeDtypeStruct((8, columns), f32),
        in_specs=[anywhere, vmem, anywhere, vmem],
        out_specs=vmem,
        scratch_shapes=scratch,
        compiler_params=pltpu.CompilerParams(
            vmem_limit_bytes=60 * 1024 * 1024, collective_id=0, has_side_effects=True),
    )(eigvecs.reshape(nx, ny * nz, columns), material.reshape(2, cells, nz), taps, around)
    return both[:4], both[4:]


def solution(mesh):
    return jax.shard_map(
        per_device,
        mesh=mesh,
        in_specs=(P("gx", "gy", "gz", None), P(None, "gx", "gy", "gz")),
        out_specs=(P(("gx", "gy", "gz"), None), P(("gx", "gy", "gz"), None)),
        check_vma=False,
    )
```

```python
import functools
import numpy as np
import jax
import jax.numpy as jnp
from jax import lax
from jax.experimental import pallas as pl
from jax.experimental.pallas import tpu as pltpu
from jax.sharding import PartitionSpec as P

AXES = ("gx", "gy", "gz")
MESH = pl.DeviceIdType.MESH
SIDES = [(0, -1, 0), (0, 1, 0), (0, 0, 1), (0, -1, 1), (0, 1, 1)]
NEAR = SIDES + [(-1, 0, 0), (1, 0, 0)]
STEP = 2


def weight(distance, middle):
    return {0: middle, 1: 1.0}.get(abs(distance), 0.0)


def own_row(y, size_y, size_z):
    half = size_y // 2
    if y < half:
        return size_z * (y + 1)
    return size_z * (half + 1) + 16 + size_z * (y - half)


def plane_taps(size_y, size_z):
    half = size_y // 2
    block = size_z * (half + 1) + 16
    taps = np.zeros((2, 2, size_y * size_z, 2 * block), np.float32)
    for side in range(2):
        edge = size_z - 1 if side == 0 else 0
        for n, middle in enumerate((2.0, 4.0)):
            line = np.array([[weight(z - o, middle) for z in range(size_z)] for o in range(size_z)])
            for y in range(size_y):
                rows = slice(y * size_z, (y + 1) * size_z)
                for near in (y - 1, y, y + 1):
                    w = weight(near - y, middle)
                    if near < 0:
                        first = 0
                    else:
                        first = own_row(near, size_y, size_z)
                    taps[side, n, rows, first:first + size_z] = w * line
                    column = near if 0 <= near < size_y else (size_y if near < 0 else size_y + 1)
                    base = (block if near < half else 2 * block) - 16
                    taps[side, n, y * size_z + edge, base + column] = w
    return taps


def material_taps(size_x, size_y):
    cells = size_x * size_y
    own = [(x, y) for x in range(size_x) for y in range(size_y)]
    faces = [(x, y) for y in (-1, size_y) for x in range(size_x)]
    rows = -(-(cells + 2 * size_x) // 128) * 128
    along_y = np.zeros((rows, cells), np.float32)
    for row, (near_x, near_y) in enumerate(own + faces):
        for col, (x, y) in enumerate(own):
            if x == near_x:
                along_y[row, col] = weight(y - near_y, 2.0)
    along_x = np.zeros((3, cells, cells), np.float32)
    for n, shift in enumerate((0, -size_x, size_x)):
        for row, (near_x, near_y) in enumerate(own):
            for col, (x, y) in enumerate(own):
                if y == near_y:
                    along_x[n, row, col] = weight(x - near_x - shift, 2.0)
    return np.concatenate([along_y, along_x.reshape(3 * cells, cells)], 0)


def inside(a, b):
    gx, gy = lax.axis_index("gx"), lax.axis_index("gy")
    ok = None
    for at, d, count in ((gx, a, lax.axis_size("gx")), (gy, b, lax.axis_size("gy"))):
        if d:
            here = at > 0 if d < 0 else at < count - 1
            ok = here if ok is None else jnp.logical_and(ok, here)
    return ok


def when(condition):
    return (lambda f: f()) if condition is None else pl.when(condition)


def device_at(a, b, c):
    device = {}
    if a:
        device["gx"] = lax.axis_index("gx") + a
    if b:
        device["gy"] = lax.axis_index("gy") + b
    if c:
        device["gz"] = 1 - lax.axis_index("gz")
    return device


def greet_around():
    barrier = pltpu.get_barrier_semaphore()
    total = jnp.int32(greet_reduction())
    for a, b, c in NEAR:
        if b and c:
            continue
        there = inside(a, b)

        @when(there)
        def _(a=a, b=b, c=c):
            pl.semaphore_signal(barrier, inc=1, device_id=device_at(a, b, c), device_id_type=MESH)

        total = total + (1 if there is None else jnp.where(there, 1, 0))
    return total


def vouch(far_sem):
    total = jnp.int32(3)
    for _, device in places_along("y"):
        pl.semaphore_signal(far_sem, inc=1, device_id=device, device_id_type=MESH)
    for b in (-1, 1):
        there = inside(0, b)

        @when(there)
        def _(b=b):
            pl.semaphore_signal(far_sem, inc=1, device_id=device_at(0, b, 0), device_id_type=MESH)

        total = total + jnp.where(there, 1, 0)
    return total


class Halo:
    def __init__(self, send, recv):
        self.send, self.recv, self.count, self.all = send, recv, 0, []

    def add(self, side, src, dst):
        a, b, c = side
        copy = pltpu.make_async_remote_copy(
            src_ref=src, dst_ref=dst, send_sem=self.send.at[self.count], recv_sem=self.recv.at[self.count],
            device_id=device_at(-a, -b, c), device_id_type=MESH)
        self.count += 1
        entry = (copy, inside(-a, -b), inside(a, b))
        self.all.append(entry)
        return entry

    def finish(self):
        for copy, sends, _ in self.all:
            when(sends)(copy.wait_send)


def begin(entries):
    for copy, sends, _ in entries:
        when(sends)(copy.start)


def arrive(entries):
    for copy, _, receives in entries:
        when(receives)(copy.wait_recv)


def zero_unless(condition, refs):
    if condition is None:
        return

    @pl.when(jnp.logical_not(condition))
    def _():
        for ref in refs:
            ref[...] = jnp.zeros(ref.shape, ref.dtype)


def kernel(scale, sizes, v_ref, m_hbm, t_hbm, w_hbm, out, m_ref, w_ref,
           e, t, ztile, zl, zn, cz, cn, faces, kall, spans, coef, u, ybuf, acc, blocks,
           own_sem, v_send, v_recv, k_send, k_recv, far_sem, *reduce_bufs):
    nx, ny, nz = sizes
    columns = e.shape[2]
    gz = lax.axis_index("gz")
    hy = ny // 2 * nz
    block = nz + hy + 16
    cells = nx * ny
    low, high = pl.ds(nz, hy), pl.ds(block, hy)
    own = [pltpu.make_async_copy(v_ref.at[:, :hy], e.at[pl.ds(1, nx), low], own_sem.at[0]),
           pltpu.make_async_copy(v_ref.at[:, hy:], e.at[pl.ds(1, nx), high], own_sem.at[1]),
           pltpu.make_async_copy(t_hbm.at[gz], t, own_sem.at[2])]
    z_first = pl.multiple_of((nz - 16) * (1 - gz), 16)
    tiles = [pltpu.make_async_copy(v_ref.at[:, pl.ds(y * nz + z_first, 16)], ztile.at[y], own_sem.at[3 + y])
             for y in range(ny)]
    own += [pltpu.make_async_copy(w_hbm, w_ref, own_sem.at[3 + ny])]
    material_in = pltpu.make_async_copy(m_hbm, m_ref, own_sem.at[4 + ny])
    for copy in [material_in] + tiles + own:
        copy.start()
    total = greet_around()
    material_in.wait()

    kappa = m_ref[0]
    for n, y in enumerate((0, ny - 1)):
        faces[n] = jnp.concatenate([kappa[x * ny + y:x * ny + y + 1] for x in range(nx)], 0)
    kall[0, :cells] = kappa

    for copy in tiles:
        copy.wait()

    def extract(at):
        def edge_row(x, y):
            return ztile[y, x].astype(jnp.float32)[at:at + 1]

        for q in range(nx // 2):
            rows = [edge_row(2 * q + n // ny, n % ny) for n in range(2 * ny)]
            zl[q] = jnp.concatenate(rows, 0).astype(zl.dtype)
        for n, y in enumerate((0, ny - 1)):
            cz[n] = jnp.concatenate([edge_row(x, y) for x in range(nx)], 0).astype(cz.dtype)

    pl.when(gz == 0)(functools.partial(extract, 15))
    pl.when(gz == 1)(functools.partial(extract, 0))

    pl.semaphore_wait(pltpu.get_barrier_semaphore(), total)
    vouched = vouch(far_sem)

    kh = Halo(k_send, k_recv)
    which = {-1: 0, 1: 1}
    y_face = {-1: 1, 1: 0}
    def exchange_material(sides):
        for a, b, c in sides:
            if b == 0:
                src, dst = m_ref.at[0], kall.at[c, pl.ds(0, cells)]
            else:
                src, dst = faces.at[y_face[b]], kall.at[c, pl.ds(cells + which[b] * nx, nx)]
            begin([kh.add((a, b, c), src, dst)])
            zero_unless(inside(a, b), [dst])

    exchange_material([side for side in SIDES if not (side[1] and side[2])])
    used = cells + 2 * nx
    for c in range(2):
        kall[c, used:] = jnp.zeros((kall.shape[1] - used, nz), jnp.float32)

    vh = Halo(v_send, v_recv)
    steps = nx // STEP
    waits = [[] for _ in range(steps)]
    y_planes = [[(2 * i + 2, 2 * i + 4)] for i in range(steps - 1)] + [[]]
    y_planes[0] = [(0, 2), (2, 4)]
    y_planes[1].append((nx - 1, nx))
    y_planes[steps - 2] = [(nx - 2, nx - 1)]
    z_pairs = [[i + 1] for i in range(steps - 2)] + [[], []]
    z_pairs[0] = [0, 1]
    z_pairs[1].append(nx // 2 - 1)
    y_src = {-1: pl.ds((ny - 1) * nz, nz), 1: pl.ds(0, nz)}
    y_dst = {-1: pl.ds(0, nz), 1: pl.ds(block + hy, nz)}

    def y_chunk(i, planes=None):
        for first, last in planes or y_planes[i]:
            made = [vh.add((0, b, 0), v_ref.at[pl.ds(first, last - first), y_src[b]],
                           e.at[pl.ds(first + 1, last - first), y_dst[b]]) for b in (-1, 1)]
            waits[i].extend(made)
            begin(made)

    def z_chunk(i):
        for pair in z_pairs[i]:
            made = [vh.add((0, 0, 1), zl.at[pair], zn.at[pair])]
            waits[i].extend(made)
            begin(made)

    far = [(a, b, c) for a, b, c in SIDES if b and c]
    z_chunk(0)
    y_chunk(0, y_planes[0][:1])
    pl.semaphore_wait(far_sem, vouched)
    exchange_material(far)
    corners = [vh.add((0, b, 1), cz.at[y_face[b]], cn.at[which[b]]) for b in (-1, 1)]
    waits[0].extend(corners)
    begin(corners)
    y_chunk(0, y_planes[0][1:])
    for i in range(1, steps):
        z_chunk(i)
        y_chunk(i)
    x_forward = {}
    for a, mine, there in ((1, 0, nx + 1), (-1, nx - 1, 0)):
        early = [vh.add((a, 0, 0), v_ref.at[mine, pl.ds(0, hy)], e.at[there, low]),
                 vh.add((a, 0, 0), v_ref.at[mine, pl.ds(hy, hy)], e.at[there, high])]
        begin(early)
        x_forward[a] = [vh.add((a, 0, 0), e.at[mine + 1, rows], e.at[there, rows])
                        for rows in (pl.ds(0, nz), pl.ds(nz + hy, 16), pl.ds(block + hy, nz + 16))]
        waits[steps - 1].extend(early + x_forward[a])
    for a, at in ((-1, 0), (1, nx + 1)):
        zero_unless(inside(a, 0), [e.at[at]])
    for b in (-1, 1):
        zero_unless(inside(0, b), [e.at[pl.ds(1, nx), y_dst[b]]])
    for b in (-1, 1):
        zero_unless(inside(0, b), [cn.at[which[b]]])
    acc[...] = jnp.zeros_like(acc)

    row = lax.broadcasted_iota(jnp.int32, (nz, nz), 0)
    col = lax.broadcasted_iota(jnp.int32, (nz, nz), 1)
    exact = functools.partial(lax.dot_general, dimension_numbers=(((1,), (1,)), ((), ())),
                              precision=lax.Precision.HIGHEST, preferred_element_type=jnp.float32)
    unit = jnp.where(row == col, 1.0, 0.0)

    def keep(n, field, only=None):
        for i in range(steps) if only is None else only:
            first = (STEP * i + 1) * ny
            coef[n, i] = pltpu.roll(field, (cells - first) % cells, 1)

    flipped = exact(unit, kappa)
    keep(1, flipped * (1.0 / 16.0))
    keep(2, exact(unit, m_ref[1]) * (1.0 / 216.0))

    own[3].wait()
    arrive(kh.all)
    edge_from = jnp.where(gz == 0, nz - 1, 0)
    near_z = jnp.where(jnp.abs(row - col) == 1, 1.0, 0.0) + 2.0 * unit
    across = jnp.where(jnp.logical_and(row == edge_from, col == nz - 1 - edge_from), 1.0, 0.0)
    along_z = exact(near_z, kall[0]) + exact(across, kall[1])
    wide = kall.shape[1]
    plain = functools.partial(jnp.dot, precision=lax.Precision.HIGHEST, preferred_element_type=jnp.float32)
    spans[0] = plain(along_z, w_ref[:wide])

    def diagonal(kappa, field):
        return 2.0 * kappa + (1.0 / 32.0) * field

    inner = plain(spans[0], w_ref[wide:wide + cells])
    keep(0, diagonal(flipped, inner))
    spreads = [kh.add((a, 0, 0), spans.at[0], spans.at[1 + which[a]]) for a in (-1, 1)]
    for a in (-1, 1):
        zero_unless(inside(a, 0), [spans.at[1 + which[a]]])
    for copy in own[:3]:
        copy.wait()

    lane = lax.broadcasted_iota(jnp.int32, (8, columns), 0)

    def fill_edge(x):
        z8 = zn[x // 2].astype(jnp.float32)[8 * (x % 2):8 * (x % 2) + 8]
        corners = [cn[n].astype(jnp.float32)[x:x + 1] for n in range(2)]
        c8 = jnp.where(lane == 0, corners[0], jnp.where(lane == 1, corners[1], 0.0))
        full = jnp.concatenate([z8, c8], 0).astype(e.dtype)
        e[x + 1, block - 16:block] = full
        e[x + 1, 2 * block - 16:] = full

    def taps_of(n, slot):
        cut = hy - nz
        one = jnp.dot(t[n, :cut, :block], u[slot, n, :block], preferred_element_type=jnp.float32)
        two = jnp.dot(t[n, cut:cut + 2 * nz], u[slot, n], preferred_element_type=jnp.float32)
        three = jnp.dot(t[n, cut + 2 * nz:, block:], u[slot, n, block:], preferred_element_type=jnp.float32)
        return jnp.concatenate([one, two, three], 0)

    def coefficient(n, i, j):
        field = coef[n, i]
        tall = [jnp.broadcast_to(field[:, j * ny + y:j * ny + y + 1], (nz, 128)) for y in range(ny)]
        return jnp.concatenate([jnp.concatenate(tall, 0)] * (columns // 128), 1)

    def iteration(i, carry):
        for c in range(steps):
            @pl.when(i == c)
            def _(c=c):
                arrive(waits[c])
                for first, last in y_planes[c]:
                    for x in range(first, last):
                        fill_edge(x)
                if c == 1:
                    begin(spreads)
                if c == 2:
                    begin(x_forward[1])
                if c == 3:
                    begin(x_forward[-1])
                if c == steps - 2:
                    arrive(spreads)
                    field = plain(spans[0], w_ref[wide:wide + cells])
                    for n in (1, 2):
                        field = field + plain(spans[n], w_ref[wide + n * cells:wide + (n + 1) * cells])
                    keep(0, diagonal(exact(unit, m_ref[0]), field), (steps - 1,))

        held = []
        for j in range(STEP):
            x = lax.rem(STEP * i + j + 1, nx)
            here = e[x + 1]
            twice = here + here
            two = e[x] + e[x + 2] + twice
            u[j, 0] = two
            u[j, 1] = two + twice
            v = jnp.concatenate([here[nz:nz + hy], here[block:block + hy]], 0)
            held.append(v)
            rows = slice(j * ny * nz, (j + 1) * ny * nz)
            stiff = coefficient(0, i, j) * v.astype(jnp.float32) - coefficient(1, i, j) * taps_of(0, j)
            ybuf[rows, :columns] = stiff.astype(ybuf.dtype)
            mass = coefficient(2, i, j) * taps_of(1, j)
            ybuf[rows, columns:] = mass.astype(ybuf.dtype)
        acc[...] += lax.dot_general(jnp.concatenate(held, 0), ybuf[...], (((0,), (0,)), ((), ())),
                                    preferred_element_type=jnp.float32)
        return carry

    lax.fori_loop(0, steps, iteration, 0)

    core = lax.axis_index("gx") % 2

    def symmetric(zl_at, core_at):
        some = pl.ds(pl.multiple_of((2 * zl_at + core_at) * 128, 128), 128)
        also = pl.ds(pl.multiple_of((2 * zl_at + core_at) * 128 + columns, 128), 128)
        stiff = ((acc[some, :columns] + acc[:, some].T) * scale).reshape(4, 4, 8, columns)
        mass = ((acc[some, columns:] + acc[:, also].T) * scale).reshape(4, 4, 8, columns)
        upper_rows = lax.broadcasted_iota(jnp.int32, stiff.shape, 2) < 4
        blocks[zl_at, core_at, :, :, 0] = jnp.where(upper_rows, stiff, pltpu.roll(mass, 4, 2))
        blocks[zl_at, core_at, :, :, 1] = jnp.where(upper_rows, pltpu.roll(stiff, 4, 2), mass)

    for zl_at in range(2):
        symmetric(zl_at, 1 - core)
    first = send_across(blocks, reduce_bufs)
    for zl_at in range(2):
        symmetric(zl_at, core)
    reduce_blocks(blocks, out, reduce_bufs, first)
    kh.finish()
    vh.finish()


def coordinates():
    gx, gy, gz = (lax.axis_index(a) for a in AXES)
    return gx // 2, gx % 2, gy // 4, gy % 4, gz


def places_along(axes):
    zl, core, cx, cy, zh = coordinates()
    if axes == "core":
        peer = 1 - core
        return [(peer, {"gx": zl * 2 + peer})]
    me = {"x": cx, "y": cy, "z": zh * 2 + zl}
    found = []
    for k in range(1, 4 ** len(axes)):
        at = dict(me)
        for n, axis in enumerate(axes):
            at[axis] = lax.rem(me[axis] + (k >> 2 * n) % 4, 4)
        device = {}
        if "x" in axes or "y" in axes:
            device["gy"] = at["x"] * 4 + at["y"]
        if "z" in axes:
            device["gx"] = (at["z"] % 2) * 2 + core
            device["gz"] = at["z"] // 2
        peer = tuple(at[axis] for axis in axes)
        found.append((peer if len(axes) > 1 else peer[0], device))
    return found


def greet_reduction():
    barrier = pltpu.get_barrier_semaphore()
    total = 0
    for axis in ("core", "x", "y", "z"):
        for _, device in places_along(axis):
            pl.semaphore_signal(barrier, inc=1, device_id=device, device_id_type=pl.DeviceIdType.MESH)
            total += 1
    return total


def spread(axis, piece, landing, send, recv, base):
    copies = []
    for k, (peer, device) in enumerate(places_along(axis)):
        copy = pltpu.make_async_remote_copy(
            src_ref=piece(peer), dst_ref=landing.at[k],
            send_sem=send.at[base + k], recv_sem=recv.at[base + k],
            device_id=device, device_id_type=pl.DeviceIdType.MESH)
        copy.start()
        copies.append(copy)
    return copies


def gathered(copies, own, landing):
    for copy in copies:
        copy.wait_recv()
    held = own
    for k in range(len(copies)):
        held = held + landing[k]
    return held


def lanes_of(columns):
    return slice(0, columns // 2), slice(columns // 2, columns)


def send_across(r, bufs):
    rc, send, recv = bufs[0], bufs[-2], bufs[-1]
    return [spread("core", lambda p, c=c: r.at[:, p, :, :, :, :, c], rc.at[i], send, recv, i)
            for i, c in enumerate(lanes_of(r.shape[-1]))]


def reduce_blocks(r, out, bufs, first):
    zl, core, cx, cy, zh = coordinates()
    rc, ha, ra1, ha1, ra2, hb, rb1, hb1, rb2, send, recv = bufs
    lanes = lanes_of(r.shape[-1])
    ha[...] = gathered(first[0], r[:, core, :, :, :, :, lanes[0]], rc.at[0])
    a1 = spread("x", lambda p: ha.at[:, p], ra1, send, recv, 2)
    hb[...] = gathered(first[1], r[:, core, :, :, :, :, lanes[1]], rc.at[1])
    b1 = spread("z", lambda p: hb.at[p % 2, :, :, p // 2], rb1, send, recv, 5)
    ha1[...] = gathered(a1, ha[:, cx], ra1)
    a2 = spread("yz", lambda p: ha1.at[p[1] % 2, p[0], p[1] // 2], ra2, send, recv, 8)
    hb1[...] = gathered(b1, hb[zl, :, :, zh], rb1)
    b2 = spread("xy", lambda p: hb1.at[p[0], p[1]], rb2, send, recv, 23)
    out[:, lanes[0]] = gathered(a2, ha1[zl, cy, zh], ra2)
    out[:, lanes[1]] = gathered(b2, hb1[cx, cy], rb2)
    for copy in first[0] + first[1] + a1 + b1 + a2 + b2:
        copy.wait_send()


def reduce_scratch(columns):
    half = columns // 2
    f32 = jnp.float32
    shapes = [(2, 1, 2, 4, 4, 2, 8, half),
              (2, 4, 4, 2, 8, half), (3, 2, 4, 2, 8, half), (2, 4, 2, 8, half), (15, 8, half),
              (2, 4, 4, 2, 8, half), (3, 4, 4, 8, half), (4, 4, 8, half), (15, 8, half)]
    return [pltpu.VMEM(shape, f32) for shape in shapes] + [pltpu.SemaphoreType.DMA((38,))] * 2


def per_device(eigvecs, material):
    nx, ny, nz, columns = eigvecs.shape
    total_cells = nx * ny * nz
    for axis in AXES:
        total_cells *= lax.axis_size(axis)
    hy = ny // 2 * nz
    block = nz + hy + 16
    cells = nx * ny
    taps = jnp.asarray(plane_taps(ny, nz), jnp.bfloat16)
    around = jnp.asarray(material_taps(nx, ny), jnp.float32)
    bf16, f32 = jnp.bfloat16, jnp.float32
    dma = pltpu.SemaphoreType.DMA
    vmem = pl.BlockSpec(memory_space=pltpu.VMEM)
    anywhere = pl.BlockSpec(memory_space=pl.ANY)
    scratch = [
        pltpu.VMEM((2, cells, nz), f32),
        pltpu.VMEM(around.shape, f32),
        pltpu.VMEM((nx + 2, 2 * block, columns), bf16),
        pltpu.VMEM((2, ny * nz, 2 * block), bf16),
        pltpu.VMEM((ny, nx, 16, columns), bf16),
        pltpu.VMEM((nx // 2, 2 * ny, columns), bf16),
        pltpu.VMEM((nx // 2, 2 * ny, columns), bf16),
        pltpu.VMEM((2, nx, columns), bf16),
        pltpu.VMEM((2, nx, columns), bf16),
        pltpu.VMEM((2, nx, nz), f32),
        pltpu.VMEM((2, around.shape[0] - 3 * cells, nz), f32),
        pltpu.VMEM((3, nz, cells), f32),
        pltpu.VMEM((3, nx // STEP, nz, cells), f32),
        pltpu.VMEM((STEP, 2, 2 * block, columns), bf16),
        pltpu.VMEM((STEP * ny * nz, 2 * columns), bf16),
        pltpu.VMEM((columns, 2 * columns), f32),
        pltpu.VMEM((2, 2, 4, 4, 2, 8, columns), f32),
        dma((5 + ny,)), dma((48,)), dma((48,)), dma((7,)), dma((7,)), pltpu.SemaphoreType.REGULAR,
    ] + reduce_scratch(columns)
    both = pl.pallas_call(
        functools.partial(kernel, 0.5 / total_cells, (nx, ny, nz)),
        out_shape=pltpu.VMEM((8, columns), f32),
        in_specs=[anywhere] * 4,
        out_specs=vmem,
        scratch_shapes=scratch,
        compiler_params=pltpu.CompilerParams(
            vmem_limit_bytes=60 * 1024 * 1024, collective_id=0, has_side_effects=True),
    )(eigvecs.reshape(nx, ny * nz, columns), material.reshape(2, cells, nz), taps, around)
    return both[:4], both[4:]


def solution(mesh):
    return jax.shard_map(
        per_device,
        mesh=mesh,
        in_specs=(P("gx", "gy", "gz", None), P(None, "gx", "gy", "gz")),
        out_specs=(P(("gx", "gy", "gz"), None), P(("gx", "gy", "gz"), None)),
        check_vma=False,
    )
```

```python
import functools
import numpy as np
import jax
import jax.numpy as jnp
from jax import lax
from jax.experimental import pallas as pl
from jax.experimental.pallas import tpu as pltpu
from jax.sharding import PartitionSpec as P

AXES = ("gx", "gy", "gz")
MESH = pl.DeviceIdType.MESH
SIDES = [(0, -1, 0), (0, 1, 0), (0, 0, 1), (0, -1, 1), (0, 1, 1)]
NEAR = SIDES + [(-1, 0, 0), (1, 0, 0)]
STEP = 2


def weight(distance, middle):
    return {0: middle, 1: 1.0}.get(abs(distance), 0.0)


def own_row(y, size_y, size_z):
    half = size_y // 2
    if y < half:
        return size_z * (y + 1)
    return size_z * (half + 1) + 16 + size_z * (y - half)


def plane_taps(size_y, size_z):
    half = size_y // 2
    block = size_z * (half + 1) + 16
    taps = np.zeros((2, 2, size_y * size_z, 2 * block), np.float32)
    for side in range(2):
        edge = size_z - 1 if side == 0 else 0
        for n, middle in enumerate((2.0, 4.0)):
            line = np.array([[weight(z - o, middle) for z in range(size_z)] for o in range(size_z)])
            for y in range(size_y):
                rows = slice(y * size_z, (y + 1) * size_z)
                for near in (y - 1, y, y + 1):
                    w = weight(near - y, middle)
                    if near < 0:
                        first = 0
                    else:
                        first = own_row(near, size_y, size_z)
                    taps[side, n, rows, first:first + size_z] = w * line
                    column = near if 0 <= near < size_y else (size_y if near < 0 else size_y + 1)
                    base = (block if near < half else 2 * block) - 16
                    taps[side, n, y * size_z + edge, base + column] = w
    return taps


def material_taps(size_x, size_y):
    cells = size_x * size_y
    own = [(x, y) for x in range(size_x) for y in range(size_y)]
    faces = [(x, y) for y in (-1, size_y) for x in range(size_x)]
    rows = -(-(cells + 2 * size_x) // 128) * 128
    along_y = np.zeros((rows, cells), np.float32)
    for row, (near_x, near_y) in enumerate(own + faces):
        for col, (x, y) in enumerate(own):
            if x == near_x:
                along_y[row, col] = weight(y - near_y, 2.0)
    along_x = np.zeros((3, cells, cells), np.float32)
    for n, shift in enumerate((0, -size_x, size_x)):
        for row, (near_x, near_y) in enumerate(own):
            for col, (x, y) in enumerate(own):
                if y == near_y:
                    along_x[n, row, col] = weight(x - near_x - shift, 2.0)
    return np.concatenate([along_y, along_x.reshape(3 * cells, cells)], 0)


def inside(a, b):
    gx, gy = lax.axis_index("gx"), lax.axis_index("gy")
    ok = None
    for at, d, count in ((gx, a, lax.axis_size("gx")), (gy, b, lax.axis_size("gy"))):
        if d:
            here = at > 0 if d < 0 else at < count - 1
            ok = here if ok is None else jnp.logical_and(ok, here)
    return ok


def when(condition):
    return (lambda f: f()) if condition is None else pl.when(condition)


def device_at(a, b, c):
    device = {}
    if a:
        device["gx"] = lax.axis_index("gx") + a
    if b:
        device["gy"] = lax.axis_index("gy") + b
    if c:
        device["gz"] = 1 - lax.axis_index("gz")
    return device


def greet_around():
    barrier = pltpu.get_barrier_semaphore()
    total = jnp.int32(0)
    for a, b, c in NEAR:
        if b and c:
            continue
        there = inside(a, b)

        @when(there)
        def _(a=a, b=b, c=c):
            pl.semaphore_signal(barrier, inc=1, device_id=device_at(a, b, c), device_id_type=MESH)

        total = total + (1 if there is None else jnp.where(there, 1, 0))
    return total + greet_reduction()


def vouch(far_sem):
    total = jnp.int32(3)
    for _, device in places_along("y"):
        pl.semaphore_signal(far_sem, inc=1, device_id=device, device_id_type=MESH)
    for b in (-1, 1):
        there = inside(0, b)

        @when(there)
        def _(b=b):
            pl.semaphore_signal(far_sem, inc=1, device_id=device_at(0, b, 0), device_id_type=MESH)

        total = total + jnp.where(there, 1, 0)
    return total


class Halo:
    def __init__(self, send, recv):
        self.send, self.recv, self.count, self.all = send, recv, 0, []

    def add(self, side, src, dst):
        a, b, c = side
        copy = pltpu.make_async_remote_copy(
            src_ref=src, dst_ref=dst, send_sem=self.send.at[self.count], recv_sem=self.recv.at[self.count],
            device_id=device_at(-a, -b, c), device_id_type=MESH)
        self.count += 1
        entry = (copy, inside(-a, -b), inside(a, b))
        self.all.append(entry)
        return entry

    def finish(self):
        for copy, sends, _ in self.all:
            when(sends)(copy.wait_send)


def begin(entries):
    for copy, sends, _ in entries:
        when(sends)(copy.start)


def arrive(entries):
    for copy, _, receives in entries:
        when(receives)(copy.wait_recv)


def zero_unless(condition, refs):
    if condition is None:
        return

    @pl.when(jnp.logical_not(condition))
    def _():
        for ref in refs:
            ref[...] = jnp.zeros(ref.shape, ref.dtype)


def kernel(scale, sizes, v_ref, m_hbm, t_hbm, w_hbm, out, m_ref, w_ref,
           e, t, ztile, zl, zn, cz, cn, faces, kall, spans, coef, u, ybuf, acc, blocks,
           own_sem, v_send, v_recv, k_send, k_recv, far_sem, *reduce_bufs):
    nx, ny, nz = sizes
    columns = e.shape[2]
    gz = lax.axis_index("gz")
    hy = ny // 2 * nz
    block = nz + hy + 16
    cells = nx * ny
    low, high = pl.ds(nz, hy), pl.ds(block, hy)
    own = [pltpu.make_async_copy(v_ref.at[:, :hy], e.at[pl.ds(1, nx), low], own_sem.at[0]),
           pltpu.make_async_copy(v_ref.at[:, hy:], e.at[pl.ds(1, nx), high], own_sem.at[1]),
           pltpu.make_async_copy(t_hbm.at[gz], t, own_sem.at[2])]
    z_first = pl.multiple_of((nz - 16) * (1 - gz), 16)
    tiles = [pltpu.make_async_copy(v_ref.at[:, pl.ds(y * nz + z_first, 16)], ztile.at[y], own_sem.at[3 + y])
             for y in range(ny)]
    own += [pltpu.make_async_copy(w_hbm, w_ref, own_sem.at[3 + ny])]
    material_in = pltpu.make_async_copy(m_hbm, m_ref, own_sem.at[4 + ny])
    for copy in [material_in] + tiles + own:
        copy.start()
    total = greet_around()
    material_in.wait()

    kappa = m_ref[0]
    for n, y in enumerate((0, ny - 1)):
        faces[n] = jnp.concatenate([kappa[x * ny + y:x * ny + y + 1] for x in range(nx)], 0)
    kall[0, :cells] = kappa

    for copy in tiles:
        copy.wait()

    def extract(at):
        def edge_row(x, y):
            return ztile[y, x].astype(jnp.float32)[at:at + 1]

        for q in range(nx // 2):
            rows = [edge_row(2 * q + n // ny, n % ny) for n in range(2 * ny)]
            zl[q] = jnp.concatenate(rows, 0).astype(zl.dtype)
        for n, y in enumerate((0, ny - 1)):
            cz[n] = jnp.concatenate([edge_row(x, y) for x in range(nx)], 0).astype(cz.dtype)

    pl.when(gz == 0)(functools.partial(extract, 15))
    pl.when(gz == 1)(functools.partial(extract, 0))

    pl.semaphore_wait(pltpu.get_barrier_semaphore(), total)
    vouched = vouch(far_sem)

    kh = Halo(k_send, k_recv)
    which = {-1: 0, 1: 1}
    y_face = {-1: 1, 1: 0}
    def exchange_material(sides):
        for a, b, c in sides:
            if b == 0:
                src, dst = m_ref.at[0], kall.at[c, pl.ds(0, cells)]
            else:
                src, dst = faces.at[y_face[b]], kall.at[c, pl.ds(cells + which[b] * nx, nx)]
            begin([kh.add((a, b, c), src, dst)])
            zero_unless(inside(a, b), [dst])

    exchange_material([side for side in SIDES if not (side[1] and side[2])])
    used = cells + 2 * nx
    for c in range(2):
        kall[c, used:] = jnp.zeros((kall.shape[1] - used, nz), jnp.float32)

    vh = Halo(v_send, v_recv)
    steps = nx // STEP
    waits = [[] for _ in range(steps)]
    y_planes = [[(2 * i + 2, 2 * i + 4)] for i in range(steps - 1)] + [[]]
    y_planes[0] = [(0, 2), (2, 4)]
    y_planes[1].append((nx - 1, nx))
    y_planes[steps - 2] = [(nx - 2, nx - 1)]
    z_pairs = [[i + 1] for i in range(steps - 2)] + [[], []]
    z_pairs[0] = [0, 1]
    z_pairs[1].append(nx // 2 - 1)
    y_src = {-1: pl.ds((ny - 1) * nz, nz), 1: pl.ds(0, nz)}
    y_dst = {-1: pl.ds(0, nz), 1: pl.ds(block + hy, nz)}

    def y_chunk(i, planes=None):
        for first, last in planes or y_planes[i]:
            made = [vh.add((0, b, 0), v_ref.at[pl.ds(first, last - first), y_src[b]],
                           e.at[pl.ds(first + 1, last - first), y_dst[b]]) for b in (-1, 1)]
            waits[i].extend(made)
            begin(made)

    def z_chunk(i):
        for pair in z_pairs[i]:
            made = [vh.add((0, 0, 1), zl.at[pair], zn.at[pair])]
            waits[i].extend(made)
            begin(made)

    far = [(a, b, c) for a, b, c in SIDES if b and c]
    z_chunk(0)
    y_chunk(0, y_planes[0][:1])
    pl.semaphore_wait(far_sem, vouched)
    exchange_material(far)
    corners = [vh.add((0, b, 1), cz.at[y_face[b]], cn.at[which[b]]) for b in (-1, 1)]
    waits[0].extend(corners)
    begin(corners)
    y_chunk(0, y_planes[0][1:])
    for i in range(1, steps):
        z_chunk(i)
        y_chunk(i)
    x_forward = {}
    for a, mine, there in ((1, 0, nx + 1), (-1, nx - 1, 0)):
        early = [vh.add((a, 0, 0), v_ref.at[mine, pl.ds(0, hy)], e.at[there, low]),
                 vh.add((a, 0, 0), v_ref.at[mine, pl.ds(hy, hy)], e.at[there, high])]
        begin(early)
        x_forward[a] = [vh.add((a, 0, 0), e.at[mine + 1, rows], e.at[there, rows])
                        for rows in (pl.ds(0, nz), pl.ds(nz + hy, 16), pl.ds(block + hy, nz + 16))]
        waits[steps - 1].extend(early + x_forward[a])
    for a, at in ((-1, 0), (1, nx + 1)):
        zero_unless(inside(a, 0), [e.at[at]])
    for b in (-1, 1):
        zero_unless(inside(0, b), [e.at[pl.ds(1, nx), y_dst[b]]])
    for b in (-1, 1):
        zero_unless(inside(0, b), [cn.at[which[b]]])
    acc[...] = jnp.zeros_like(acc)

    row = lax.broadcasted_iota(jnp.int32, (nz, nz), 0)
    col = lax.broadcasted_iota(jnp.int32, (nz, nz), 1)
    exact = functools.partial(lax.dot_general, dimension_numbers=(((1,), (1,)), ((), ())),
                              precision=lax.Precision.HIGHEST, preferred_element_type=jnp.float32)
    unit = jnp.where(row == col, 1.0, 0.0)

    def keep(n, field, only=None):
        for i in range(steps) if only is None else only:
            first = (STEP * i + 1) * ny
            coef[n, i] = pltpu.roll(field, (cells - first) % cells, 1)

    flipped = exact(unit, kappa)
    keep(1, flipped * (1.0 / 16.0))
    keep(2, exact(unit, m_ref[1]) * (1.0 / 216.0))

    own[3].wait()
    arrive(kh.all)
    edge_from = jnp.where(gz == 0, nz - 1, 0)
    near_z = jnp.where(jnp.abs(row - col) == 1, 1.0, 0.0) + 2.0 * unit
    across = jnp.where(jnp.logical_and(row == edge_from, col == nz - 1 - edge_from), 1.0, 0.0)
    along_z = exact(near_z, kall[0]) + exact(across, kall[1])
    wide = kall.shape[1]
    plain = functools.partial(jnp.dot, precision=lax.Precision.HIGHEST, preferred_element_type=jnp.float32)
    spans[0] = plain(along_z, w_ref[:wide])

    def diagonal(kappa, field):
        return 2.0 * kappa + (1.0 / 32.0) * field

    inner = plain(spans[0], w_ref[wide:wide + cells])
    keep(0, diagonal(flipped, inner))
    spreads = [kh.add((a, 0, 0), spans.at[0], spans.at[1 + which[a]]) for a in (-1, 1)]
    for a in (-1, 1):
        zero_unless(inside(a, 0), [spans.at[1 + which[a]]])
    for copy in own[:3]:
        copy.wait()

    lane = lax.broadcasted_iota(jnp.int32, (8, columns), 0)

    def fill_edge(x):
        z8 = zn[x // 2].astype(jnp.float32)[8 * (x % 2):8 * (x % 2) + 8]
        corners = [cn[n].astype(jnp.float32)[x:x + 1] for n in range(2)]
        c8 = jnp.where(lane == 0, corners[0], jnp.where(lane == 1, corners[1], 0.0))
        full = jnp.concatenate([z8, c8], 0).astype(e.dtype)
        e[x + 1, block - 16:block] = full
        e[x + 1, 2 * block - 16:] = full

    def taps_of(n, slot):
        cut = hy - nz
        one = jnp.dot(t[n, :cut, :block], u[slot, n, :block], preferred_element_type=jnp.float32)
        two = jnp.dot(t[n, cut:cut + 2 * nz], u[slot, n], preferred_element_type=jnp.float32)
        three = jnp.dot(t[n, cut + 2 * nz:, block:], u[slot, n, block:], preferred_element_type=jnp.float32)
        return jnp.concatenate([one, two, three], 0)

    def coefficient(n, i, j):
        field = coef[n, i]
        tall = [jnp.broadcast_to(field[:, j * ny + y:j * ny + y + 1], (nz, 128)) for y in range(ny)]
        return jnp.concatenate([jnp.concatenate(tall, 0)] * (columns // 128), 1)

    def iteration(i, carry):
        for c in range(steps):
            @pl.when(i == c)
            def _(c=c):
                arrive(waits[c])
                for first, last in y_planes[c]:
                    for x in range(first, last):
                        fill_edge(x)
                if c == 1:
                    begin(spreads)
                if c == 2:
                    begin(x_forward[1])
                if c == 3:
                    begin(x_forward[-1])
                if c == steps - 2:
                    arrive(spreads)
                    field = plain(spans[0], w_ref[wide:wide + cells])
                    for n in (1, 2):
                        field = field + plain(spans[n], w_ref[wide + n * cells:wide + (n + 1) * cells])
                    keep(0, diagonal(exact(unit, m_ref[0]), field), (steps - 1,))

        held = []
        for j in range(STEP):
            x = lax.rem(STEP * i + j + 1, nx)
            here = e[x + 1]
            twice = here + here
            two = e[x] + e[x + 2] + twice
            u[j, 0] = two
            u[j, 1] = two + twice
            v = jnp.concatenate([here[nz:nz + hy], here[block:block + hy]], 0)
            held.append(v)
            rows = slice(j * ny * nz, (j + 1) * ny * nz)
            stiff = coefficient(0, i, j) * v.astype(jnp.float32) - coefficient(1, i, j) * taps_of(0, j)
            ybuf[rows, :columns] = stiff.astype(ybuf.dtype)
            mass = coefficient(2, i, j) * taps_of(1, j)
            ybuf[rows, columns:] = mass.astype(ybuf.dtype)
        acc[...] += lax.dot_general(jnp.concatenate(held, 0), ybuf[...], (((0,), (0,)), ((), ())),
                                    preferred_element_type=jnp.float32)
        return carry

    plan = plan_reduction(blocks, reduce_bufs)
    lax.fori_loop(0, steps, iteration, 0)

    core = plan[0][1]

    def symmetric(zl_at, core_at):
        some = pl.ds(pl.multiple_of((2 * zl_at + core_at) * 128, 128), 128)
        also = pl.ds(pl.multiple_of((2 * zl_at + core_at) * 128 + columns, 128), 128)
        stiff = ((acc[some, :columns] + acc[:, some].T) * scale).reshape(4, 4, 8, columns)
        mass = ((acc[some, columns:] + acc[:, also].T) * scale).reshape(4, 4, 8, columns)
        upper_rows = lax.broadcasted_iota(jnp.int32, stiff.shape, 2) < 4
        blocks[zl_at, core_at, :, :, 0] = jnp.where(upper_rows, stiff, pltpu.roll(mass, 4, 2))
        blocks[zl_at, core_at, :, :, 1] = jnp.where(upper_rows, pltpu.roll(stiff, 4, 2), mass)

    for zl_at in range(2):
        symmetric(zl_at, 1 - core)
    launch(plan[1][0] + plan[1][1])
    for zl_at in range(2):
        symmetric(zl_at, core)
    def finish():
        kh.finish()
        vh.finish()

    reduce_blocks(blocks, out, reduce_bufs, plan, finish)


def coordinates():
    gx, gy, gz = (lax.axis_index(a) for a in AXES)
    return gx // 2, gx % 2, gy // 4, gy % 4, gz


def places_along(axes):
    zl, core, cx, cy, zh = coordinates()
    if axes == "core":
        peer = 1 - core
        return [(peer, {"gx": zl * 2 + peer})]
    me = {"x": cx, "y": cy, "z": zh * 2 + zl}
    found = []
    for k in range(1, 4 ** len(axes)):
        at = dict(me)
        for n, axis in enumerate(axes):
            at[axis] = lax.rem(me[axis] + (k >> 2 * n) % 4, 4)
        device = {}
        if "x" in axes or "y" in axes:
            device["gy"] = at["x"] * 4 + at["y"]
        if "z" in axes:
            device["gx"] = (at["z"] % 2) * 2 + core
            device["gz"] = at["z"] // 2
        peer = tuple(at[axis] for axis in axes)
        found.append((peer if len(axes) > 1 else peer[0], device))
    return found


def greet_reduction():
    barrier = pltpu.get_barrier_semaphore()
    total = 0
    for axis in ("core", "x", "y", "z"):
        for _, device in places_along(axis):
            pl.semaphore_signal(barrier, inc=1, device_id=device, device_id_type=pl.DeviceIdType.MESH)
            total += 1
    return total


def spread(axis, piece, landing, send, recv, base):
    copies = []
    for k, (peer, device) in enumerate(places_along(axis)):
        copy = pltpu.make_async_remote_copy(
            src_ref=piece(peer), dst_ref=landing.at[k],
            send_sem=send.at[base + k], recv_sem=recv.at[base + k],
            device_id=device, device_id_type=pl.DeviceIdType.MESH)
        copies.append(copy)
    return copies


def gathered(copies, own, landing):
    for copy in copies:
        copy.wait_recv()
    held = own
    for k in range(len(copies)):
        held = held + landing[k]
    return held


def lanes_of(columns):
    return slice(0, columns // 2), slice(columns // 2, columns)


def launch(copies):
    for copy in copies:
        copy.start()


def settle(copies):
    for copy in copies:
        copy.wait_send()


def plan_reduction(r, bufs):
    rc, ha, ra1, ha1, ra2, hb, rb1, hb1, rb2, send, recv = bufs
    first = [spread("core", lambda p, c=c: r.at[:, p, :, :, :, :, c], rc.at[i], send, recv, i)
             for i, c in enumerate(lanes_of(r.shape[-1]))]
    a1 = spread("x", lambda p: ha.at[:, p], ra1, send, recv, 2)
    b1 = spread("z", lambda p: hb.at[p % 2, :, :, p // 2], rb1, send, recv, 5)
    a2 = spread("yz", lambda p: ha1.at[p[1] % 2, p[0], p[1] // 2], ra2, send, recv, 8)
    b2 = spread("xy", lambda p: hb1.at[p[0], p[1]], rb2, send, recv, 23)
    return coordinates(), first, a1, b1, a2, b2


def reduce_blocks(r, out, bufs, plan, finish):
    rc, ha, ra1, ha1, ra2, hb, rb1, hb1, rb2, send, recv = bufs
    (zl, core, cx, cy, zh), first, a1, b1, a2, b2 = plan
    lanes = lanes_of(r.shape[-1])
    ha[...] = gathered(first[0], r[:, core, :, :, :, :, lanes[0]], rc.at[0])
    launch(a1)
    hb[...] = gathered(first[1], r[:, core, :, :, :, :, lanes[1]], rc.at[1])
    launch(b1)
    finish()
    settle(first[0] + first[1])
    ha1[...] = gathered(a1, ha[:, cx], ra1)
    launch(a2)
    hb1[...] = gathered(b1, hb[zl, :, :, zh], rb1)
    launch(b2)
    settle(a1 + b1)
    out[:, lanes[0]] = gathered(a2, ha1[zl, cy, zh], ra2)
    settle(a2)
    out[:, lanes[1]] = gathered(b2, hb1[cx, cy], rb2)
    settle(b2)


def reduce_scratch(columns):
    half = columns // 2
    f32 = jnp.float32
    shapes = [(2, 1, 2, 4, 4, 2, 8, half),
              (2, 4, 4, 2, 8, half), (3, 2, 4, 2, 8, half), (2, 4, 2, 8, half), (15, 8, half),
              (2, 4, 4, 2, 8, half), (3, 4, 4, 8, half), (4, 4, 8, half), (15, 8, half)]
    return [pltpu.VMEM(shape, f32) for shape in shapes] + [pltpu.SemaphoreType.DMA((38,))] * 2


def per_device(eigvecs, material):
    nx, ny, nz, columns = eigvecs.shape
    total_cells = nx * ny * nz
    for axis in AXES:
        total_cells *= lax.axis_size(axis)
    hy = ny // 2 * nz
    block = nz + hy + 16
    cells = nx * ny
    taps = jnp.asarray(plane_taps(ny, nz), jnp.bfloat16)
    around = jnp.asarray(material_taps(nx, ny), jnp.float32)
    bf16, f32 = jnp.bfloat16, jnp.float32
    dma = pltpu.SemaphoreType.DMA
    vmem = pl.BlockSpec(memory_space=pltpu.VMEM)
    anywhere = pl.BlockSpec(memory_space=pl.ANY)
    scratch = [
        pltpu.VMEM((2, cells, nz), f32),
        pltpu.VMEM(around.shape, f32),
        pltpu.VMEM((nx + 2, 2 * block, columns), bf16),
        pltpu.VMEM((2, ny * nz, 2 * block), bf16),
        pltpu.VMEM((ny, nx, 16, columns), bf16),
        pltpu.VMEM((nx // 2, 2 * ny, columns), bf16),
        pltpu.VMEM((nx // 2, 2 * ny, columns), bf16),
        pltpu.VMEM((2, nx, columns), bf16),
        pltpu.VMEM((2, nx, columns), bf16),
        pltpu.VMEM((2, nx, nz), f32),
        pltpu.VMEM((2, around.shape[0] - 3 * cells, nz), f32),
        pltpu.VMEM((3, nz, cells), f32),
        pltpu.VMEM((3, nx // STEP, nz, cells), f32),
        pltpu.VMEM((STEP, 2, 2 * block, columns), bf16),
        pltpu.VMEM((STEP * ny * nz, 2 * columns), bf16),
        pltpu.VMEM((columns, 2 * columns), f32),
        pltpu.VMEM((2, 2, 4, 4, 2, 8, columns), f32),
        dma((5 + ny,)), dma((48,)), dma((48,)), dma((7,)), dma((7,)), pltpu.SemaphoreType.REGULAR,
    ] + reduce_scratch(columns)
    both = pl.pallas_call(
        functools.partial(kernel, 0.5 / total_cells, (nx, ny, nz)),
        out_shape=pltpu.VMEM((8, columns), f32),
        in_specs=[anywhere] * 4,
        out_specs=vmem,
        scratch_shapes=scratch,
        compiler_params=pltpu.CompilerParams(
            vmem_limit_bytes=60 * 1024 * 1024, collective_id=0, has_side_effects=True),
    )(eigvecs.reshape(nx, ny * nz, columns), material.reshape(2, cells, nz), taps, around)
    return both[:4], both[4:]


def solution(mesh):
    return jax.shard_map(
        per_device,
        mesh=mesh,
        in_specs=(P("gx", "gy", "gz", None), P(None, "gx", "gy", "gz")),
        out_specs=(P(("gx", "gy", "gz"), None), P(("gx", "gy", "gz"), None)),
        check_vma=False,
    )
```

```python
import functools
import numpy as np
import jax
import jax.numpy as jnp
from jax import lax
from jax.experimental import pallas as pl
from jax.experimental.pallas import tpu as pltpu
from jax.sharding import PartitionSpec as P

AXES = ("gx", "gy", "gz")
MESH = pl.DeviceIdType.MESH
SIDES = [(0, -1, 0), (0, 1, 0), (0, 0, 1), (0, -1, 1), (0, 1, 1)]
NEAR = SIDES + [(-1, 0, 0), (1, 0, 0)]
STEP = 2


def weight(distance, middle):
    return {0: middle, 1: 1.0}.get(abs(distance), 0.0)


def own_row(y, size_y, size_z):
    half = size_y // 2
    if y < half:
        return size_z * (y + 1)
    return size_z * (half + 1) + 16 + size_z * (y - half)


def plane_taps(size_y, size_z):
    half = size_y // 2
    block = size_z * (half + 1) + 16
    taps = np.zeros((2, 2, size_y * size_z, 2 * block), np.float32)
    for side in range(2):
        edge = size_z - 1 if side == 0 else 0
        for n, middle in enumerate((2.0, 4.0)):
            line = np.array([[weight(z - o, middle) for z in range(size_z)] for o in range(size_z)])
            for y in range(size_y):
                rows = slice(y * size_z, (y + 1) * size_z)
                for near in (y - 1, y, y + 1):
                    w = weight(near - y, middle)
                    if near < 0:
                        first = 0
                    else:
                        first = own_row(near, size_y, size_z)
                    taps[side, n, rows, first:first + size_z] = w * line
                    column = near if 0 <= near < size_y else (size_y if near < 0 else size_y + 1)
                    base = (block if near < half else 2 * block) - 16
                    taps[side, n, y * size_z + edge, base + column] = w
    return taps


def material_taps(size_x, size_y):
    cells = size_x * size_y
    own = [(x, y) for x in range(size_x) for y in range(size_y)]
    faces = [(x, y) for y in (-1, size_y) for x in range(size_x)]
    rows = -(-(cells + 2 * size_x) // 128) * 128
    along_y = np.zeros((rows, cells), np.float32)
    for row, (near_x, near_y) in enumerate(own + faces):
        for col, (x, y) in enumerate(own):
            if x == near_x:
                along_y[row, col] = weight(y - near_y, 2.0)
    along_x = np.zeros((3, cells, cells), np.float32)
    for n, shift in enumerate((0, -size_x, size_x)):
        for row, (near_x, near_y) in enumerate(own):
            for col, (x, y) in enumerate(own):
                if y == near_y:
                    along_x[n, row, col] = weight(x - near_x - shift, 2.0)
    return np.concatenate([along_y, along_x.reshape(3 * cells, cells)], 0)


def inside(a, b):
    gx, gy = lax.axis_index("gx"), lax.axis_index("gy")
    ok = None
    for at, d, count in ((gx, a, lax.axis_size("gx")), (gy, b, lax.axis_size("gy"))):
        if d:
            here = at > 0 if d < 0 else at < count - 1
            ok = here if ok is None else jnp.logical_and(ok, here)
    return ok


def when(condition):
    return (lambda f: f()) if condition is None else pl.when(condition)


def device_at(a, b, c):
    device = {}
    if a:
        device["gx"] = lax.axis_index("gx") + a
    if b:
        device["gy"] = lax.axis_index("gy") + b
    if c:
        device["gz"] = 1 - lax.axis_index("gz")
    return device


def greet_around():
    barrier = pltpu.get_barrier_semaphore()
    total = jnp.int32(0)
    for a, b, c in NEAR:
        if b and c:
            continue
        there = inside(a, b)

        @when(there)
        def _(a=a, b=b, c=c):
            pl.semaphore_signal(barrier, inc=1, device_id=device_at(a, b, c), device_id_type=MESH)

        total = total + (1 if there is None else jnp.where(there, 1, 0))
    return total + greet_reduction()


def vouch(far_sem):
    total = jnp.int32(3)
    for _, device in places_along("y"):
        pl.semaphore_signal(far_sem, inc=1, device_id=device, device_id_type=MESH)
    for b in (-1, 1):
        there = inside(0, b)

        @when(there)
        def _(b=b):
            pl.semaphore_signal(far_sem, inc=1, device_id=device_at(0, b, 0), device_id_type=MESH)

        total = total + jnp.where(there, 1, 0)
    return total


class Halo:
    def __init__(self, send, recv):
        self.send, self.recv, self.count, self.all = send, recv, 0, []

    def add(self, side, src, dst):
        a, b, c = side
        copy = pltpu.make_async_remote_copy(
            src_ref=src, dst_ref=dst, send_sem=self.send.at[self.count], recv_sem=self.recv.at[self.count],
            device_id=device_at(-a, -b, c), device_id_type=MESH)
        self.count += 1
        entry = (copy, inside(-a, -b), inside(a, b))
        self.all.append(entry)
        return entry

    def finish(self):
        for copy, sends, _ in self.all:
            when(sends)(copy.wait_send)


def begin(entries):
    for copy, sends, _ in entries:
        when(sends)(copy.start)


def arrive(entries):
    for copy, _, receives in entries:
        when(receives)(copy.wait_recv)


def zero_unless(condition, refs):
    if condition is None:
        return

    @pl.when(jnp.logical_not(condition))
    def _():
        for ref in refs:
            ref[...] = jnp.zeros(ref.shape, ref.dtype)


def kernel(scale, sizes, v_ref, m_hbm, t_hbm, w_hbm, out, m_ref, w_ref,
           e, t, ztile, zl, zn, cz, cn, faces, kall, spans, coef, u, ybuf, acc, blocks,
           own_sem, v_send, v_recv, k_send, k_recv, far_sem, *reduce_bufs):
    nx, ny, nz = sizes
    columns = e.shape[2]
    gz = lax.axis_index("gz")
    hy = ny // 2 * nz
    block = nz + hy + 16
    cells = nx * ny
    low, high = pl.ds(nz, hy), pl.ds(block, hy)
    own = [pltpu.make_async_copy(v_ref.at[:, :hy], e.at[pl.ds(1, nx), low], own_sem.at[0]),
           pltpu.make_async_copy(v_ref.at[:, hy:], e.at[pl.ds(1, nx), high], own_sem.at[1]),
           pltpu.make_async_copy(t_hbm.at[gz], t, own_sem.at[2])]
    z_first = pl.multiple_of((nz - 16) * (1 - gz), 16)
    tiles = [pltpu.make_async_copy(v_ref.at[:, pl.ds(y * nz + z_first, 16)], ztile.at[y], own_sem.at[3 + y])
             for y in range(ny)]
    own += [pltpu.make_async_copy(w_hbm, w_ref, own_sem.at[3 + ny])]
    material_in = pltpu.make_async_copy(m_hbm, m_ref, own_sem.at[4 + ny])
    for copy in [material_in] + tiles + own:
        copy.start()
    total = greet_around()
    material_in.wait()

    kappa = m_ref[0]
    for n, y in enumerate((0, ny - 1)):
        faces[n] = jnp.concatenate([kappa[x * ny + y:x * ny + y + 1] for x in range(nx)], 0)
    kall[0, :cells] = kappa

    for copy in tiles:
        copy.wait()

    def extract(at):
        def edge_row(x, y):
            return ztile[y, x].astype(jnp.float32)[at:at + 1]

        for q in range(nx // 2):
            rows = [edge_row(2 * q + n // ny, n % ny) for n in range(2 * ny)]
            zl[q] = jnp.concatenate(rows, 0).astype(zl.dtype)
        for n, y in enumerate((0, ny - 1)):
            cz[n] = jnp.concatenate([edge_row(x, y) for x in range(nx)], 0).astype(cz.dtype)

    pl.when(gz == 0)(functools.partial(extract, 15))
    pl.when(gz == 1)(functools.partial(extract, 0))

    pl.semaphore_wait(pltpu.get_barrier_semaphore(), total)
    vouched = vouch(far_sem)

    kh = Halo(k_send, k_recv)
    which = {-1: 0, 1: 1}
    y_face = {-1: 1, 1: 0}
    def exchange_material(sides):
        for a, b, c in sides:
            if b == 0:
                src, dst = m_ref.at[0], kall.at[c, pl.ds(0, cells)]
            else:
                src, dst = faces.at[y_face[b]], kall.at[c, pl.ds(cells + which[b] * nx, nx)]
            begin([kh.add((a, b, c), src, dst)])
            zero_unless(inside(a, b), [dst])

    exchange_material([side for side in SIDES if not (side[1] and side[2])])
    used = cells + 2 * nx
    for c in range(2):
        kall[c, used:] = jnp.zeros((kall.shape[1] - used, nz), jnp.float32)

    vh = Halo(v_send, v_recv)
    steps = nx // STEP
    waits = [[] for _ in range(steps)]
    y_planes = [[(2 * i + 2, 2 * i + 4)] for i in range(steps - 1)] + [[]]
    y_planes[0] = [(0, 2), (2, 4)]
    y_planes[1].append((nx - 1, nx))
    y_planes[steps - 2] = [(nx - 2, nx - 1)]
    z_pairs = [[i + 1] for i in range(steps - 2)] + [[], []]
    z_pairs[0] = [0, 1]
    z_pairs[1].append(nx // 2 - 1)
    y_src = {-1: pl.ds((ny - 1) * nz, nz), 1: pl.ds(0, nz)}
    y_dst = {-1: pl.ds(0, nz), 1: pl.ds(block + hy, nz)}

    def y_chunk(i, planes=None):
        for first, last in planes or y_planes[i]:
            made = [vh.add((0, b, 0), v_ref.at[pl.ds(first, last - first), y_src[b]],
                           e.at[pl.ds(first + 1, last - first), y_dst[b]]) for b in (-1, 1)]
            waits[i].extend(made)
            begin(made)

    def z_chunk(i):
        for pair in z_pairs[i]:
            made = [vh.add((0, 0, 1), zl.at[pair], zn.at[pair])]
            waits[i].extend(made)
            begin(made)

    far = [(a, b, c) for a, b, c in SIDES if b and c]
    z_chunk(0)
    y_chunk(0, y_planes[0][:1])
    pl.semaphore_wait(far_sem, vouched)
    exchange_material(far)
    corners = [vh.add((0, b, 1), cz.at[y_face[b]], cn.at[which[b]]) for b in (-1, 1)]
    waits[0].extend(corners)
    begin(corners)
    y_chunk(0, y_planes[0][1:])
    for i in range(1, steps):
        z_chunk(i)
        y_chunk(i)
    x_forward = {}
    for a, mine, there in ((1, 0, nx + 1), (-1, nx - 1, 0)):
        early = [vh.add((a, 0, 0), v_ref.at[mine, pl.ds(0, hy)], e.at[there, low]),
                 vh.add((a, 0, 0), v_ref.at[mine, pl.ds(hy, hy)], e.at[there, high])]
        begin(early)
        x_forward[a] = [vh.add((a, 0, 0), e.at[mine + 1, rows], e.at[there, rows])
                        for rows in (pl.ds(0, nz), pl.ds(nz + hy, 16), pl.ds(block + hy, nz + 16))]
        waits[steps - 1].extend(early + x_forward[a])
    for a, at in ((-1, 0), (1, nx + 1)):
        zero_unless(inside(a, 0), [e.at[at]])
    for b in (-1, 1):
        zero_unless(inside(0, b), [e.at[pl.ds(1, nx), y_dst[b]]])
    for b in (-1, 1):
        zero_unless(inside(0, b), [cn.at[which[b]]])
    acc[...] = jnp.zeros_like(acc)

    row = lax.broadcasted_iota(jnp.int32, (nz, nz), 0)
    col = lax.broadcasted_iota(jnp.int32, (nz, nz), 1)
    exact = functools.partial(lax.dot_general, dimension_numbers=(((1,), (1,)), ((), ())),
                              precision=lax.Precision.HIGHEST, preferred_element_type=jnp.float32)
    unit = jnp.where(row == col, 1.0, 0.0)

    def keep(n, field, only=None):
        for i in range(steps) if only is None else only:
            first = (STEP * i + 1) * ny
            coef[n, i] = pltpu.roll(field, (cells - first) % cells, 1)

    flipped = exact(unit, kappa)
    keep(1, flipped * (1.0 / 16.0))
    keep(2, exact(unit, m_ref[1]) * (1.0 / 216.0))

    own[3].wait()
    arrive(kh.all)
    edge_from = jnp.where(gz == 0, nz - 1, 0)
    near_z = jnp.where(jnp.abs(row - col) == 1, 1.0, 0.0) + 2.0 * unit
    across = jnp.where(jnp.logical_and(row == edge_from, col == nz - 1 - edge_from), 1.0, 0.0)
    along_z = exact(near_z, kall[0]) + exact(across, kall[1])
    wide = kall.shape[1]
    plain = functools.partial(jnp.dot, precision=lax.Precision.HIGHEST, preferred_element_type=jnp.float32)
    spans[0] = plain(along_z, w_ref[:wide])

    def diagonal(kappa, field):
        return 2.0 * kappa + (1.0 / 32.0) * field

    inner = plain(spans[0], w_ref[wide:wide + cells])
    keep(0, diagonal(flipped, inner))
    spreads = [kh.add((a, 0, 0), spans.at[0], spans.at[1 + which[a]]) for a in (-1, 1)]
    for a in (-1, 1):
        zero_unless(inside(a, 0), [spans.at[1 + which[a]]])
    for copy in own[:3]:
        copy.wait()

    lane = lax.broadcasted_iota(jnp.int32, (8, columns), 0)

    def fill_edge(x):
        z8 = zn[x // 2].astype(jnp.float32)[8 * (x % 2):8 * (x % 2) + 8]
        corners = [cn[n].astype(jnp.float32)[x:x + 1] for n in range(2)]
        c8 = jnp.where(lane == 0, corners[0], jnp.where(lane == 1, corners[1], 0.0))
        full = jnp.concatenate([z8, c8], 0).astype(e.dtype)
        e[x + 1, block - 16:block] = full
        e[x + 1, 2 * block - 16:] = full

    def taps_of(n, slot):
        cut = hy - nz
        one = jnp.dot(t[n, :cut, :block], u[slot, n, :block], preferred_element_type=jnp.float32)
        two = jnp.dot(t[n, cut:cut + 2 * nz], u[slot, n], preferred_element_type=jnp.float32)
        three = jnp.dot(t[n, cut + 2 * nz:, block:], u[slot, n, block:], preferred_element_type=jnp.float32)
        return jnp.concatenate([one, two, three], 0)

    def coefficient(n, i, j):
        field = coef[n, i]
        tall = [jnp.broadcast_to(field[:, j * ny + y:j * ny + y + 1], (nz, 128)) for y in range(ny)]
        return jnp.concatenate([jnp.concatenate(tall, 0)] * (columns // 128), 1)

    def iteration(i, carry):
        for c in range(steps):
            @pl.when(i == c)
            def _(c=c):
                arrive(waits[c])
                for first, last in y_planes[c]:
                    for x in range(first, last):
                        fill_edge(x)
                if c == 1:
                    begin(spreads)
                if c == 2:
                    begin(x_forward[1])
                if c == 3:
                    begin(x_forward[-1])
                if c == steps - 2:
                    arrive(spreads)
                    field = plain(spans[0], w_ref[wide:wide + cells])
                    for n in (1, 2):
                        field = field + plain(spans[n], w_ref[wide + n * cells:wide + (n + 1) * cells])
                    keep(0, diagonal(exact(unit, m_ref[0]), field), (steps - 1,))

        held = []
        for j in range(STEP):
            x = lax.rem(STEP * i + j + 1, nx)
            here = e[x + 1]
            twice = here + here
            two = e[x] + e[x + 2] + twice
            u[j, 0] = two
            u[j, 1] = two + twice
            v = jnp.concatenate([here[nz:nz + hy], here[block:block + hy]], 0)
            held.append(v)
            rows = slice(j * ny * nz, (j + 1) * ny * nz)
            stiff = coefficient(0, i, j) * v.astype(jnp.float32) - coefficient(1, i, j) * taps_of(0, j)
            ybuf[rows, :columns] = stiff.astype(ybuf.dtype)
            mass = coefficient(2, i, j) * taps_of(1, j)
            ybuf[rows, columns:] = mass.astype(ybuf.dtype)
        acc[...] += lax.dot_general(jnp.concatenate(held, 0), ybuf[...], (((0,), (0,)), ((), ())),
                                    preferred_element_type=jnp.float32)
        return carry

    plan = plan_reduction(blocks, reduce_bufs)
    lax.fori_loop(0, steps, iteration, 0)

    core = plan[0][1]

    def symmetric(zl_at, core_at):
        some = pl.ds(pl.multiple_of((2 * zl_at + core_at) * 128, 128), 128)
        also = pl.ds(pl.multiple_of((2 * zl_at + core_at) * 128 + columns, 128), 128)
        stiff = ((acc[some, :columns] + acc[:, some].T) * scale).reshape(4, 4, 8, columns)
        mass = ((acc[some, columns:] + acc[:, also].T) * scale).reshape(4, 4, 8, columns)
        upper_rows = lax.broadcasted_iota(jnp.int32, stiff.shape, 2) < 4
        blocks[zl_at, core_at, :, :, 0] = jnp.where(upper_rows, stiff, pltpu.roll(mass, 4, 2))
        blocks[zl_at, core_at, :, :, 1] = jnp.where(upper_rows, pltpu.roll(stiff, 4, 2), mass)

    symmetric(0, 1 - core)
    launch(plan[1][0][:1])
    symmetric(1, 1 - core)
    launch(plan[1][0][1:] + plan[1][1])
    for zl_at in range(2):
        symmetric(zl_at, core)
    def finish():
        kh.finish()
        vh.finish()

    reduce_blocks(blocks, out, reduce_bufs, plan, finish)


def coordinates():
    gx, gy, gz = (lax.axis_index(a) for a in AXES)
    return gx // 2, gx % 2, gy // 4, gy % 4, gz


def places_along(axes):
    zl, core, cx, cy, zh = coordinates()
    if axes == "core":
        peer = 1 - core
        return [(peer, {"gx": zl * 2 + peer})]
    me = {"x": cx, "y": cy, "z": zh * 2 + zl}
    found = []
    for k in range(1, 4 ** len(axes)):
        at = dict(me)
        for n, axis in enumerate(axes):
            at[axis] = lax.rem(me[axis] + (k >> 2 * n) % 4, 4)
        device = {}
        if "x" in axes or "y" in axes:
            device["gy"] = at["x"] * 4 + at["y"]
        if "z" in axes:
            device["gx"] = (at["z"] % 2) * 2 + core
            device["gz"] = at["z"] // 2
        peer = tuple(at[axis] for axis in axes)
        found.append((peer if len(axes) > 1 else peer[0], device))
    return found


def greet_reduction():
    barrier = pltpu.get_barrier_semaphore()
    total = 0
    for axis in ("core", "x", "y", "z"):
        for _, device in places_along(axis):
            pl.semaphore_signal(barrier, inc=1, device_id=device, device_id_type=pl.DeviceIdType.MESH)
            total += 1
    return total


def spread(axis, piece, landing, send, recv, base):
    copies = []
    for k, (peer, device) in enumerate(places_along(axis)):
        copy = pltpu.make_async_remote_copy(
            src_ref=piece(peer), dst_ref=landing.at[k],
            send_sem=send.at[base + k], recv_sem=recv.at[base + k],
            device_id=device, device_id_type=pl.DeviceIdType.MESH)
        copies.append(copy)
    return copies


def gathered(copies, own, landing):
    for copy in copies:
        copy.wait_recv()
    held = own
    for k in range(len(copies)):
        held = held + landing[k]
    return held


def lanes_of(columns):
    return slice(0, columns // 2), slice(columns // 2, columns)


def launch(copies):
    for copy in copies:
        copy.start()


def settle(copies):
    for copy in copies:
        copy.wait_send()


def crossed(copies, own, landing):
    for copy in copies:
        copy.wait_recv()
    return own + landing[0]


def plan_reduction(r, bufs):
    rc, ha, ra1, ha1, ra2, hb, rb1, hb1, rb2, send, recv = bufs
    first = [[spread("core", lambda p, c=c, z=z: r.at[z, p, :, :, :, :, c], rc.at[i, :, z], send, recv,
                     i if z == 0 else 38 + i)[0] for z in range(2)] for i, c in enumerate(lanes_of(r.shape[-1]))]
    a1 = spread("x", lambda p: ha.at[:, p], ra1, send, recv, 2)
    b1 = spread("z", lambda p: hb.at[p % 2, :, :, p // 2], rb1, send, recv, 5)
    a2 = spread("yz", lambda p: ha1.at[p[1] % 2, p[0], p[1] // 2], ra2, send, recv, 8)
    b2 = spread("xy", lambda p: hb1.at[p[0], p[1]], rb2, send, recv, 23)
    return coordinates(), first, a1, b1, a2, b2


def reduce_blocks(r, out, bufs, plan, finish):
    rc, ha, ra1, ha1, ra2, hb, rb1, hb1, rb2, send, recv = bufs
    (zl, core, cx, cy, zh), first, a1, b1, a2, b2 = plan
    lanes = lanes_of(r.shape[-1])
    ha[...] = crossed(first[0], r[:, core, :, :, :, :, lanes[0]], rc.at[0])
    launch(a1)
    hb[...] = crossed(first[1], r[:, core, :, :, :, :, lanes[1]], rc.at[1])
    launch(b1)
    finish()
    settle(first[0] + first[1])
    ha1[...] = gathered(a1, ha[:, cx], ra1)
    launch(a2)
    hb1[...] = gathered(b1, hb[zl, :, :, zh], rb1)
    launch(b2)
    settle(a1 + b1)
    out[:, lanes[0]] = gathered(a2, ha1[zl, cy, zh], ra2)
    settle(a2)
    out[:, lanes[1]] = gathered(b2, hb1[cx, cy], rb2)
    settle(b2)


def reduce_scratch(columns):
    half = columns // 2
    f32 = jnp.float32
    shapes = [(2, 1, 2, 4, 4, 2, 8, half),
              (2, 4, 4, 2, 8, half), (3, 2, 4, 2, 8, half), (2, 4, 2, 8, half), (15, 8, half),
              (2, 4, 4, 2, 8, half), (3, 4, 4, 8, half), (4, 4, 8, half), (15, 8, half)]
    return [pltpu.VMEM(shape, f32) for shape in shapes] + [pltpu.SemaphoreType.DMA((40,))] * 2


def per_device(eigvecs, material):
    nx, ny, nz, columns = eigvecs.shape
    total_cells = nx * ny * nz
    for axis in AXES:
        total_cells *= lax.axis_size(axis)
    hy = ny // 2 * nz
    block = nz + hy + 16
    cells = nx * ny
    taps = jnp.asarray(plane_taps(ny, nz), jnp.bfloat16)
    around = jnp.asarray(material_taps(nx, ny), jnp.float32)
    bf16, f32 = jnp.bfloat16, jnp.float32
    dma = pltpu.SemaphoreType.DMA
    vmem = pl.BlockSpec(memory_space=pltpu.VMEM)
    anywhere = pl.BlockSpec(memory_space=pl.ANY)
    scratch = [
        pltpu.VMEM((2, cells, nz), f32),
        pltpu.VMEM(around.shape, f32),
        pltpu.VMEM((nx + 2, 2 * block, columns), bf16),
        pltpu.VMEM((2, ny * nz, 2 * block), bf16),
        pltpu.VMEM((ny, nx, 16, columns), bf16),
        pltpu.VMEM((nx // 2, 2 * ny, columns), bf16),
        pltpu.VMEM((nx // 2, 2 * ny, columns), bf16),
        pltpu.VMEM((2, nx, columns), bf16),
        pltpu.VMEM((2, nx, columns), bf16),
        pltpu.VMEM((2, nx, nz), f32),
        pltpu.VMEM((2, around.shape[0] - 3 * cells, nz), f32),
        pltpu.VMEM((3, nz, cells), f32),
        pltpu.VMEM((3, nx // STEP, nz, cells), f32),
        pltpu.VMEM((STEP, 2, 2 * block, columns), bf16),
        pltpu.VMEM((STEP * ny * nz, 2 * columns), bf16),
        pltpu.VMEM((columns, 2 * columns), f32),
        pltpu.VMEM((2, 2, 4, 4, 2, 8, columns), f32),
        dma((5 + ny,)), dma((48,)), dma((48,)), dma((7,)), dma((7,)), pltpu.SemaphoreType.REGULAR,
    ] + reduce_scratch(columns)
    both = pl.pallas_call(
        functools.partial(kernel, 0.5 / total_cells, (nx, ny, nz)),
        out_shape=pltpu.VMEM((8, columns), f32),
        in_specs=[anywhere] * 4,
        out_specs=vmem,
        scratch_shapes=scratch,
        compiler_params=pltpu.CompilerParams(
            vmem_limit_bytes=60 * 1024 * 1024, collective_id=0, has_side_effects=True),
    )(eigvecs.reshape(nx, ny * nz, columns), material.reshape(2, cells, nz), taps, around)
    return both[:4], both[4:]


def solution(mesh):
    return jax.shard_map(
        per_device,
        mesh=mesh,
        in_specs=(P("gx", "gy", "gz", None), P(None, "gx", "gy", "gz")),
        out_specs=(P(("gx", "gy", "gz"), None), P(("gx", "gy", "gz"), None)),
        check_vma=False,
    )
```
